32 devices in a mesh: seq: 16 (over z, y, x), head: 2 (over core).
Axes of the slice: x: 2, y: 2, z: 4, core: 2. Of those that a mesh axis runs over, the one named last changes fastest.
Arguments:
- acceptance_signal: bfloat16 [8192, 2048], P(('seq', 'head')), may hold values from -6 to 6
- lookup_entries: bfloat16 [8192, 2048], P(('seq', 'head')), may hold values from -6 to 6
- content_entries: bfloat16 [8192, 2048], P(('seq', 'head')), may hold values from -6 to 6
- fading_exponent_table: bfloat16 [8192, 2048], P(('seq', 'head')), may hold values from -17 to 0
- raw_control_signal: bfloat16 [8192, 2048], P(('seq', 'head')), may hold values from -6 to 6
- current_token_reward: float32 [32, 64], P('head'), may hold values from -1 to 1
- slice_scaling_factor: float32 [2048], P('head'), may hold values from 0.1 to 1.9
- result_mapping: bfloat16 [2048, 4096], P('head'), may hold values from -0.125 to 0.125
Outputs:
- time_mixed: bfloat16 [8192, 4096], P(('seq', 'head'))
The draws below stay inside these ranges and needn't reach their ends.
All inputs are finite; a program needn't handle non-finite values.
Results may differ from the reference program's by a relative error of at most 0.009.
Values may be sent and summed in bfloat16 or wider, within the bound.
A program may use at most 192 MiB of HBM per device.

```python
import math
import jax
import jax.numpy as jnp
from jax import lax

D = 4096
ATTENTION_SLICES = 32
SLICE_BREADTH = 64
BLOCK = 128
TOK_SEQ = 512
TOKEN_SPAN = 8192


def draw_fading_exponent_table(key, part):
    hidden_breadth = ATTENTION_SLICES * SLICE_BREADTH
    lookup_lines = jax.random.split(jax.random.fold_in(key, 7), 7)
    share = 0.5
    fast_heads = jax.random.uniform(lookup_lines[0], (ATTENTION_SLICES,)) < share
    fast_rate = jnp.exp(jax.random.uniform(lookup_lines[1], (ATTENTION_SLICES, SLICE_BREADTH), jnp.float32, math.log(1.0 / 50.0), math.log(1.0 / 30.0)))
    slow_rate = jnp.exp(jax.random.uniform(lookup_lines[2], (ATTENTION_SLICES, SLICE_BREADTH), jnp.float32, math.log(1.0 / (8.0 * TOK_SEQ)), math.log(1.0 / TOK_SEQ)))
    base = jnp.where(fast_heads[:, None], fast_rate, slow_rate).reshape(hidden_breadth)
    token_factor = jnp.exp(jax.random.uniform(lookup_lines[3], (TOKEN_SPAN, hidden_breadth), jnp.float32, -math.log(2.0), math.log(2.0)))
    groups = TOKEN_SPAN // TOK_SEQ
    group_factor = jnp.exp(jax.random.uniform(lookup_lines[4], (groups, 1, hidden_breadth), jnp.float32, -math.log(2.0), math.log(2.0)))
    fading_quickness = (token_factor.reshape(groups, TOK_SEQ, hidden_breadth) * group_factor).reshape(TOKEN_SPAN, hidden_breadth) * base[None]
    spike_location = jax.random.randint(lookup_lines[5], (3,), 0, TOKEN_SPAN)
    spike_portion = jax.random.uniform(lookup_lines[6], (3, hidden_breadth), jnp.float32, 0.2, 0.5)
    spike_quickness = -jnp.log(1.0 - spike_portion)
    indicator_selector = (jnp.arange(TOKEN_SPAN)[:, None] == spike_location[None, :]).astype(jnp.float32)
    fading_quickness = fading_quickness + jnp.dot(indicator_selector, spike_quickness)
    return jnp.log(fading_quickness).astype(jnp.bfloat16)


def level_of(key, shape, cuts, least, high):
    level, own = 1.0, jax.random.fold_in(key, 6)
    for axis_at, shards_of in cuts:
        heights = jnp.exp(jax.random.uniform(jax.random.fold_in(own, axis_at), (shards_of,), jnp.float32, least / len(cuts), high / len(cuts)))
        level = level * jnp.repeat(heights, shape[axis_at] // shards_of).reshape([-1 if axis == axis_at else 1 for axis in range(len(shape))])
    return level


def normal_values(own_key, dims, width, most, cuts=(), dtype=jnp.bfloat16):
    loudness = level_of(own_key, dims, cuts, -0.22, 0.18) if cuts else 1.0
    drawn = jax.random.normal(own_key, dims, jnp.float32) * width * loudness
    return jnp.minimum(jnp.maximum(drawn, -most), most).astype(dtype)


def setup_inputs(seed: int = 0) -> dict:
    key_of = jax.random.split(jax.random.key(seed), 9)
    acceptance_signal = normal_values(key_of[0], (TOKEN_SPAN, ATTENTION_SLICES * SLICE_BREADTH), 1.0, 6.0, ((0, 32),))
    lookup_entries = normal_values(key_of[1], (TOKEN_SPAN, ATTENTION_SLICES * SLICE_BREADTH), 1.0, 6.0, ((0, 32),))
    content_entries = normal_values(key_of[2], (TOKEN_SPAN, ATTENTION_SLICES * SLICE_BREADTH), 1.0, 6.0, ((0, 32),))
    fading_exponent_table = draw_fading_exponent_table(jax.random.fold_in(key_of[8], 71), 0)
    raw_control_signal = normal_values(key_of[4], (TOKEN_SPAN, ATTENTION_SLICES * SLICE_BREADTH), 1.0, 6.0, ((0, 32),))
    current_token_reward = jnp.clip(jax.random.uniform(key_of[5], (ATTENTION_SLICES, SLICE_BREADTH), jnp.float32, -1.0, 1.0) * level_of(key_of[5], (ATTENTION_SLICES, SLICE_BREADTH), ((0, 2),), -0.4, 0.0), -1.0, 1.0)
    slice_scaling_factor = jnp.clip(1.0 + 0.18 * jax.random.normal(key_of[6], (ATTENTION_SLICES * SLICE_BREADTH,), jnp.float32), 0.1, 1.9)
    result_mapping = normal_values(key_of[7], (ATTENTION_SLICES * SLICE_BREADTH, D), (ATTENTION_SLICES * SLICE_BREADTH) ** -0.5, 0.125, ((0, 2),))
    return {"acceptance_signal": acceptance_signal, "lookup_entries": lookup_entries, "content_entries": content_entries, "fading_exponent_table": fading_exponent_table, "raw_control_signal": raw_control_signal, "current_token_reward": current_token_reward, "slice_scaling_factor": slice_scaling_factor, "result_mapping": result_mapping}


EPS = 1e-05

def reference(acceptance_signal, lookup_entries, content_entries, fading_exponent_table, raw_control_signal, current_token_reward, slice_scaling_factor, result_mapping):
    length = acceptance_signal.shape[0]
    blocks = length // BLOCK
    high = lax.Precision.HIGHEST
    hidden_breadth = ATTENTION_SLICES * SLICE_BREADTH
    positions = jnp.arange(BLOCK)
    strict = (positions[:, None] > positions[None, :]).astype(jnp.float32)
    gain = slice_scaling_factor.reshape(ATTENTION_SLICES, SLICE_BREADTH)

    def block_step(state, inputs):
        rec_in, key_in, val_in, logit_in, gate_in = inputs
        acceptance_single_real = rec_in.astype(jnp.float32)
        lookup_single_real = key_in.astype(jnp.float32)
        content_single_real = val_in.astype(jnp.float32)
        log_decay = -jnp.exp(logit_in.astype(jnp.float32))
        cum_incl = jnp.cumsum(log_decay, axis=0)
        cum_excl = cum_incl - log_decay
        total = cum_incl[-1]
        rec_scaled = acceptance_single_real * jnp.exp(cum_excl)
        key_scaled = lookup_single_real * jnp.exp(-cum_incl)
        key_ending = lookup_single_real * jnp.exp(total[None] - cum_incl)
        scores = jnp.einsum('thi,shi->hts', rec_scaled, key_scaled, precision=high) * strict[None]
        within = jnp.einsum('hts,shj->thj', scores, content_single_real, precision=high)
        diagonal_contribution = lax.optimization_barrier(jnp.sum(acceptance_single_real * current_token_reward[None] * lookup_single_real, axis=-1, keepdims=True)) * content_single_real
        across = jnp.einsum('thi,hij->thj', rec_scaled, state, precision=high)
        output = within + diagonal_contribution + across
        new_state = jnp.exp(total)[..., None] * state + jnp.einsum('shi,shj->hij', key_ending, content_single_real, precision=high)
        mean = lax.optimization_barrier(jnp.mean(output, axis=-1, keepdims=True))
        centred = output - mean
        var = lax.optimization_barrier(jnp.mean(centred * centred, axis=-1, keepdims=True))
        normed = centred / jnp.sqrt(var + EPS) * gain[None]
        gate_f = gate_in.astype(jnp.float32)
        gated = (normed.reshape(BLOCK, hidden_breadth) * jax.nn.silu(gate_f)).astype(jnp.bfloat16)
        return (new_state, gated)
    shape4 = (blocks, BLOCK, ATTENTION_SLICES, SLICE_BREADTH)
    inputs = (acceptance_signal.reshape(shape4), lookup_entries.reshape(shape4), content_entries.reshape(shape4), fading_exponent_table.reshape(shape4), raw_control_signal.reshape(blocks, BLOCK, hidden_breadth))
    start = jnp.zeros((ATTENTION_SLICES, SLICE_BREADTH, SLICE_BREADTH), jnp.float32)
    final_state, gated = lax.scan(block_step, start, inputs)
    gated = gated.reshape(length, hidden_breadth)
    return jnp.dot(gated, result_mapping, preferred_element_type=jnp.float32).astype(jnp.bfloat16)
```

```python
import functools

import jax
import jax.numpy as jnp
from jax import lax
from jax.experimental import pallas as pl
from jax.experimental.pallas import tpu as pltpu
from jax.sharding import PartitionSpec as P

BLOCK = 128
LANES = 128
QUAD = 256
CHUNK = 512
EXTRA = 16
EPS = 1e-05
MESH = pl.DeviceIdType.MESH
F32 = jnp.float32
BF16 = jnp.bfloat16


def dot(a, b):
    return jnp.dot(a, b, preferred_element_type=F32)


def dot_nt(a, b):
    return lax.dot_general(a, b, (((1,), (1,)), ((), ())), preferred_element_type=F32)


def dot_tn(a, b):
    return lax.dot_general(a, b, (((0,), (0,)), ((), ())), preferred_element_type=F32)


def split_heads(x, low):
    zero = jnp.zeros_like(x)
    return jnp.concatenate([jnp.where(low, x, zero), jnp.where(low, zero, x)], axis=0)


def flip(r, i, members):
    q, bit = 0, 1
    while bit < members:
        q = q + bit * (((r // bit) % 2 + (i // bit) % 2) % 2)
        bit *= 2
    return q


def kernel(
    n, cores, breadth,
    rec_hbm, key_hbm, val_hbm, fade_hbm, gate_hbm, reward_hbm, gain_hbm, map_hbm,
    out_ref,
    fade, key, val, rec, gate, rewards, gains, weight,
    reward_row, cumx, key_mid, centred, recs, local_out, swish, entering, pref_row, mid_row,
    outbox, inbox, before, before_dec, gout, gin, cbox, carry, gated,
    in_sem, p_local, p_send, p_recv, w_sem, w_send, w_recv,
    s_send, s_recv, g_send, g_recv, c_send, c_recv, ready,
):
    me, core = lax.axis_index("seq"), lax.axis_index("head")
    other = 1 - core
    tokens, width = fade.shape
    blocks, quads = tokens // BLOCK, width // QUAD
    half = width // cores
    chunks = weight.shape[1]
    members = quads
    span = members // cores
    groups = n // span
    group = me // span
    r = (me % span) * cores + core

    def place(q):
        return (group * span + q // cores, q % cores)

    def above(g):
        return (g * span + me % span, core)

    sources = (fade_hbm, key_hbm, val_hbm, rec_hbm, gate_hbm)
    held = (fade, key, val, rec, gate)
    first = (1 - r // (members // 2)) * (width // 2)
    second = (r // (members // 2)) * (width // 2)

    def load(i, part):
        at = pl.ds(pl.multiple_of((first, second)[part], LANES), width // 2)
        return pltpu.make_async_copy(
            sources[i].at[:, at], held[i].at[:, at], in_sem.at[2 * i + part]
        )

    for part in range(2):
        for i in range(3):
            load(i, part).start()

    barrier = pltpu.get_barrier_semaphore()

    def greet(i, c):
        pl.semaphore_signal(
            barrier, inc=1, device_id=place(flip(r, i, members)), device_id_type=MESH
        )
        return c

    def greet_above(g, c):
        pl.semaphore_signal(barrier, inc=1, device_id=above(g), device_id_type=MESH)
        return c

    lax.fori_loop(1, members, greet, 0)
    lax.fori_loop(group + 1, groups, greet_above, 0)
    for i in range(3, 5):
        for part in range(2):
            load(i, part).start()

    small = ((reward_hbm, rewards), (gain_hbm, gains))
    small_local = [
        pltpu.make_async_copy(src, dst.at[core], p_local.at[i]) for i, (src, dst) in enumerate(small)
    ]
    small_remote = [
        pltpu.make_async_remote_copy(
            src_ref=src, dst_ref=dst.at[core], send_sem=p_send.at[i], recv_sem=p_recv.at[i],
            device_id=(me, other), device_id_type=MESH,
        )
        for i, (src, dst) in enumerate(small)
    ]
    small_in = [
        pltpu.make_async_remote_copy(
            src_ref=src, dst_ref=dst.at[other], send_sem=p_send.at[i], recv_sem=p_recv.at[i],
            device_id=(me, other), device_id_type=MESH,
        )
        for i, (src, dst) in enumerate(small)
    ]
    for copy in small_local:
        copy.start()

    def columns(k):
        return map_hbm.at[:, pl.ds(pl.multiple_of(k * CHUNK, CHUNK), CHUNK)]

    def weight_local(k):
        return pltpu.make_async_copy(columns(k), weight.at[core, k], w_sem.at[k])

    def weight_remote(k, side):
        return pltpu.make_async_remote_copy(
            src_ref=columns(k), dst_ref=weight.at[side, k],
            send_sem=w_send.at[k], recv_sem=w_recv.at[k],
            device_id=(me, other), device_id_type=MESH,
        )

    def send_weight(start, stop):
        for k in range(start, min(stop, chunks)):
            weight_remote(k, core).start()

    t_id = lax.broadcasted_iota(jnp.int32, (BLOCK, 2 * BLOCK), 0)
    s_id = lax.rem(lax.broadcasted_iota(jnp.int32, (BLOCK, 2 * BLOCK), 1), BLOCK)
    incl = jnp.where(t_id >= s_id, 1.0, 0.0).astype(BF16)
    low = lax.broadcasted_iota(jnp.int32, (BLOCK, LANES), 1) < breadth
    low_s = lax.broadcasted_iota(jnp.int32, (breadth, LANES), 1) < breadth
    row_x = lax.broadcasted_iota(jnp.int32, (EXTRA, LANES), 0)

    def same_head(size):
        i = lax.broadcasted_iota(jnp.int32, (size, size), 0)
        j = lax.broadcasted_iota(jnp.int32, (size, size), 1)
        return i // breadth == j // breadth, i == j

    same, equal = same_head(QUAD)
    means = jnp.where(same, 1.0 / breadth, 0.0).astype(BF16)
    centre = (jnp.where(equal, 1.0, 0.0) - jnp.where(same, 1.0 / breadth, 0.0)).astype(BF16)
    ones = jnp.where(same, 1.0, 0.0).astype(BF16)

    def pack_rows(dec):
        hi = dec.astype(BF16).astype(F32)
        lo = dec - hi
        rows = (hi[:, :LANES], lo[:, :LANES], hi[:, LANES:], lo[:, LANES:])
        out = jnp.zeros((EXTRA, LANES), F32)
        for i, row in enumerate(rows):
            out = jnp.where(row_x == i, row, out)
        return out.astype(BF16)

    def unpack_rows(x):
        x = x.astype(F32)
        return x[0:1] + x[1:2], x[2:3] + x[3:4]

    def member_copy(src, dst, j, slot, send, recv):
        return pltpu.make_async_remote_copy(
            src_ref=src.at[j], dst_ref=dst.at[slot], send_sem=send.at[j], recv_sem=recv.at[slot],
            device_id=place(j), device_id_type=MESH,
        )

    def decays(step, c):
        i = members - 1 - step
        q = flip(r, i, members)
        lanes = pl.ds(pl.multiple_of(q * QUAD, QUAD), QUAD)
        states = [jnp.zeros((breadth, LANES), F32) for _ in range(2)]
        pref = jnp.zeros((1, QUAD), F32)
        for b in range(blocks):
            at = pl.ds(b * BLOCK, BLOCK)
            log_decay = -jnp.exp(fade[at, lanes].astype(F32))
            hi = log_decay.astype(BF16)
            lo = (log_decay - hi.astype(F32)).astype(BF16)
            cum = dot(incl, jnp.concatenate([hi, lo], axis=0))
            mid, total = cum[BLOCK // 2 - 1 : BLOCK // 2], cum[BLOCK - 1 :]
            km = (key[at, lanes].astype(F32) * jnp.exp(mid - cum)).astype(BF16)
            vb = dot(val[at, lanes], centre).astype(BF16)
            cumx[at, lanes] = cum - log_decay
            key_mid[at, lanes] = km
            centred[at, lanes] = vb
            pref_row[b, :, lanes] = pref
            mid_row[b, :, lanes] = mid
            end, whole, begin = jnp.exp(total - mid), jnp.exp(total), jnp.exp(mid)
            for j in range(2):
                cut = slice(j * LANES, (j + 1) * LANES)
                if b > 0:
                    entering[b - 1, 2 * q + j] = (states[j] * begin[:, cut]).astype(BF16)
                product = dot_tn(vb[:, cut], km[:, cut])
                own = jnp.where(low_s, product[:breadth], product[breadth:])
                states[j] = states[j] * whole[:, cut] + own * end[:, cut]
            pref = pref + total
        for j in range(2):
            outbox[q, pl.ds(j * breadth, breadth), :] = states[j].astype(BF16)
        outbox[q, pl.ds(2 * breadth, EXTRA), :] = pack_rows(jnp.exp(pref))

        @pl.when(i > 0)
        def _():
            member_copy(outbox, inbox, q, r, s_send, s_recv).start()

        return c

    def within(step, c):
        q = flip(r, step, members)
        lanes = pl.ds(pl.multiple_of(q * QUAD, QUAD), QUAD)
        gain = gains[q // span, :, pl.ds(pl.multiple_of((q % span) * QUAD, QUAD), QUAD)]
        reward = reward_row[:, lanes]
        for b in range(blocks):
            at = pl.ds(b * BLOCK, BLOCK)
            g = gate[at, lanes].astype(F32)
            swish[at, lanes] = g / (1.0 + jnp.exp(-g)) * gain
            cx = cumx[at, lanes]
            rf = rec[at, lanes].astype(F32)
            kb, vb = key_mid[at, lanes], centred[at, lanes]
            rm = (rf * jnp.exp(cx - mid_row[b, :, lanes])).astype(BF16)
            recs[at, lanes] = (rf * jnp.exp(cx + pref_row[b, :, lanes])).astype(BF16)
            own = rf * key[at, lanes].astype(F32) * reward
            diag = dot(own.astype(BF16), ones)
            for j in range(2):
                cut = slice(j * LANES, (j + 1) * LANES)
                scores = dot_nt(rm[:, cut], split_heads(kb[:, cut], low))
                scores = jnp.where(t_id > s_id, scores, 0.0).astype(BF16)
                o = dot(scores, split_heads(vb[:, cut], low)) + diag[:, cut] * vb[:, cut].astype(F32)
                if b > 0:
                    o = o + dot_nt(rm[:, cut], split_heads(entering[b - 1, 2 * q + j], low_s))
                local_out[at, pl.ds(pl.multiple_of(q * QUAD + j * LANES, LANES), LANES)] = o
        return c

    with jax.named_scope("in0"):
        for i in range(3):
            load(i, 0).wait()
    with jax.named_scope("barrier"):
        pl.semaphore_wait(barrier, members - 1 + group)
        for copy in small_remote:
            copy.start()

        def here(g, c):
            pl.semaphore_signal(ready, inc=1, device_id=above(g), device_id_type=MESH)
            return c

        lax.fori_loop(0, group, here, 0)
        send_weight(0, 2)
        for k in range(chunks):
            weight_local(k).start()
    with jax.named_scope("decays0"):
        lax.fori_loop(0, members // 2, decays, 0)
    with jax.named_scope("in1"):
        for i in range(3):
            load(i, 1).wait()
    with jax.named_scope("decays1"):
        lax.fori_loop(members // 2, members, decays, 0)
    send_weight(2, 5)
    inbox[r] = outbox[r]

    with jax.named_scope("in2"):
        for i in range(3, 5):
            for part in range(2):
                load(i, part).wait()
        for copy in small_local:
            copy.wait()
        for copy in small_in:
            copy.wait_recv()
        heads_held = half // breadth
        for h in range(cores * heads_held):
            reward_row[:, pl.ds(h * breadth, breadth)] = rewards[
                h // heads_held, pl.ds(h % heads_held, 1), :
            ]
    with jax.named_scope("within0"):
        lax.fori_loop(0, members // 2, within, 0)

    def wait_states(i, c):
        j = flip(r, i, members)
        copy = member_copy(outbox, inbox, j, j, s_send, s_recv)
        copy.wait_recv()
        copy.wait_send()
        return c

    with jax.named_scope("wait_states"):
        lax.fori_loop(1, members, wait_states, 0)

    upper, lower = pl.ds(0, breadth), pl.ds(breadth, breadth)

    def advance(box, state):
        s0, s1, d0, d1 = state
        e0, e1 = unpack_rows(box[pl.ds(2 * breadth, EXTRA), :])
        return (
            s0 * e0 + box[upper, :].astype(F32), s1 * e1 + box[lower, :].astype(F32),
            d0 * e0, d1 * e1,
        )

    def scan(j, state):
        before[j, upper, :] = state[0]
        before[j, lower, :] = state[1]
        before_dec[j, :, pl.ds(0, LANES)] = state[2]
        before_dec[j, :, pl.ds(LANES, LANES)] = state[3]
        return advance(inbox.at[j], state)

    zero, one = jnp.zeros((breadth, LANES), F32), jnp.ones((1, LANES), F32)
    with jax.named_scope("scan"):
        s0, s1, d0, d1 = lax.fori_loop(0, members, scan, (zero, zero, one, one))
        gout[upper, :] = s0.astype(BF16)
        gout[lower, :] = s1.astype(BF16)
        gout[pl.ds(2 * breadth, EXTRA), :] = pack_rows(jnp.concatenate([d0, d1], axis=1))

    def group_copy(g, slot):
        return pltpu.make_async_remote_copy(
            src_ref=gout, dst_ref=gin.at[slot], send_sem=g_send.at[g], recv_sem=g_recv.at[slot],
            device_id=above(g), device_id_type=MESH,
        )

    def send_group(g, c):
        group_copy(g, group).start()
        return c

    with jax.named_scope("send_group"):
        @pl.when(group < groups - 1)
        def _():
            pl.semaphore_wait(ready, groups - 1 - group)

        lax.fori_loop(group + 1, groups, send_group, 0)
        send_weight(5, 7)
    with jax.named_scope("within1"):
        lax.fori_loop(members // 2, 3 * members // 4, within, 0)

    def take_group(g, state):
        group_copy(g, g).wait_recv()
        return advance(gin.at[g], state)

    with jax.named_scope("take_group"):
        e0, e1, _, _ = lax.fori_loop(0, group, take_group, (zero, zero, one, one))

    def send_carry(step, c):
        i = members - 1 - step
        j = flip(r, i, members)
        d = before_dec[j]
        cbox[j, upper, :] = (e0 * d[:, :LANES] + before[j, upper, :]).astype(BF16)
        cbox[j, lower, :] = (e1 * d[:, LANES:] + before[j, lower, :]).astype(BF16)

        @pl.when(i > 0)
        def _():
            member_copy(cbox, carry, j, r, c_send, c_recv).start()

        return c

    with jax.named_scope("send_carry"):
        lax.fori_loop(0, members, send_carry, 0)
        carry[r] = cbox[r]
        send_weight(7, chunks)
    with jax.named_scope("within2"):
        lax.fori_loop(3 * members // 4, members, within, 0)

    def finish(i, c):
        q = flip(r, i, members)

        @pl.when(i > 0)
        def _():
            member_copy(cbox, carry, q, q, c_send, c_recv).wait_recv()

        lanes = pl.ds(pl.multiple_of(q * QUAD, QUAD), QUAD)
        a = split_heads(carry[q, upper, :], low_s)
        b = split_heads(carry[q, lower, :], low_s)
        none = jnp.zeros_like(a)
        state = jnp.concatenate(
            [jnp.concatenate([a, none], axis=1), jnp.concatenate([none, b], axis=1)], axis=0
        )
        for k in range(blocks):
            at = pl.ds(k * BLOCK, BLOCK)
            o = local_out[at, lanes] + dot_nt(recs[at, lanes], state)
            var = dot((o * o).astype(BF16), means)
            gated[at, lanes] = (o * lax.rsqrt(var + EPS) * swish[at, lanes]).astype(BF16)
        return c

    with jax.named_scope("finish"):
        lax.fori_loop(0, members, finish, 0)

    def project(k, c):
        weight_local(k).wait()
        weight_remote(k, other).wait_recv()
        total = dot(gated[:, pl.ds(0, half)], weight[0, k])
        for side in range(1, cores):
            total = total + dot(gated[:, pl.ds(side * half, half)], weight[side, k])
        out_ref[:, pl.ds(pl.multiple_of(k * CHUNK, CHUNK), CHUNK)] = total.astype(BF16)
        return c

    with jax.named_scope("project"):
        lax.fori_loop(0, chunks, project, 0)

    def drain_members(i, c):
        j = flip(r, i, members)
        member_copy(cbox, carry, j, j, c_send, c_recv).wait_send()
        return c

    def drain_groups(g, c):
        group_copy(g, group).wait_send()
        return c

    with jax.named_scope("drain"):
        lax.fori_loop(1, members, drain_members, 0)
        lax.fori_loop(group + 1, groups, drain_groups, 0)
        for k in range(chunks):
            weight_remote(k, core).wait_send()
        for copy in small_remote:
            copy.wait_send()


def shards(n, cores, rec, key, val, fade, gate, reward, gain, mapping):
    tokens, width = rec.shape
    breadth = reward.shape[1]
    half, depth = mapping.shape
    blocks, quads, chunks = tokens // BLOCK, width // QUAD, depth // CHUNK
    groups = n * cores // quads
    boxed = 2 * breadth + EXTRA
    dma = pltpu.SemaphoreType.DMA
    held = pltpu.VMEM((tokens, width), BF16)
    wide = pltpu.VMEM((tokens, width), F32)
    anywhere = pl.BlockSpec(memory_space=pl.ANY)
    return pl.pallas_call(
        functools.partial(kernel, n, cores, breadth),
        out_shape=pltpu.VMEM((tokens, depth), BF16),
        in_specs=[anywhere] * 8,
        out_specs=pl.BlockSpec(memory_space=pltpu.VMEM),
        scratch_shapes=[
            held, held, held, held, held,
            pltpu.VMEM((cores,) + reward.shape, F32),
            pltpu.VMEM((cores, 1, half), F32),
            pltpu.VMEM((cores, chunks, half, CHUNK), BF16),
            pltpu.VMEM((1, width), F32),
            wide, held, held, held, wide, wide,
            pltpu.VMEM((max(blocks - 1, 1), 2 * quads, breadth, LANES), BF16),
            pltpu.VMEM((blocks, 1, width), F32),
            pltpu.VMEM((blocks, 1, width), F32),
            pltpu.VMEM((quads, boxed, LANES), BF16),
            pltpu.VMEM((quads, boxed, LANES), BF16),
            pltpu.VMEM((quads, 2 * breadth, LANES), F32),
            pltpu.VMEM((quads, 1, QUAD), F32),
            pltpu.VMEM((boxed, LANES), BF16),
            pltpu.VMEM((groups, boxed, LANES), BF16),
            pltpu.VMEM((quads, 2 * breadth, LANES), BF16),
            pltpu.VMEM((quads, 2 * breadth, LANES), BF16),
            held,
            dma((10,)), dma((2,)), dma((2,)), dma((2,)),
            dma((chunks,)), dma((chunks,)), dma((chunks,)),
            dma((quads,)), dma((quads,)), dma((groups,)), dma((groups,)), dma((quads,)), dma((quads,)),
            pltpu.SemaphoreType.REGULAR,
        ],
        compiler_params=pltpu.CompilerParams(
            collective_id=0, has_side_effects=True, vmem_limit_bytes=52 * 2**20
        ),
    )(rec, key, val, fade, gate, reward, gain.reshape(1, -1), mapping)


def solution(mesh):
    tokens = P(("seq", "head"), None)
    placed = (tokens,) * 5 + (P("head", None), P("head"), P("head", None))
    return jax.shard_map(
        functools.partial(shards, mesh.shape["seq"], mesh.shape["head"]),
        mesh=mesh, in_specs=placed, out_specs=tokens, check_vma=False,
    )
```

```python
import functools

import jax
import jax.numpy as jnp
from jax import lax
from jax.experimental import pallas as pl
from jax.experimental.pallas import tpu as pltpu
from jax.sharding import PartitionSpec as P

BLOCK = 128
LANES = 128
QUAD = 256
CHUNK = 512
EXTRA = 16
EPS = 1e-05
MESH = pl.DeviceIdType.MESH
F32 = jnp.float32
BF16 = jnp.bfloat16


def dot(a, b):
    return jnp.dot(a, b, preferred_element_type=F32)


def dot_nt(a, b):
    return lax.dot_general(a, b, (((1,), (1,)), ((), ())), preferred_element_type=F32)


def dot_tn(a, b):
    return lax.dot_general(a, b, (((0,), (0,)), ((), ())), preferred_element_type=F32)


def split_heads(x, low):
    zero = jnp.zeros_like(x)
    return jnp.concatenate([jnp.where(low, x, zero), jnp.where(low, zero, x)], axis=0)


def flip(r, i, members):
    q, bit = 0, 1
    while bit < members:
        q = q + bit * (((r // bit) % 2 + (i // bit) % 2) % 2)
        bit *= 2
    return q


def kernel(
    n, cores, breadth,
    rec_hbm, key_hbm, val_hbm, fade_hbm, gate_hbm, reward_hbm, gain_hbm, map_hbm,
    out_ref,
    fade, key, val, rec, gate, rewards, gains, weight,
    reward_row, cumx, key_mid, centred, recs, local_out, swish, entering, pref_row, mid_row,
    outbox, inbox, before, before_dec, gout, gin, cbox, carry, gated,
    in_sem, p_local, p_send, p_recv, w_sem, w_send, w_recv,
    s_send, s_recv, g_send, g_recv, c_send, c_recv, ready,
):
    me, core = lax.axis_index("seq"), lax.axis_index("head")
    other = 1 - core
    tokens, width = fade.shape
    blocks, quads = tokens // BLOCK, width // QUAD
    half = width // cores
    chunks = weight.shape[1]
    members = quads
    span = members // cores
    groups = n // span
    group = me // span
    r = (me % span) * cores + core

    def place(q):
        return (group * span + q // cores, q % cores)

    def above(g):
        return (g * span + me % span, core)

    sources = (fade_hbm, key_hbm, val_hbm, rec_hbm, gate_hbm)
    held = (fade, key, val, rec, gate)
    first = (1 - r // (members // 2)) * (width // 2)
    second = (r // (members // 2)) * (width // 2)

    def load(i, part):
        at = pl.ds(pl.multiple_of((first, second)[part], LANES), width // 2)
        return pltpu.make_async_copy(
            sources[i].at[:, at], held[i].at[:, at], in_sem.at[2 * i + part]
        )

    for part in range(2):
        for i in range(3):
            load(i, part).start()

    barrier = pltpu.get_barrier_semaphore()

    def greet(i, c):
        pl.semaphore_signal(
            barrier, inc=1, device_id=place(flip(r, i, members)), device_id_type=MESH
        )
        return c

    def greet_above(g, c):
        pl.semaphore_signal(barrier, inc=1, device_id=above(g), device_id_type=MESH)
        return c

    lax.fori_loop(1, members, greet, 0)
    lax.fori_loop(group + 1, groups, greet_above, 0)
    for i in range(3, 5):
        for part in range(2):
            load(i, part).start()

    small = ((reward_hbm, rewards), (gain_hbm, gains))
    small_local = [
        pltpu.make_async_copy(src, dst.at[core], p_local.at[i]) for i, (src, dst) in enumerate(small)
    ]
    small_remote = [
        pltpu.make_async_remote_copy(
            src_ref=src, dst_ref=dst.at[core], send_sem=p_send.at[i], recv_sem=p_recv.at[i],
            device_id=(me, other), device_id_type=MESH,
        )
        for i, (src, dst) in enumerate(small)
    ]
    small_in = [
        pltpu.make_async_remote_copy(
            src_ref=src, dst_ref=dst.at[other], send_sem=p_send.at[i], recv_sem=p_recv.at[i],
            device_id=(me, other), device_id_type=MESH,
        )
        for i, (src, dst) in enumerate(small)
    ]
    for copy in small_local:
        copy.start()

    def columns(k):
        return map_hbm.at[:, pl.ds(pl.multiple_of(k * CHUNK, CHUNK), CHUNK)]

    def weight_local(k):
        return pltpu.make_async_copy(columns(k), weight.at[core, k], w_sem.at[k])

    def weight_remote(k, side):
        return pltpu.make_async_remote_copy(
            src_ref=columns(k), dst_ref=weight.at[side, k],
            send_sem=w_send.at[k], recv_sem=w_recv.at[k],
            device_id=(me, other), device_id_type=MESH,
        )

    def send_weight(start, stop):
        for k in range(start, min(stop, chunks)):
            weight_remote(k, core).start()

    t_id = lax.broadcasted_iota(jnp.int32, (BLOCK, 2 * BLOCK), 0)
    s_id = lax.rem(lax.broadcasted_iota(jnp.int32, (BLOCK, 2 * BLOCK), 1), BLOCK)
    incl = jnp.where(t_id >= s_id, 1.0, 0.0).astype(BF16)
    low = lax.broadcasted_iota(jnp.int32, (BLOCK, LANES), 1) < breadth
    low_s = lax.broadcasted_iota(jnp.int32, (breadth, LANES), 1) < breadth
    row_x = lax.broadcasted_iota(jnp.int32, (EXTRA, LANES), 0)

    def same_head(size):
        i = lax.broadcasted_iota(jnp.int32, (size, size), 0)
        j = lax.broadcasted_iota(jnp.int32, (size, size), 1)
        return i // breadth == j // breadth, i == j

    same, equal = same_head(QUAD)
    means = jnp.where(same, 1.0 / breadth, 0.0).astype(BF16)
    centre = (jnp.where(equal, 1.0, 0.0) - jnp.where(same, 1.0 / breadth, 0.0)).astype(BF16)
    ones = jnp.where(same, 1.0, 0.0).astype(BF16)

    def pack_rows(dec):
        hi = dec.astype(BF16).astype(F32)
        lo = dec - hi
        rows = (hi[:, :LANES], lo[:, :LANES], hi[:, LANES:], lo[:, LANES:])
        out = jnp.zeros((EXTRA, LANES), F32)
        for i, row in enumerate(rows):
            out = jnp.where(row_x == i, row, out)
        return out.astype(BF16)

    def unpack_rows(x):
        x = x.astype(F32)
        return x[0:1] + x[1:2], x[2:3] + x[3:4]

    def member_copy(src, dst, j, slot, send, recv):
        return pltpu.make_async_remote_copy(
            src_ref=src.at[j], dst_ref=dst.at[slot], send_sem=send.at[j], recv_sem=recv.at[slot],
            device_id=place(j), device_id_type=MESH,
        )

    def quad_lanes(q):
        return pl.ds(pl.multiple_of(q * QUAD, QUAD), QUAD)

    def decays(qs):
        cells = [(k, b) for k in range(len(qs)) for b in range(blocks)]
        cums, logs, vbs, kms = {}, {}, {}, {}
        for k, b in cells:
            at, lanes = pl.ds(b * BLOCK, BLOCK), quad_lanes(qs[k])
            log_decay = -jnp.exp(fade[at, lanes].astype(F32))
            hi = log_decay.astype(BF16)
            lo = (log_decay - hi.astype(F32)).astype(BF16)
            cum = dot(incl, jnp.concatenate([hi, lo], axis=0))
            cumx[at, lanes] = cum - log_decay
            cums[k, b] = cum
        for k, b in cells:
            at, lanes = pl.ds(b * BLOCK, BLOCK), quad_lanes(qs[k])
            vbs[k, b] = dot(val[at, lanes], centre).astype(BF16)
            centred[at, lanes] = vbs[k, b]
        for k, b in cells:
            at, lanes = pl.ds(b * BLOCK, BLOCK), quad_lanes(qs[k])
            cum = cums[k, b]
            mid = cum[BLOCK // 2 - 1 : BLOCK // 2]
            kms[k, b] = (key[at, lanes].astype(F32) * jnp.exp(mid - cum)).astype(BF16)
            key_mid[at, lanes] = kms[k, b]
            mid_row[b, :, lanes] = mid
        products = {}
        for k, b in cells:
            for j in range(2):
                cut = slice(j * LANES, (j + 1) * LANES)
                products[k, b, j] = dot_tn(vbs[k, b][:, cut], kms[k, b][:, cut])
        for k, q in enumerate(qs):
            lanes = quad_lanes(q)
            states = [jnp.zeros((breadth, LANES), F32) for _ in range(2)]
            pref = jnp.zeros((1, QUAD), F32)
            for b in range(blocks):
                cum = cums[k, b]
                mid, total = cum[BLOCK // 2 - 1 : BLOCK // 2], cum[BLOCK - 1 :]
                end, whole, begin = jnp.exp(total - mid), jnp.exp(total), jnp.exp(mid)
                pref_row[b, :, lanes] = pref
                for j in range(2):
                    cut = slice(j * LANES, (j + 1) * LANES)
                    if b > 0:
                        entering[b - 1, 2 * q + j] = (states[j] * begin[:, cut]).astype(BF16)
                    product = products[k, b, j]
                    own = jnp.where(low_s, product[:breadth], product[breadth:])
                    states[j] = states[j] * whole[:, cut] + own * end[:, cut]
                pref = pref + total
            for j in range(2):
                outbox[q, pl.ds(j * breadth, breadth), :] = states[j].astype(BF16)
            outbox[q, pl.ds(2 * breadth, EXTRA), :] = pack_rows(jnp.exp(pref))

    def within(qs):
        cells = [(k, b) for k in range(len(qs)) for b in range(blocks)]
        rms, diags, scored = {}, {}, {}
        for k, b in cells:
            q = qs[k]
            at, lanes = pl.ds(b * BLOCK, BLOCK), quad_lanes(q)
            cx = cumx[at, lanes]
            rf = rec[at, lanes].astype(F32)
            rms[k, b] = (rf * jnp.exp(cx - mid_row[b, :, lanes])).astype(BF16)
            recs[at, lanes] = (rf * jnp.exp(cx + pref_row[b, :, lanes])).astype(BF16)
            own = rf * key[at, lanes].astype(F32) * reward_row[:, lanes]
            diags[k, b] = dot(own.astype(BF16), ones)
            kb = key_mid[at, lanes]
            for j in range(2):
                cut = slice(j * LANES, (j + 1) * LANES)
                scored[k, b, j] = dot_nt(rms[k, b][:, cut], split_heads(kb[:, cut], low))
        for k, b in cells:
            q = qs[k]
            at, lanes = pl.ds(b * BLOCK, BLOCK), quad_lanes(q)
            gain = gains[q // span, :, pl.ds(pl.multiple_of((q % span) * QUAD, QUAD), QUAD)]
            g = gate[at, lanes].astype(F32)
            swish[at, lanes] = g / (1.0 + jnp.exp(-g)) * gain
        for k, b in cells:
            q = qs[k]
            at, lanes = pl.ds(b * BLOCK, BLOCK), quad_lanes(q)
            vb = centred[at, lanes]
            for j in range(2):
                cut = slice(j * LANES, (j + 1) * LANES)
                scores = jnp.where(t_id > s_id, scored[k, b, j], 0.0).astype(BF16)
                o = dot(scores, split_heads(vb[:, cut], low))
                if b > 0:
                    o = o + dot_nt(rms[k, b][:, cut], split_heads(entering[b - 1, 2 * q + j], low_s))
                o = o + diags[k, b][:, cut] * vb[:, cut].astype(F32)
                local_out[at, pl.ds(pl.multiple_of(q * QUAD + j * LANES, LANES), LANES)] = o

    def withins(first, batch):
        def body(step, c):
            within([flip(r, first + step * batch + k, members) for k in range(batch)])
            return c
        return body

    def finish(qs):
        cells = [(k, b) for k in range(len(qs)) for b in range(blocks)]
        states, outs, variances = [], {}, {}
        for q in qs:
            a = split_heads(carry[q, upper, :], low_s)
            b = split_heads(carry[q, lower, :], low_s)
            none = jnp.zeros_like(a)
            states.append(jnp.concatenate(
                [jnp.concatenate([a, none], axis=1), jnp.concatenate([none, b], axis=1)], axis=0
            ))
        for k, b in cells:
            at, lanes = pl.ds(b * BLOCK, BLOCK), quad_lanes(qs[k])
            outs[k, b] = local_out[at, lanes] + dot_nt(recs[at, lanes], states[k])
        for k, b in cells:
            variances[k, b] = dot((outs[k, b] * outs[k, b]).astype(BF16), means)
        for k, b in cells:
            at, lanes = pl.ds(b * BLOCK, BLOCK), quad_lanes(qs[k])
            scale = lax.rsqrt(variances[k, b] + EPS) * swish[at, lanes]
            gated[at, lanes] = (outs[k, b] * scale).astype(BF16)

    upper, lower = pl.ds(0, breadth), pl.ds(breadth, breadth)
    far = [flip(r, i, members) for i in range(members - 1, members // 2 - 1, -1)]
    near = [flip(r, i, members) for i in range(members // 2 - 1, -1, -1)]

    with jax.named_scope("in0"):
        for i in range(3):
            load(i, 0).wait()
    with jax.named_scope("decays0"):
        decays(far)
    with jax.named_scope("barrier"):
        pl.semaphore_wait(barrier, members - 1 + group)
        for q in far:
            member_copy(outbox, inbox, q, r, s_send, s_recv).start()
        for copy in small_remote:
            copy.start()

        def here(g, c):
            pl.semaphore_signal(ready, inc=1, device_id=above(g), device_id_type=MESH)
            return c

        lax.fori_loop(0, group, here, 0)
    with jax.named_scope("in1"):
        for i in range(3):
            load(i, 1).wait()
        for k in range(chunks):
            weight_local(k).start()
    with jax.named_scope("decays1"):
        decays(near)
    for q in near[:-1]:
        member_copy(outbox, inbox, q, r, s_send, s_recv).start()
    send_weight(0, 3)
    inbox[r] = outbox[r]

    with jax.named_scope("in2"):
        for i in range(3, 5):
            for part in range(2):
                load(i, part).wait()
        for copy in small_local:
            copy.wait()
        for copy in small_in:
            copy.wait_recv()
        heads_held = half // breadth
        for h in range(cores * heads_held):
            reward_row[:, pl.ds(h * breadth, breadth)] = rewards[
                h // heads_held, pl.ds(h % heads_held, 1), :
            ]
    with jax.named_scope("within0"):
        lax.fori_loop(0, 2, withins(0, 2), 0)

    def wait_states(i, c):
        j = flip(r, i, members)
        copy = member_copy(outbox, inbox, j, j, s_send, s_recv)
        copy.wait_recv()
        copy.wait_send()
        return c

    with jax.named_scope("wait_states"):
        lax.fori_loop(1, members, wait_states, 0)

    def advance(box, state):
        s0, s1, d0, d1 = state
        e0, e1 = unpack_rows(box[pl.ds(2 * breadth, EXTRA), :])
        return (
            s0 * e0 + box[upper, :].astype(F32), s1 * e1 + box[lower, :].astype(F32),
            d0 * e0, d1 * e1,
        )

    def scan(j, state):
        before[j, upper, :] = state[0]
        before[j, lower, :] = state[1]
        before_dec[j, :, pl.ds(0, LANES)] = state[2]
        before_dec[j, :, pl.ds(LANES, LANES)] = state[3]
        return advance(inbox.at[j], state)

    zero, one = jnp.zeros((breadth, LANES), F32), jnp.ones((1, LANES), F32)
    with jax.named_scope("scan"):
        s0, s1, d0, d1 = lax.fori_loop(0, members, scan, (zero, zero, one, one))
        gout[upper, :] = s0.astype(BF16)
        gout[lower, :] = s1.astype(BF16)
        gout[pl.ds(2 * breadth, EXTRA), :] = pack_rows(jnp.concatenate([d0, d1], axis=1))

    def group_copy(g, slot):
        return pltpu.make_async_remote_copy(
            src_ref=gout, dst_ref=gin.at[slot], send_sem=g_send.at[g], recv_sem=g_recv.at[slot],
            device_id=above(g), device_id_type=MESH,
        )

    def send_group(g, c):
        group_copy(g, group).start()
        return c

    with jax.named_scope("send_group"):
        @pl.when(group < groups - 1)
        def _():
            pl.semaphore_wait(ready, groups - 1 - group)

        lax.fori_loop(group + 1, groups, send_group, 0)
        send_weight(3, 5)
    with jax.named_scope("within1"):
        withins(members // 2, 2)(0, 0)

    def take_group(g, state):
        group_copy(g, g).wait_recv()
        return advance(gin.at[g], state)

    with jax.named_scope("take_group"):
        e0, e1, _, _ = lax.fori_loop(0, group, take_group, (zero, zero, one, one))

    def send_carry(step, c):
        i = members - 1 - step
        j = flip(r, i, members)
        d = before_dec[j]
        cbox[j, upper, :] = (e0 * d[:, :LANES] + before[j, upper, :]).astype(BF16)
        cbox[j, lower, :] = (e1 * d[:, LANES:] + before[j, lower, :]).astype(BF16)

        @pl.when(i > 0)
        def _():
            member_copy(cbox, carry, j, r, c_send, c_recv).start()

        return c

    with jax.named_scope("send_carry"):
        lax.fori_loop(0, members, send_carry, 0)
        carry[r] = cbox[r]
        send_weight(5, chunks)
    with jax.named_scope("within2"):
        withins(3 * members // 4, 2)(0, 0)

    for name, qs in (("near", near), ("far", far)):
        with jax.named_scope("wait_" + name):
            for q in qs:
                if q is not near[-1]:
                    member_copy(cbox, carry, q, q, c_send, c_recv).wait_recv()
        with jax.named_scope("finish_" + name):
            finish(qs)

    def project(k, c):
        weight_local(k).wait()
        weight_remote(k, other).wait_recv()
        total = dot(gated[:, pl.ds(0, half)], weight[0, k])
        for side in range(1, cores):
            total = total + dot(gated[:, pl.ds(side * half, half)], weight[side, k])
        out_ref[:, pl.ds(pl.multiple_of(k * CHUNK, CHUNK), CHUNK)] = total.astype(BF16)
        return c

    with jax.named_scope("project"):
        lax.fori_loop(0, chunks, project, 0)

    def drain_members(i, c):
        j = flip(r, i, members)
        member_copy(cbox, carry, j, j, c_send, c_recv).wait_send()
        return c

    def drain_groups(g, c):
        group_copy(g, group).wait_send()
        return c

    with jax.named_scope("drain"):
        lax.fori_loop(1, members, drain_members, 0)
        lax.fori_loop(group + 1, groups, drain_groups, 0)
        for k in range(chunks):
            weight_remote(k, core).wait_send()
        for copy in small_remote:
            copy.wait_send()


def shards(n, cores, rec, key, val, fade, gate, reward, gain, mapping):
    tokens, width = rec.shape
    breadth = reward.shape[1]
    half, depth = mapping.shape
    blocks, quads, chunks = tokens // BLOCK, width // QUAD, depth // CHUNK
    groups = n * cores // quads
    boxed = 2 * breadth + EXTRA
    dma = pltpu.SemaphoreType.DMA
    held = pltpu.VMEM((tokens, width), BF16)
    wide = pltpu.VMEM((tokens, width), F32)
    anywhere = pl.BlockSpec(memory_space=pl.ANY)
    return pl.pallas_call(
        functools.partial(kernel, n, cores, breadth),
        out_shape=pltpu.VMEM((tokens, depth), BF16),
        in_specs=[anywhere] * 8,
        out_specs=pl.BlockSpec(memory_space=pltpu.VMEM),
        scratch_shapes=[
            held, held, held, held, held,
            pltpu.VMEM((cores,) + reward.shape, F32),
            pltpu.VMEM((cores, 1, half), F32),
            pltpu.VMEM((cores, chunks, half, CHUNK), BF16),
            pltpu.VMEM((1, width), F32),
            wide, held, held, held, wide, wide,
            pltpu.VMEM((max(blocks - 1, 1), 2 * quads, breadth, LANES), BF16),
            pltpu.VMEM((blocks, 1, width), F32),
            pltpu.VMEM((blocks, 1, width), F32),
            pltpu.VMEM((quads, boxed, LANES), BF16),
            pltpu.VMEM((quads, boxed, LANES), BF16),
            pltpu.VMEM((quads, 2 * breadth, LANES), F32),
            pltpu.VMEM((quads, 1, QUAD), F32),
            pltpu.VMEM((boxed, LANES), BF16),
            pltpu.VMEM((groups, boxed, LANES), BF16),
            pltpu.VMEM((quads, 2 * breadth, LANES), BF16),
            pltpu.VMEM((quads, 2 * breadth, LANES), BF16),
            held,
            dma((10,)), dma((2,)), dma((2,)), dma((2,)),
            dma((chunks,)), dma((chunks,)), dma((chunks,)),
            dma((quads,)), dma((quads,)), dma((groups,)), dma((groups,)), dma((quads,)), dma((quads,)),
            pltpu.SemaphoreType.REGULAR,
        ],
        compiler_params=pltpu.CompilerParams(
            collective_id=0, has_side_effects=True, vmem_limit_bytes=52 * 2**20
        ),
    )(rec, key, val, fade, gate, reward, gain.reshape(1, -1), mapping)


def solution(mesh):
    tokens = P(("seq", "head"), None)
    placed = (tokens,) * 5 + (P("head", None), P("head"), P("head", None))
    return jax.shard_map(
        functools.partial(shards, mesh.shape["seq"], mesh.shape["head"]),
        mesh=mesh, in_specs=placed, out_specs=tokens, check_vma=False,
    )
```

```python
import functools

import jax
import jax.numpy as jnp
from jax import lax
from jax.experimental import pallas as pl
from jax.experimental.pallas import tpu as pltpu
from jax.sharding import PartitionSpec as P

BLOCK = 128
LANES = 128
QUAD = 256
CHUNK = 512
LEAD = 4
EXTRA = 8
EPS = 1e-05
MESH = pl.DeviceIdType.MESH
F32 = jnp.float32
BF16 = jnp.bfloat16


def dot(a, b):
    return jnp.dot(a, b, preferred_element_type=F32)


def dot_nt(a, b):
    return lax.dot_general(a, b, (((1,), (1,)), ((), ())), preferred_element_type=F32)


def dot_tn(a, b):
    return lax.dot_general(a, b, (((0,), (0,)), ((), ())), preferred_element_type=F32)


def split_heads(x, low):
    zero = jnp.zeros_like(x)
    return jnp.concatenate([jnp.where(low, x, zero), jnp.where(low, zero, x)], axis=0)


def flip(r, i, members):
    q, bit = 0, 1
    while bit < members:
        q = q + bit * (((r // bit) % 2 + (i // bit) % 2) % 2)
        bit *= 2
    return q


def kernel(
    n, cores, breadth,
    rec_hbm, key_hbm, val_hbm, fade_hbm, gate_hbm, reward_hbm, gain_hbm, map_hbm,
    out_ref,
    held, rewards, gains, weight,
    reward_row, cumx, key_mid, centred, recs, local_out, swish, entering, pref_row, mid_row,
    outbox, inbox, before, before_dec, gout, gin, cbox, carry, gated, partial,
    in_sem, p_local, p_send, p_recv, w_sem, w_send,
    s_send, s_recv, g_send, g_recv, c_send, c_recv, ready,
):
    me, core = lax.axis_index("seq"), lax.axis_index("head")
    other = 1 - core
    tokens, width = held.shape[1:]
    half = width // cores
    blocks, quads = tokens // BLOCK, half // QUAD
    chunks = weight.shape[1]
    lead = min(LEAD, chunks)
    members = half // LANES
    span = members // cores
    groups = n // span
    group = me // span
    r = (me % span) * cores + core
    peers = [flip(r, i, members) for i in range(members - 1, 0, -1)]
    fade, key, val, rec, gate = (held.at[i] for i in range(5))
    sources = (fade_hbm, key_hbm, val_hbm, rec_hbm, gate_hbm)

    def place(q):
        return (group * span + q // cores, q % cores)

    def above(g):
        return (g * span + me % span, core)

    barrier = pltpu.get_barrier_semaphore()
    for q in peers:
        pl.semaphore_signal(barrier, inc=1, device_id=place(q), device_id_type=MESH)

    for p in range(cores):
        for i in range(3):
            at = pl.ds(p * half, half)
            pltpu.make_async_copy(sources[i].at[:, at], held.at[i, :, at], in_sem.at[p]).start()

    def greet_above(g, c):
        pl.semaphore_signal(barrier, inc=1, device_id=above(g), device_id_type=MESH)
        return c

    lax.fori_loop(group + 1, groups, greet_above, 0)
    for i in range(3, 5):
        pltpu.make_async_copy(sources[i], held.at[i], in_sem.at[cores]).start()

    def wait_all(ref, sem):
        pltpu.make_async_copy(ref, ref, sem).wait()

    small = ((reward_hbm, rewards), (gain_hbm, gains))
    small_local = [
        pltpu.make_async_copy(src, dst.at[core], p_local.at[i]) for i, (src, dst) in enumerate(small)
    ]

    def small_copy(i, side):
        src, dst = small[i]
        return pltpu.make_async_remote_copy(
            src_ref=src, dst_ref=dst.at[side], send_sem=p_send.at[i], recv_sem=p_recv.at[i],
            device_id=(me, other), device_id_type=MESH,
        )

    for copy in small_local:
        copy.start()

    def columns(k):
        return map_hbm.at[:, pl.ds(k * CHUNK, CHUNK)]

    def weight_sem(k):
        return w_sem.at[max(k - lead + 1, 0)]

    def send_weight(start, stop):
        for k in range(start, min(stop, chunks)):
            pltpu.make_async_remote_copy(
                src_ref=columns(k), dst_ref=weight.at[core, k],
                send_sem=w_send.at[0], recv_sem=weight_sem(k),
                device_id=(me, other), device_id_type=MESH,
            ).start()

    t_id = lax.broadcasted_iota(jnp.int32, (BLOCK, 2 * BLOCK), 0)
    s_id = lax.rem(lax.broadcasted_iota(jnp.int32, (BLOCK, 2 * BLOCK), 1), BLOCK)
    incl = jnp.where(t_id >= s_id, 1.0, 0.0).astype(BF16)
    low = lax.broadcasted_iota(jnp.int32, (BLOCK, LANES), 1) < breadth
    low_s = lax.broadcasted_iota(jnp.int32, (breadth, LANES), 1) < breadth
    row_x = lax.broadcasted_iota(jnp.int32, (EXTRA, LANES), 0)
    head_i = lax.broadcasted_iota(jnp.int32, (QUAD, QUAD), 0)
    head_j = lax.broadcasted_iota(jnp.int32, (QUAD, QUAD), 1)
    same, equal = head_i // breadth == head_j // breadth, head_i == head_j
    means = jnp.where(same, 1.0 / breadth, 0.0).astype(BF16)
    centre = (jnp.where(equal, 1.0, 0.0) - jnp.where(same, 1.0 / breadth, 0.0)).astype(BF16)
    ones = jnp.where(same, 1.0, 0.0).astype(BF16)
    state_rows, decay_rows = pl.ds(0, breadth), pl.ds(breadth, EXTRA)
    cuts = [slice(j * LANES, (j + 1) * LANES) for j in range(2)]

    def pack_rows(dec):
        hi = dec.astype(BF16).astype(F32)
        return jnp.where(row_x == 0, hi, jnp.where(row_x == 1, dec - hi, 0.0)).astype(BF16)

    def unpack_rows(x):
        x = x.astype(F32)
        return x[0:1] + x[1:2]

    def quad_lanes(p, t):
        return pl.ds(p * half + t * QUAD, QUAD)

    def decays(p):
        cells = [(t, b) for t in range(quads) for b in range(blocks)]
        cums, vbs, kms, products = {}, {}, {}, {}
        for t, b in cells:
            at, lanes = pl.ds(b * BLOCK, BLOCK), quad_lanes(p, t)
            log_decay = -jnp.exp(fade[at, lanes].astype(F32))
            hi = log_decay.astype(BF16)
            lo = (log_decay - hi.astype(F32)).astype(BF16)
            cum = dot(incl, jnp.concatenate([hi, lo], axis=0))
            cumx[at, lanes] = cum - log_decay
            cums[t, b] = cum
        for t, b in cells:
            at, lanes = pl.ds(b * BLOCK, BLOCK), quad_lanes(p, t)
            vbs[t, b] = dot(val[at, lanes], centre).astype(BF16)
            centred[at, lanes] = vbs[t, b]
        for t, b in cells:
            at, lanes = pl.ds(b * BLOCK, BLOCK), quad_lanes(p, t)
            mid = cums[t, b][BLOCK // 2 - 1 : BLOCK // 2]
            kms[t, b] = (key[at, lanes].astype(F32) * jnp.exp(mid - cums[t, b])).astype(BF16)
            key_mid[at, lanes] = kms[t, b]
            mid_row[b, :, lanes] = mid
        for t, b in cells:
            for j, cut in enumerate(cuts):
                products[t, b, j] = dot_tn(vbs[t, b][:, cut], kms[t, b][:, cut])
        for t in range(quads):
            lanes = quad_lanes(p, t)
            states = [jnp.zeros((breadth, LANES), F32) for _ in range(2)]
            pref = jnp.zeros((1, QUAD), F32)
            for b in range(blocks):
                cum = cums[t, b]
                mid, total = cum[BLOCK // 2 - 1 : BLOCK // 2], cum[BLOCK - 1 :]
                end, whole, begin = jnp.exp(total - mid), jnp.exp(total), jnp.exp(mid)
                pref_row[b, :, lanes] = pref
                for j, cut in enumerate(cuts):
                    if b > 0:
                        entering[p, b - 1, 2 * t + j] = (states[j] * begin[:, cut]).astype(BF16)
                    product = products[t, b, j]
                    own = jnp.where(low_s, product[:breadth], product[breadth:])
                    states[j] = states[j] * whole[:, cut] + own * end[:, cut]
                pref = pref + total
            gone = jnp.exp(pref)
            for j, cut in enumerate(cuts):
                outbox[p, 2 * t + j, state_rows, :] = states[j].astype(BF16)
                outbox[p, 2 * t + j, decay_rows, :] = pack_rows(gone[:, cut])

    def within(units):
        cells = [(p, t, b) for p, t in units for b in range(blocks)]
        rms, diags, scored = {}, {}, {}
        for p, t, b in cells:
            at, lanes = pl.ds(b * BLOCK, BLOCK), quad_lanes(p, t)
            cx = cumx[at, lanes]
            rf = rec[at, lanes].astype(F32)
            rms[p, t, b] = (rf * jnp.exp(cx - mid_row[b, :, lanes])).astype(BF16)
            recs[at, lanes] = (rf * jnp.exp(cx + pref_row[b, :, lanes])).astype(BF16)
            own = rf * key[at, lanes].astype(F32) * reward_row[:, lanes]
            diags[p, t, b] = dot(own.astype(BF16), ones)
            kb = key_mid[at, lanes]
            for j, cut in enumerate(cuts):
                scored[p, t, b, j] = dot_nt(rms[p, t, b][:, cut], split_heads(kb[:, cut], low))
        for p, t, b in cells:
            at, lanes = pl.ds(b * BLOCK, BLOCK), quad_lanes(p, t)
            g = gate[at, lanes].astype(F32)
            swish[at, lanes] = g / (1.0 + jnp.exp(-g)) * gains[p, :, pl.ds(t * QUAD, QUAD)]
        for p, t, b in cells:
            at, lanes = pl.ds(b * BLOCK, BLOCK), quad_lanes(p, t)
            vb = centred[at, lanes]
            for j, cut in enumerate(cuts):
                scores = jnp.where(t_id > s_id, scored[p, t, b, j], 0.0).astype(BF16)
                o = dot(scores, split_heads(vb[:, cut], low))
                if b > 0:
                    came = split_heads(entering[p, b - 1, 2 * t + j], low_s)
                    o = o + dot_nt(rms[p, t, b][:, cut], came)
                o = o + diags[p, t, b][:, cut] * vb[:, cut].astype(F32)
                local_out[at, pl.ds(p * half + t * QUAD + j * LANES, LANES)] = o

    def finish(p):
        cells = [(t, b) for t in range(quads) for b in range(blocks)]
        states, outs, variances = [], {}, {}
        for t in range(quads):
            x, y = (split_heads(carry[p, 2 * t + j], low_s) for j in range(2))
            none = jnp.zeros_like(x)
            states.append(jnp.concatenate(
                [jnp.concatenate([x, none], axis=1), jnp.concatenate([none, y], axis=1)], axis=0
            ))
        for t, b in cells:
            at, lanes = pl.ds(b * BLOCK, BLOCK), quad_lanes(p, t)
            outs[t, b] = local_out[at, lanes] + dot_nt(recs[at, lanes], states[t])
        for t, b in cells:
            variances[t, b] = dot((outs[t, b] * outs[t, b]).astype(BF16), means)
        for t, b in cells:
            at, lanes = pl.ds(b * BLOCK, BLOCK), quad_lanes(p, t)
            scale = lax.rsqrt(variances[t, b] + EPS) * swish[at, lanes]
            gated[at, lanes] = (outs[t, b] * scale).astype(BF16)

    def member_copy(src, dst, p, j, send, recv):
        return pltpu.make_async_remote_copy(
            src_ref=src.at[p, j], dst_ref=dst.at[p, r], send_sem=send.at[p], recv_sem=recv.at[p],
            device_id=place(j), device_id_type=MESH,
        )

    def send_states(p):
        for q in peers:
            member_copy(outbox, inbox, p, q, s_send, s_recv).start()
        inbox[p, r] = outbox[p, r]

    some = pl.ds(0, members - 1)

    def advance(box, state):
        s, d = state
        e = unpack_rows(box[decay_rows, :])
        return s * e + box[state_rows, :].astype(F32), d * e

    nothing = (jnp.zeros((breadth, LANES), F32), jnp.ones((1, LANES), F32))

    def scan(p):
        state = nothing
        for j in range(members):
            before[p, j] = state[0]
            before_dec[p, j] = state[1]
            state = advance(inbox.at[p, j], state)
        gout[p, state_rows, :] = state[0].astype(BF16)
        gout[p, decay_rows, :] = pack_rows(state[1])

    def group_copy(p, g, slot):
        return pltpu.make_async_remote_copy(
            src_ref=gout.at[p], dst_ref=gin.at[p, slot],
            send_sem=g_send.at[p, g], recv_sem=g_recv.at[p, slot],
            device_id=above(g), device_id_type=MESH,
        )

    def send_group(p):
        def body(i, c):
            group_copy(p, groups - 1 - i, group).start()
            return c

        lax.fori_loop(0, groups - 1 - group, body, 0)

    def take_group(p):
        def body(g, state):
            group_copy(p, g, g).wait_recv()
            return advance(gin.at[p, g], state)

        return lax.fori_loop(0, group, body, nothing)[0]

    def send_carry(p, came):
        for j in range(members):
            cbox[p, j] = (came * before_dec[p, j] + before[p, j]).astype(BF16)
        for q in peers:
            member_copy(cbox, carry, p, q, c_send, c_recv).start()
        carry[p, r] = cbox[p, r]

    with jax.named_scope("in0"):
        wait_all(held.at[pl.ds(0, 3), :, pl.ds(0, half)], in_sem.at[0])
    with jax.named_scope("decays0"):
        decays(0)
    with jax.named_scope("barrier"):
        pl.semaphore_wait(barrier, members - 1 + group)
        send_states(0)
        for i in range(2):
            small_copy(i, core).start()

        def here(g, c):
            pl.semaphore_signal(ready, inc=1, device_id=above(g), device_id_type=MESH)
            return c

        lax.fori_loop(0, group, here, 0)
        for k in range(chunks):
            pltpu.make_async_copy(columns(k), weight.at[core, k], weight_sem(k)).start()
    for p in range(1, cores):
        with jax.named_scope("in1"):
            wait_all(held.at[pl.ds(0, 3), :, pl.ds(p * half, half)], in_sem.at[p])
        with jax.named_scope("decays1"):
            decays(p)
        with jax.named_scope("send1"):
            send_states(p)
    send_weight(0, 2)

    with jax.named_scope("in2"):
        wait_all(held.at[pl.ds(3, 2)], in_sem.at[cores])
        for i in range(2):
            small_local[i].wait()
            small_copy(i, other).wait_recv()
        for h in range(width // breadth):
            reward_row[:, pl.ds(h * breadth, breadth)] = rewards[
                h * breadth // half, pl.ds(h % (half // breadth), 1), :
            ]

    units = [(p, t) for p in range(cores) for t in range(quads)]
    done = 0

    def some_within(count):
        nonlocal done
        for at in range(done, min(done + count, len(units)), 2):
            with jax.named_scope("within"):
                within(units[at : at + 2])
        done += count

    some_within(4)
    for p in range(cores):
        with jax.named_scope("wait_states"):
            wait_all(inbox.at[p, some], s_recv.at[p])
        with jax.named_scope("scan"):
            scan(p)
        with jax.named_scope("send_group"):
            if p == 0:
                @pl.when(group < groups - 1)
                def _():
                    pl.semaphore_wait(ready, groups - 1 - group)

            send_group(p)

            @pl.when(group > 0)
            def _():
                send_weight(2 + p, 3 + p if p < cores - 1 else lead)

        some_within(2 if p < cores - 1 else len(units))
    for p in range(cores):
        with jax.named_scope("take_group"):
            came = take_group(p)
        with jax.named_scope("send_carry"):
            send_carry(p, came)
    with jax.named_scope("send_weight"):
        @pl.when(group == 0)
        def _():
            send_weight(2, lead)

        send_weight(lead, chunks)

    def project(k, first, last):
        at = pl.ds(k * CHUNK, CHUNK)
        total = partial[:, at] if first > 0 else None
        for p in range(first, last):
            term = dot(gated[:, pl.ds(p * half, half)], weight[p, k])
            total = term if total is None else total + term
        if last < cores:
            partial[:, at] = total
        else:
            out_ref[:, at] = total.astype(BF16)

    for p in range(cores - 1):
        with jax.named_scope("wait_carry"):
            wait_all(carry.at[p, some], c_recv.at[p])
        with jax.named_scope("finish"):
            finish(p)
    with jax.named_scope("wait_weight"):
        wait_all(weight.at[:, pl.ds(0, lead)], w_sem.at[0])
    with jax.named_scope("project_lead"):
        for k in range(lead):
            project(k, 0, cores - 1)
    with jax.named_scope("wait_carry"):
        wait_all(carry.at[cores - 1, some], c_recv.at[cores - 1])
    with jax.named_scope("finish"):
        finish(cores - 1)
    with jax.named_scope("project_led"):
        for k in range(lead):
            project(k, cores - 1, cores)
    for k in range(lead, chunks):
        with jax.named_scope("wait_weight"):
            wait_all(weight.at[:, k], weight_sem(k))
        with jax.named_scope("project_rest"):
            project(k, 0, cores)

    def drain_groups(g, c):
        for p in range(cores):
            group_copy(p, g, group).wait_send()
        return c

    with jax.named_scope("drain"):
        lax.fori_loop(group + 1, groups, drain_groups, 0)
        for p in range(cores):
            wait_all(outbox.at[p, some], s_send.at[p])
            wait_all(cbox.at[p, some], c_send.at[p])
        wait_all(weight.at[other], w_send.at[0])
        for i in range(2):
            small_copy(i, core).wait_send()


def shards(n, cores, rec, key, val, fade, gate, reward, gain, mapping):
    tokens, width = rec.shape
    breadth = reward.shape[1]
    half, depth = mapping.shape
    blocks, chunks, members = tokens // BLOCK, depth // CHUNK, half // LANES
    groups = n * cores // members
    boxed = breadth + EXTRA
    dma = pltpu.SemaphoreType.DMA
    narrow = pltpu.VMEM((tokens, width), BF16)
    wide = pltpu.VMEM((tokens, width), F32)
    return pl.pallas_call(
        functools.partial(kernel, n, cores, breadth),
        out_shape=pltpu.VMEM((tokens, depth), BF16),
        in_specs=[pl.BlockSpec(memory_space=pl.ANY)] * 8,
        out_specs=pl.BlockSpec(memory_space=pltpu.VMEM),
        scratch_shapes=[
            pltpu.VMEM((5, tokens, width), BF16),
            pltpu.VMEM((cores,) + reward.shape, F32),
            pltpu.VMEM((cores, 1, half), F32),
            pltpu.VMEM((cores, chunks, half, CHUNK), BF16),
            pltpu.VMEM((1, width), F32),
            wide, narrow, narrow, narrow, wide, wide,
            pltpu.VMEM((cores, max(blocks - 1, 1), members, breadth, LANES), BF16),
            pltpu.VMEM((blocks, 1, width), F32),
            pltpu.VMEM((blocks, 1, width), F32),
            pltpu.VMEM((cores, members, boxed, LANES), BF16),
            pltpu.VMEM((cores, members, boxed, LANES), BF16),
            pltpu.VMEM((cores, members, breadth, LANES), F32),
            pltpu.VMEM((cores, members, 1, LANES), F32),
            pltpu.VMEM((cores, boxed, LANES), BF16),
            pltpu.VMEM((cores, groups, boxed, LANES), BF16),
            pltpu.VMEM((cores, members, breadth, LANES), BF16),
            pltpu.VMEM((cores, members, breadth, LANES), BF16),
            narrow,
            pltpu.VMEM((tokens, depth), F32),
            dma((cores + 1,)), dma((2,)), dma((2,)), dma((2,)),
            dma((max(chunks - LEAD, 0) + 1,)), dma((1,)),
            dma((cores,)), dma((cores,)), dma((cores, groups)), dma((cores, groups)),
            dma((cores,)), dma((cores,)), pltpu.SemaphoreType.REGULAR,
        ],
        compiler_params=pltpu.CompilerParams(
            collective_id=0, has_side_effects=True, vmem_limit_bytes=52 * 2**20
        ),
    )(rec, key, val, fade, gate, reward, gain.reshape(1, -1), mapping)


def solution(mesh):
    tokens = P(("seq", "head"), None)
    placed = (tokens,) * 5 + (P("head", None), P("head"), P("head", None))
    return jax.shard_map(
        functools.partial(shards, mesh.shape["seq"], mesh.shape["head"]),
        mesh=mesh, in_specs=placed, out_specs=tokens, check_vma=False,
    )
```

```python
import functools

import jax
import jax.numpy as jnp
from jax import lax
from jax.experimental import pallas as pl
from jax.experimental.pallas import tpu as pltpu
from jax.sharding import PartitionSpec as P

BLOCK = 128
LANES = 128
QUAD = 256
CHUNK = 512
LEAD = 4
EXTRA = 8
EPS = 1e-05
MESH = pl.DeviceIdType.MESH
F32 = jnp.float32
BF16 = jnp.bfloat16


def dot(a, b):
    return jnp.dot(a, b, preferred_element_type=F32)


def dot_nt(a, b):
    return lax.dot_general(a, b, (((1,), (1,)), ((), ())), preferred_element_type=F32)


def dot_tn(a, b):
    return lax.dot_general(a, b, (((0,), (0,)), ((), ())), preferred_element_type=F32)


def split_heads(x, low):
    zero = jnp.zeros_like(x)
    return jnp.concatenate([jnp.where(low, x, zero), jnp.where(low, zero, x)], axis=0)


def flip(r, i, members):
    q, bit = 0, 1
    while bit < members:
        q = q + bit * (((r // bit) % 2 + (i // bit) % 2) % 2)
        bit *= 2
    return q


def kernel(
    n, cores, breadth,
    rec_hbm, key_hbm, val_hbm, fade_hbm, gate_hbm, reward_hbm, gain_hbm, map_hbm,
    out_ref,
    held, rewards, gains, weight,
    reward_row, cumx, key_mid, centred, recs, local_out, swish, entering, pref_row, mid_row,
    outbox, inbox, before, before_dec, gout, gin, cbox, carry, gated, partial,
    in_sem, p_local, p_send, p_recv, w_sem, w_send,
    s_send, s_recv, g_send, g_recv, c_send, c_recv, ready,
):
    me, core = lax.axis_index("seq"), lax.axis_index("head")
    other = 1 - core
    tokens, width = held.shape[1:]
    half = width // cores
    blocks, quads = tokens // BLOCK, half // QUAD
    chunks = weight.shape[1]
    lead = min(LEAD, chunks)
    members = half // LANES
    span = members // cores
    groups = n // span
    group = me // span
    r = (me % span) * cores + core
    peers = [flip(r, i, members) for i in range(members - 1, 0, -1)]
    fade, key, val, rec, gate = (held.at[i] for i in range(5))
    sources = (fade_hbm, key_hbm, val_hbm, rec_hbm, gate_hbm)

    def place(q):
        return (group * span + q // cores, q % cores)

    def above(g):
        return (g * span + me % span, core)

    barrier = pltpu.get_barrier_semaphore()
    for q in peers:
        pl.semaphore_signal(barrier, inc=1, device_id=place(q), device_id_type=MESH)

    for p in range(cores):
        for i in (0, 2, 1):
            at = pl.ds(p * half, half)
            sem = in_sem.at[i if p == 0 else p + 2]
            pltpu.make_async_copy(sources[i].at[:, at], held.at[i, :, at], sem).start()

    def greet_above(g, c):
        pl.semaphore_signal(barrier, inc=1, device_id=above(g), device_id_type=MESH)
        return c

    lax.fori_loop(group + 1, groups, greet_above, 0)
    for i in range(3, 5):
        pltpu.make_async_copy(sources[i], held.at[i], in_sem.at[cores + 2]).start()

    def wait_all(ref, sem):
        pltpu.make_async_copy(ref, ref, sem).wait()

    small = ((reward_hbm, rewards), (gain_hbm, gains))
    small_local = [
        pltpu.make_async_copy(src, dst.at[core], p_local.at[i]) for i, (src, dst) in enumerate(small)
    ]

    def small_copy(i, side):
        src, dst = small[i]
        return pltpu.make_async_remote_copy(
            src_ref=src, dst_ref=dst.at[side], send_sem=p_send.at[i], recv_sem=p_recv.at[i],
            device_id=(me, other), device_id_type=MESH,
        )

    for copy in small_local:
        copy.start()

    def columns(k):
        return map_hbm.at[:, pl.ds(k * CHUNK, CHUNK)]

    def weight_sem(k):
        return w_sem.at[max(k - lead + 1, 0)]

    def send_weight(start, stop=2 * chunks):
        for piece in range(start, min(stop, 2 * chunks)):
            k, rows = piece // 2, pl.ds(piece % 2 * (half // 2), half // 2)
            pltpu.make_async_remote_copy(
                src_ref=map_hbm.at[rows, pl.ds(k * CHUNK, CHUNK)], dst_ref=weight.at[core, k, rows],
                send_sem=w_send.at[0], recv_sem=weight_sem(k),
                device_id=(me, other), device_id_type=MESH,
            ).start()

    t_id = lax.broadcasted_iota(jnp.int32, (BLOCK, 2 * BLOCK), 0)
    s_id = lax.rem(lax.broadcasted_iota(jnp.int32, (BLOCK, 2 * BLOCK), 1), BLOCK)
    incl = jnp.where(t_id >= s_id, 1.0, 0.0).astype(BF16)
    low = lax.broadcasted_iota(jnp.int32, (BLOCK, LANES), 1) < breadth
    low_s = lax.broadcasted_iota(jnp.int32, (breadth, LANES), 1) < breadth
    row_x = lax.broadcasted_iota(jnp.int32, (EXTRA, LANES), 0)
    head_i = lax.broadcasted_iota(jnp.int32, (QUAD, QUAD), 0)
    head_j = lax.broadcasted_iota(jnp.int32, (QUAD, QUAD), 1)
    same, equal = head_i // breadth == head_j // breadth, head_i == head_j
    means = jnp.where(same, 1.0 / breadth, 0.0).astype(BF16)
    centre = (jnp.where(equal, 1.0, 0.0) - jnp.where(same, 1.0 / breadth, 0.0)).astype(BF16)
    ones = jnp.where(same, 1.0, 0.0).astype(BF16)
    state_rows, decay_rows = pl.ds(0, breadth), pl.ds(breadth, EXTRA)
    cuts = [slice(j * LANES, (j + 1) * LANES) for j in range(2)]

    def pack_rows(dec):
        hi = dec.astype(BF16).astype(F32)
        return jnp.where(row_x == 0, hi, jnp.where(row_x == 1, dec - hi, 0.0)).astype(BF16)

    def unpack_rows(x):
        x = x.astype(F32)
        return x[0:1] + x[1:2]

    def quad_lanes(p, t):
        return pl.ds(p * half + t * QUAD, QUAD)

    def arrive(p, i):
        if p == 0:
            wait_all(held.at[i, :, pl.ds(0, half)], in_sem.at[i])

    def decays(p):
        cells = [(t, b) for t in range(quads) for b in range(blocks)]
        cums, vbs, kms, products = {}, {}, {}, {}
        arrive(p, 0)
        for t, b in cells:
            at, lanes = pl.ds(b * BLOCK, BLOCK), quad_lanes(p, t)
            log_decay = -jnp.exp(fade[at, lanes].astype(F32))
            hi = log_decay.astype(BF16)
            lo = (log_decay - hi.astype(F32)).astype(BF16)
            cum = dot(incl, jnp.concatenate([hi, lo], axis=0))
            cumx[at, lanes] = cum - log_decay
            cums[t, b] = cum
        arrive(p, 2)
        for t, b in cells:
            at, lanes = pl.ds(b * BLOCK, BLOCK), quad_lanes(p, t)
            vbs[t, b] = dot(val[at, lanes], centre).astype(BF16)
            centred[at, lanes] = vbs[t, b]
        arrive(p, 1)
        for t, b in cells:
            at, lanes = pl.ds(b * BLOCK, BLOCK), quad_lanes(p, t)
            mid = cums[t, b][BLOCK // 2 - 1 : BLOCK // 2]
            kms[t, b] = (key[at, lanes].astype(F32) * jnp.exp(mid - cums[t, b])).astype(BF16)
            key_mid[at, lanes] = kms[t, b]
            mid_row[b, :, lanes] = mid
        for t, b in cells:
            for j, cut in enumerate(cuts):
                products[t, b, j] = dot_tn(vbs[t, b][:, cut], kms[t, b][:, cut])
        for t in range(quads):
            lanes = quad_lanes(p, t)
            states = [jnp.zeros((breadth, LANES), F32) for _ in range(2)]
            pref = jnp.zeros((1, QUAD), F32)
            for b in range(blocks):
                cum = cums[t, b]
                mid, total = cum[BLOCK // 2 - 1 : BLOCK // 2], cum[BLOCK - 1 :]
                end, whole, begin = jnp.exp(total - mid), jnp.exp(total), jnp.exp(mid)
                pref_row[b, :, lanes] = pref
                for j, cut in enumerate(cuts):
                    if b > 0:
                        entering[p, b - 1, 2 * t + j] = (states[j] * begin[:, cut]).astype(BF16)
                    product = products[t, b, j]
                    own = jnp.where(low_s, product[:breadth], product[breadth:])
                    states[j] = states[j] * whole[:, cut] + own * end[:, cut]
                pref = pref + total
            gone = jnp.exp(pref)
            for j, cut in enumerate(cuts):
                outbox[p, 2 * t + j, state_rows, :] = states[j].astype(BF16)
                outbox[p, 2 * t + j, decay_rows, :] = pack_rows(gone[:, cut])

    def within(units):
        cells = [(p, t, b) for p, t in units for b in range(blocks)]
        rms, diags, scored = {}, {}, {}
        for p, t, b in cells:
            at, lanes = pl.ds(b * BLOCK, BLOCK), quad_lanes(p, t)
            cx = cumx[at, lanes]
            rf = rec[at, lanes].astype(F32)
            rms[p, t, b] = (rf * jnp.exp(cx - mid_row[b, :, lanes])).astype(BF16)
            recs[at, lanes] = (rf * jnp.exp(cx + pref_row[b, :, lanes])).astype(BF16)
            own = rf * key[at, lanes].astype(F32) * reward_row[:, lanes]
            diags[p, t, b] = dot(own.astype(BF16), ones)
            kb = key_mid[at, lanes]
            for j, cut in enumerate(cuts):
                scored[p, t, b, j] = dot_nt(rms[p, t, b][:, cut], split_heads(kb[:, cut], low))
        for p, t, b in cells:
            at, lanes = pl.ds(b * BLOCK, BLOCK), quad_lanes(p, t)
            g = gate[at, lanes].astype(F32)
            swish[at, lanes] = g / (1.0 + jnp.exp(-g)) * gains[p, :, pl.ds(t * QUAD, QUAD)]
        for p, t, b in cells:
            at, lanes = pl.ds(b * BLOCK, BLOCK), quad_lanes(p, t)
            vb = centred[at, lanes]
            for j, cut in enumerate(cuts):
                scores = jnp.where(t_id > s_id, scored[p, t, b, j], 0.0).astype(BF16)
                o = dot(scores, split_heads(vb[:, cut], low))
                if b > 0:
                    came = split_heads(entering[p, b - 1, 2 * t + j], low_s)
                    o = o + dot_nt(rms[p, t, b][:, cut], came)
                o = o + diags[p, t, b][:, cut] * vb[:, cut].astype(F32)
                local_out[at, pl.ds(p * half + t * QUAD + j * LANES, LANES)] = o

    def finish(p, between=()):
        cells = [(t, b) for t in range(quads) for b in range(blocks)]
        states, outs, variances = [], {}, {}
        for t in range(quads):
            x, y = (split_heads(carry[p, 2 * t + j], low_s) for j in range(2))
            none = jnp.zeros_like(x)
            states.append(jnp.concatenate(
                [jnp.concatenate([x, none], axis=1), jnp.concatenate([none, y], axis=1)], axis=0
            ))
        for t, b in cells:
            at, lanes = pl.ds(b * BLOCK, BLOCK), quad_lanes(p, t)
            outs[t, b] = local_out[at, lanes] + dot_nt(recs[at, lanes], states[t])
        for t, b in cells:
            variances[t, b] = dot((outs[t, b] * outs[t, b]).astype(BF16), means)
        for k in between:
            project(k, 0, p)
        for t, b in cells:
            at, lanes = pl.ds(b * BLOCK, BLOCK), quad_lanes(p, t)
            scale = lax.rsqrt(variances[t, b] + EPS) * swish[at, lanes]
            gated[at, lanes] = (outs[t, b] * scale).astype(BF16)

    def member_copy(src, dst, p, j, send, recv):
        return pltpu.make_async_remote_copy(
            src_ref=src.at[p, j], dst_ref=dst.at[p, r], send_sem=send.at[p], recv_sem=recv.at[p],
            device_id=place(j), device_id_type=MESH,
        )

    def send_states(p):
        for q in peers:
            member_copy(outbox, inbox, p, q, s_send, s_recv).start()
        inbox[p, r] = outbox[p, r]

    some = pl.ds(0, members - 1)

    def advance(box, state):
        s, d = state
        e = unpack_rows(box[decay_rows, :])
        return s * e + box[state_rows, :].astype(F32), d * e

    nothing = (jnp.zeros((breadth, LANES), F32), jnp.ones((1, LANES), F32))

    def scan(p):
        state = nothing
        for j in range(members):
            before[p, j] = state[0]
            before_dec[p, j] = state[1]
            state = advance(inbox.at[p, j], state)
        gout[p, state_rows, :] = state[0].astype(BF16)
        gout[p, decay_rows, :] = pack_rows(state[1])

    def group_copy(p, g, slot):
        return pltpu.make_async_remote_copy(
            src_ref=gout.at[p], dst_ref=gin.at[p, slot],
            send_sem=g_send.at[p, g], recv_sem=g_recv.at[p, slot],
            device_id=above(g), device_id_type=MESH,
        )

    def send_group(p):
        def body(i, c):
            group_copy(p, groups - 1 - i, group).start()
            return c

        lax.fori_loop(0, groups - 1 - group, body, 0)

    def take_group(p):
        def body(g, state):
            group_copy(p, g, g).wait_recv()
            return advance(gin.at[p, g], state)

        return lax.fori_loop(0, group, body, nothing)[0]

    def send_carry(p, came):
        for j in range(members):
            cbox[p, j] = (came * before_dec[p, j] + before[p, j]).astype(BF16)
        for q in peers:
            member_copy(cbox, carry, p, q, c_send, c_recv).start()
        carry[p, r] = cbox[p, r]

    with jax.named_scope("decays0"):
        decays(0)
    with jax.named_scope("barrier"):
        pl.semaphore_wait(barrier, members - 1 + group)
        send_states(0)
        for i in range(2):
            small_copy(i, core).start()

        def here(g, c):
            pl.semaphore_signal(ready, inc=1, device_id=above(g), device_id_type=MESH)
            return c

        lax.fori_loop(0, group, here, 0)
        for k in range(chunks):
            pltpu.make_async_copy(columns(k), weight.at[core, k], weight_sem(k)).start()
    for p in range(1, cores):
        with jax.named_scope("in1"):
            wait_all(held.at[pl.ds(0, 3), :, pl.ds(p * half, half)], in_sem.at[p + 2])
        with jax.named_scope("decays1"):
            decays(p)
        with jax.named_scope("send1"):
            send_states(p)
    send_weight(0, 4)

    @pl.when(group == 0)
    def _():
        send_weight(4, 5)

    with jax.named_scope("in2"):
        wait_all(held.at[pl.ds(3, 2)], in_sem.at[cores + 2])
        for i in range(2):
            small_local[i].wait()
            small_copy(i, other).wait_recv()
        for h in range(width // breadth):
            reward_row[:, pl.ds(h * breadth, breadth)] = rewards[
                h * breadth // half, pl.ds(h % (half // breadth), 1), :
            ]

    units = [(p, t) for p in range(cores) for t in range(quads)]
    done = 0

    def some_within(count):
        nonlocal done
        for at in range(done, min(done + count, len(units)), 2):
            with jax.named_scope("within"):
                within(units[at : at + 2])
        done += count

    some_within(4)
    for p in range(cores):
        with jax.named_scope("wait_states"):
            wait_all(inbox.at[p, some], s_recv.at[p])
        with jax.named_scope("scan"):
            scan(p)
        with jax.named_scope("send_group"):
            if p == 0:
                @pl.when(group < groups - 1)
                def _():
                    pl.semaphore_wait(ready, groups - 1 - group)

            send_group(p)

            @pl.when(group == 0)
            def _():
                send_carry(p, nothing[0])
                if p < cores - 1:
                    send_weight(5 + 2 * p, 7 + 2 * p)
                else:
                    send_weight(3 + 2 * cores)

            @pl.when(group > 0)
            def _():
                send_weight(4 + 2 * p, 6 + 2 * p)

        some_within(2 if p < cores - 1 else len(units))
    with jax.named_scope("take_group"):
        @pl.when(group > 0)
        def _():
            for p in range(cores):
                send_carry(p, take_group(p))
            send_weight(4 + 2 * cores)

    def project(k, first, last):
        at = pl.ds(k * CHUNK, CHUNK)
        total = partial[:, at] if first > 0 else None
        for p in range(first, last):
            term = dot(gated[:, pl.ds(p * half, half)], weight[p, k])
            total = term if total is None else total + term
        if last < cores:
            partial[:, at] = total
        else:
            out_ref[:, at] = total.astype(BF16)

    for p in range(cores - 1):
        with jax.named_scope("wait_carry"):
            wait_all(carry.at[p, some], c_recv.at[p])
        with jax.named_scope("finish"):
            finish(p)
    with jax.named_scope("wait_weight"):
        wait_all(weight.at[:, pl.ds(0, lead)], w_sem.at[0])
    with jax.named_scope("project_lead"):
        for k in range(lead - 2):
            project(k, 0, cores - 1)
    with jax.named_scope("wait_carry"):
        wait_all(carry.at[cores - 1, some], c_recv.at[cores - 1])
    with jax.named_scope("finish"):
        finish(cores - 1, range(lead - 2, lead))
    with jax.named_scope("project_led"):
        for k in range(lead):
            project(k, cores - 1, cores)
    with jax.named_scope("wait_weight"):
        for k in range(lead, chunks):
            wait_all(weight.at[:, k], weight_sem(k))
    with jax.named_scope("project_rest"):
        for k in range(lead, chunks):
            project(k, 0, cores)

    def drain_groups(g, c):
        for p in range(cores):
            group_copy(p, g, group).wait_send()
        return c

    with jax.named_scope("drain"):
        lax.fori_loop(group + 1, groups, drain_groups, 0)
        for p in range(cores):
            wait_all(outbox.at[p, some], s_send.at[p])
            wait_all(cbox.at[p, some], c_send.at[p])
        wait_all(weight.at[other], w_send.at[0])
        for i in range(2):
            small_copy(i, core).wait_send()


def shards(n, cores, rec, key, val, fade, gate, reward, gain, mapping):
    tokens, width = rec.shape
    breadth = reward.shape[1]
    half, depth = mapping.shape
    blocks, chunks, members = tokens // BLOCK, depth // CHUNK, half // LANES
    groups = n * cores // members
    boxed = breadth + EXTRA
    dma = pltpu.SemaphoreType.DMA
    narrow = pltpu.VMEM((tokens, width), BF16)
    wide = pltpu.VMEM((tokens, width), F32)
    return pl.pallas_call(
        functools.partial(kernel, n, cores, breadth),
        out_shape=pltpu.VMEM((tokens, depth), BF16),
        in_specs=[pl.BlockSpec(memory_space=pl.ANY)] * 8,
        out_specs=pl.BlockSpec(memory_space=pltpu.VMEM),
        scratch_shapes=[
            pltpu.VMEM((5, tokens, width), BF16),
            pltpu.VMEM((cores,) + reward.shape, F32),
            pltpu.VMEM((cores, 1, half), F32),
            pltpu.VMEM((cores, chunks, half, CHUNK), BF16),
            pltpu.VMEM((1, width), F32),
            wide, narrow, narrow, narrow, wide, wide,
            pltpu.VMEM((cores, max(blocks - 1, 1), members, breadth, LANES), BF16),
            pltpu.VMEM((blocks, 1, width), F32),
            pltpu.VMEM((blocks, 1, width), F32),
            pltpu.VMEM((cores, members, boxed, LANES), BF16),
            pltpu.VMEM((cores, members, boxed, LANES), BF16),
            pltpu.VMEM((cores, members, breadth, LANES), F32),
            pltpu.VMEM((cores, members, 1, LANES), F32),
            pltpu.VMEM((cores, boxed, LANES), BF16),
            pltpu.VMEM((cores, groups, boxed, LANES), BF16),
            pltpu.VMEM((cores, members, breadth, LANES), BF16),
            pltpu.VMEM((cores, members, breadth, LANES), BF16),
            narrow,
            pltpu.VMEM((tokens, depth), F32),
            dma((cores + 3,)), dma((2,)), dma((2,)), dma((2,)),
            dma((max(chunks - LEAD, 0) + 1,)), dma((1,)),
            dma((cores,)), dma((cores,)), dma((cores, groups)), dma((cores, groups)),
            dma((cores,)), dma((cores,)), pltpu.SemaphoreType.REGULAR,
        ],
        compiler_params=pltpu.CompilerParams(
            collective_id=0, has_side_effects=True, vmem_limit_bytes=52 * 2**20
        ),
    )(rec, key, val, fade, gate, reward, gain.reshape(1, -1), mapping)


def solution(mesh):
    tokens = P(("seq", "head"), None)
    placed = (tokens,) * 5 + (P("head", None), P("head"), P("head", None))
    return jax.shard_map(
        functools.partial(shards, mesh.shape["seq"], mesh.shape["head"]),
        mesh=mesh, in_specs=placed, out_specs=tokens, check_vma=False,
    )
```

```python
import functools

import jax
import jax.numpy as jnp
from jax import lax
from jax.experimental import pallas as pl
from jax.experimental.pallas import tpu as pltpu
from jax.sharding import PartitionSpec as P

BLOCK = 128
LANES = 128
QUAD = 256
CHUNK = 512
LEAD = 4
WAYS = 2
EXTRA = 8
EPS = 1e-05
MESH = pl.DeviceIdType.MESH
F32 = jnp.float32
BF16 = jnp.bfloat16


def dot(a, b):
    return jnp.dot(a, b, preferred_element_type=F32)


def dot_nt(a, b):
    return lax.dot_general(a, b, (((1,), (1,)), ((), ())), preferred_element_type=F32)


def dot_tn(a, b):
    return lax.dot_general(a, b, (((0,), (0,)), ((), ())), preferred_element_type=F32)


def split_heads(x, low):
    zero = jnp.zeros_like(x)
    return jnp.concatenate([jnp.where(low, x, zero), jnp.where(low, zero, x)], axis=0)


def flip(r, i, members):
    q, bit = 0, 1
    while bit < members:
        q = q + bit * (((r // bit) % 2 + (i // bit) % 2) % 2)
        bit *= 2
    return q


def kernel(
    n, cores, breadth,
    rec_hbm, key_hbm, val_hbm, fade_hbm, gate_hbm, reward_hbm, gain_hbm, map_hbm,
    out_ref,
    held, rewards, gains, weight,
    reward_row, cumx, key_mid, centred, recs, local_out, swish, entering, pref_row, mid_row,
    outbox, inbox, before, before_dec, gout, gin, cbox, carry, gated, partial,
    in_sem, p_local, p_send, p_recv, w_sem, w_send,
    s_send, s_recv, g_send, g_recv, c_send, c_recv, ready,
):
    me, core = lax.axis_index("seq"), lax.axis_index("head")
    other = 1 - core
    tokens, width = held.shape[1:]
    half = width // cores
    parts, span = outbox.shape[:2]
    ways = parts // cores
    lane = width // parts
    blocks, quads = tokens // BLOCK, lane // QUAD
    chunks = weight.shape[1]
    lead = min(LEAD, chunks)
    members = span * cores
    groups = n // span
    group = me // span
    chip = me % span
    r = chip * cores + core
    peers = [flip(r, i, members) for i in range(members - 1, 0, -1)]
    chips = [flip(chip, i, span) for i in range(span - 1, -1, -1)]
    fade, key, val, rec, gate = (held.at[i] for i in range(5))
    sources = (fade_hbm, key_hbm, val_hbm, rec_hbm, gate_hbm)

    def place(q):
        return (group * span + q // cores, q % cores)

    def above(g):
        return (g * span + me % span, core)

    barrier = pltpu.get_barrier_semaphore()
    for q in peers:
        pl.semaphore_signal(barrier, inc=1, device_id=place(q), device_id_type=MESH)

    for p in range(cores):
        for i in (0, 2, 1):
            at = pl.ds(p * half, half)
            sem = in_sem.at[i if p == 0 else p + 2]
            pltpu.make_async_copy(sources[i].at[:, at], held.at[i, :, at], sem).start()

    def greet_above(g, c):
        pl.semaphore_signal(barrier, inc=1, device_id=above(g), device_id_type=MESH)
        return c

    lax.fori_loop(group + 1, groups, greet_above, 0)
    for i in range(3, 5):
        pltpu.make_async_copy(sources[i], held.at[i], in_sem.at[cores + 2]).start()

    def wait_all(ref, sem):
        pltpu.make_async_copy(ref, ref, sem).wait()

    small = ((reward_hbm, rewards), (gain_hbm, gains))
    small_local = [
        pltpu.make_async_copy(src, dst.at[core], p_local.at[i]) for i, (src, dst) in enumerate(small)
    ]

    def small_copy(i, side):
        src, dst = small[i]
        return pltpu.make_async_remote_copy(
            src_ref=src, dst_ref=dst.at[side], send_sem=p_send.at[i], recv_sem=p_recv.at[i],
            device_id=(me, other), device_id_type=MESH,
        )

    for copy in small_local:
        copy.start()

    def columns(k):
        return map_hbm.at[:, pl.ds(k * CHUNK, CHUNK)]

    def weight_sem(k):
        return w_sem.at[max(k - lead + 1, 0)]

    def send_weight(start, stop=2 * chunks):
        for piece in range(start, min(stop, 2 * chunks)):
            k, rows = piece // 2, pl.ds(piece % 2 * (half // 2), half // 2)
            pltpu.make_async_remote_copy(
                src_ref=map_hbm.at[rows, pl.ds(k * CHUNK, CHUNK)], dst_ref=weight.at[core, k, rows],
                send_sem=w_send.at[0], recv_sem=weight_sem(k),
                device_id=(me, other), device_id_type=MESH,
            ).start()

    t_id = lax.broadcasted_iota(jnp.int32, (BLOCK, 2 * BLOCK), 0)
    s_id = lax.rem(lax.broadcasted_iota(jnp.int32, (BLOCK, 2 * BLOCK), 1), BLOCK)
    incl = jnp.where(t_id >= s_id, 1.0, 0.0).astype(BF16)
    low = lax.broadcasted_iota(jnp.int32, (BLOCK, LANES), 1) < breadth
    low_s = lax.broadcasted_iota(jnp.int32, (breadth, LANES), 1) < breadth
    row_x = lax.broadcasted_iota(jnp.int32, (EXTRA, LANES), 0)
    head_i = lax.broadcasted_iota(jnp.int32, (QUAD, QUAD), 0)
    head_j = lax.broadcasted_iota(jnp.int32, (QUAD, QUAD), 1)
    same, equal = head_i // breadth == head_j // breadth, head_i == head_j
    means = jnp.where(same, 1.0 / breadth, 0.0).astype(BF16)
    centre = (jnp.where(equal, 1.0, 0.0) - jnp.where(same, 1.0 / breadth, 0.0)).astype(BF16)
    ones = jnp.where(same, 1.0, 0.0).astype(BF16)
    state_rows, decay_rows = pl.ds(0, breadth), pl.ds(breadth, EXTRA)
    cuts = [slice(j * LANES, (j + 1) * LANES) for j in range(2)]

    def pack_rows(dec):
        hi = dec.astype(BF16).astype(F32)
        return jnp.where(row_x == 0, hi, jnp.where(row_x == 1, dec - hi, 0.0)).astype(BF16)

    def unpack_rows(x):
        x = x.astype(F32)
        return x[0:1] + x[1:2]

    def quad_lanes(p, t):
        return pl.ds(p * lane + t * QUAD, QUAD)

    def arrive(p, i):
        if p == 0:
            wait_all(held.at[i, :, pl.ds(0, half)], in_sem.at[i])

    def decays(p):
        cells = [(t, b) for t in range(quads) for b in range(blocks)]
        cums, vbs, kms, products = {}, {}, {}, {}
        arrive(p, 0)
        for t, b in cells:
            at, lanes = pl.ds(b * BLOCK, BLOCK), quad_lanes(p, t)
            log_decay = -jnp.exp(fade[at, lanes].astype(F32))
            hi = log_decay.astype(BF16)
            lo = (log_decay - hi.astype(F32)).astype(BF16)
            cum = dot(incl, jnp.concatenate([hi, lo], axis=0))
            cumx[at, lanes] = cum - log_decay
            cums[t, b] = cum
        arrive(p, 2)
        for t, b in cells:
            at, lanes = pl.ds(b * BLOCK, BLOCK), quad_lanes(p, t)
            vbs[t, b] = dot(val[at, lanes], centre).astype(BF16)
            centred[at, lanes] = vbs[t, b]
        arrive(p, 1)
        for t, b in cells:
            at, lanes = pl.ds(b * BLOCK, BLOCK), quad_lanes(p, t)
            mid = cums[t, b][BLOCK // 2 - 1 : BLOCK // 2]
            kms[t, b] = (key[at, lanes].astype(F32) * jnp.exp(mid - cums[t, b])).astype(BF16)
            key_mid[at, lanes] = kms[t, b]
            mid_row[b, :, lanes] = mid
        for t, b in cells:
            for j, cut in enumerate(cuts):
                products[t, b, j] = dot_tn(vbs[t, b][:, cut], kms[t, b][:, cut])
        for t in range(quads):
            lanes = quad_lanes(p, t)
            states = [jnp.zeros((breadth, LANES), F32) for _ in range(2)]
            pref = jnp.zeros((1, QUAD), F32)
            for b in range(blocks):
                cum = cums[t, b]
                mid, total = cum[BLOCK // 2 - 1 : BLOCK // 2], cum[BLOCK - 1 :]
                end, whole, begin = jnp.exp(total - mid), jnp.exp(total), jnp.exp(mid)
                pref_row[b, :, lanes] = pref
                for j, cut in enumerate(cuts):
                    if b > 0:
                        entering[p, b - 1, 2 * t + j] = (states[j] * begin[:, cut]).astype(BF16)
                    product = products[t, b, j]
                    own = jnp.where(low_s, product[:breadth], product[breadth:])
                    states[j] = states[j] * whole[:, cut] + own * end[:, cut]
                pref = pref + total
            gone = jnp.exp(pref)
            for j, cut in enumerate(cuts):
                outbox[p, 2 * t + j, state_rows, :] = states[j].astype(BF16)
                outbox[p, 2 * t + j, decay_rows, :] = pack_rows(gone[:, cut])

    def within(units):
        cells = [(p, t, b) for p, t in units for b in range(blocks)]
        rms, diags, scored = {}, {}, {}
        for p, t, b in cells:
            at, lanes = pl.ds(b * BLOCK, BLOCK), quad_lanes(p, t)
            cx = cumx[at, lanes]
            rf = rec[at, lanes].astype(F32)
            rms[p, t, b] = (rf * jnp.exp(cx - mid_row[b, :, lanes])).astype(BF16)
            recs[at, lanes] = (rf * jnp.exp(cx + pref_row[b, :, lanes])).astype(BF16)
            own = rf * key[at, lanes].astype(F32) * reward_row[:, lanes]
            diags[p, t, b] = dot(own.astype(BF16), ones)
            kb = key_mid[at, lanes]
            for j, cut in enumerate(cuts):
                scored[p, t, b, j] = dot_nt(rms[p, t, b][:, cut], split_heads(kb[:, cut], low))
        for p, t, b in cells:
            at, lanes = pl.ds(b * BLOCK, BLOCK), quad_lanes(p, t)
            g = gate[at, lanes].astype(F32)
            swish[at, lanes] = g / (1.0 + jnp.exp(-g)) * gains[p * lane // half, :, pl.ds(p * lane % half + t * QUAD, QUAD)]
        for p, t, b in cells:
            at, lanes = pl.ds(b * BLOCK, BLOCK), quad_lanes(p, t)
            vb = centred[at, lanes]
            for j, cut in enumerate(cuts):
                scores = jnp.where(t_id > s_id, scored[p, t, b, j], 0.0).astype(BF16)
                o = dot(scores, split_heads(vb[:, cut], low))
                if b > 0:
                    came = split_heads(entering[p, b - 1, 2 * t + j], low_s)
                    o = o + dot_nt(rms[p, t, b][:, cut], came)
                o = o + diags[p, t, b][:, cut] * vb[:, cut].astype(F32)
                local_out[at, pl.ds(p * lane + t * QUAD + j * LANES, LANES)] = o

    def finish(ps, between=()):
        cells = [(p, t, b) for p in ps for t in range(quads) for b in range(blocks)]
        states, outs, variances = {}, {}, {}
        for p in ps:
            for t in range(quads):
                x, y = (split_heads(carry[p, 2 * t + j], low_s) for j in range(2))
                none = jnp.zeros_like(x)
                states[p, t] = jnp.concatenate(
                    [jnp.concatenate([x, none], axis=1), jnp.concatenate([none, y], axis=1)], axis=0
                )
        for p, t, b in cells:
            at, lanes = pl.ds(b * BLOCK, BLOCK), quad_lanes(p, t)
            outs[p, t, b] = local_out[at, lanes] + dot_nt(recs[at, lanes], states[p, t])
        for p, t, b in cells:
            out = outs[p, t, b]
            variances[p, t, b] = dot((out * out).astype(BF16), means)
        for k in between:
            project(k, 0, cores - 1)
        for p, t, b in cells:
            at, lanes = pl.ds(b * BLOCK, BLOCK), quad_lanes(p, t)
            scale = lax.rsqrt(variances[p, t, b] + EPS) * swish[at, lanes]
            gated[at, lanes] = (outs[p, t, b] * scale).astype(BF16)

    def send_states(p):
        way, owner = p // cores, p % cores
        for t in chips[:-1]:
            pltpu.make_async_remote_copy(
                src_ref=outbox.at[p, t], dst_ref=inbox.at[way, r],
                send_sem=s_send.at[0], recv_sem=s_recv.at[way],
                device_id=(group * span + t, owner), device_id_type=MESH,
            ).start()

        @pl.when(core == owner)
        def _():
            inbox[way, r] = outbox[p, chip]

        @pl.when(core != owner)
        def _():
            pltpu.make_async_remote_copy(
                src_ref=outbox.at[p, chip], dst_ref=inbox.at[way, r],
                send_sem=s_send.at[0], recv_sem=s_recv.at[way],
                device_id=(me, owner), device_id_type=MESH,
            ).start()

    some = pl.ds(0, members - 1)

    def advance(box, state):
        s, d = state
        e = unpack_rows(box[decay_rows, :])
        return s * e + box[state_rows, :].astype(F32), d * e

    nothing = (jnp.zeros((breadth, LANES), F32), jnp.ones((1, LANES), F32))

    def scan(p):
        state = nothing
        for j in range(members):
            before[p, j] = state[0]
            before_dec[p, j] = state[1]
            state = advance(inbox.at[p, j], state)
        gout[p, state_rows, :] = state[0].astype(BF16)
        gout[p, decay_rows, :] = pack_rows(state[1])

    def group_copy(p, g, slot):
        return pltpu.make_async_remote_copy(
            src_ref=gout.at[p], dst_ref=gin.at[p, slot],
            send_sem=g_send.at[p, g], recv_sem=g_recv.at[p, slot],
            device_id=above(g), device_id_type=MESH,
        )

    def send_group(p):
        def body(i, c):
            group_copy(p, groups - 1 - i, group).start()
            return c

        lax.fori_loop(0, groups - 1 - group, body, 0)

    def take_group(p):
        def body(g, state):
            group_copy(p, g, g).wait_recv()
            return advance(gin.at[p, g], state)

        return lax.fori_loop(0, group, body, nothing)[0]

    def send_carry(way, came):
        p = way * cores + core
        for j in range(members):
            cbox[way, j] = (came * before_dec[way, j] + before[way, j]).astype(BF16)
        for q in peers:
            pltpu.make_async_remote_copy(
                src_ref=cbox.at[way, q], dst_ref=carry.at[p, chip],
                send_sem=c_send.at[0], recv_sem=c_recv.at[p],
                device_id=place(q), device_id_type=MESH,
            ).start()
        carry[p, chip] = cbox[way, r]

    def wait_carry(p):
        @pl.when(core == p % cores)
        def _():
            wait_all(carry.at[p, pl.ds(0, span - 1)], c_recv.at[p])

        @pl.when(core != p % cores)
        def _():
            wait_all(carry.at[p], c_recv.at[p])

    with jax.named_scope("decays0"):
        decays(0)
    with jax.named_scope("barrier"):
        pl.semaphore_wait(barrier, members - 1 + group)
        send_states(0)
        for i in range(2):
            small_copy(i, core).start()
        send_weight(0, 1)

        def here(g, c):
            pl.semaphore_signal(ready, inc=1, device_id=above(g), device_id_type=MESH)
            return c

        lax.fori_loop(0, group, here, 0)
        for k in range(chunks):
            pltpu.make_async_copy(columns(k), weight.at[core, k], weight_sem(k)).start()
    for p in range(1, parts):
        if p % ways == 0:
            with jax.named_scope("in1"):
                side = p // ways
                wait_all(held.at[pl.ds(0, 3), :, pl.ds(side * half, half)], in_sem.at[side + 2])
        with jax.named_scope("decays1"):
            decays(p)
        with jax.named_scope("send1"):
            send_states(p)
            send_weight(p, p + 1 if p < parts - 1 else p + 2)
    sent = parts + 1

    with jax.named_scope("in2"):
        wait_all(held.at[pl.ds(3, 2)], in_sem.at[cores + 2])
        for i in range(2):
            small_local[i].wait()
            small_copy(i, other).wait_recv()
        for h in range(width // breadth):
            reward_row[:, pl.ds(h * breadth, breadth)] = rewards[
                h * breadth // half, pl.ds(h % (half // breadth), 1), :
            ]

    units = [(p, t) for p in range(parts) for t in range(quads)]
    done = 0

    def some_within(count):
        nonlocal done
        for at in range(done, min(done + count, len(units)), 2):
            with jax.named_scope("within"):
                within(units[at : at + 2])
        done += count

    some_within(4)
    for p in range(ways):
        with jax.named_scope("wait_states"):
            wait_all(inbox.at[p, some], s_recv.at[p])
        with jax.named_scope("scan"):
            scan(p)
        with jax.named_scope("send_group"):
            if p == 0:
                @pl.when(group < groups - 1)
                def _():
                    pl.semaphore_wait(ready, groups - 1 - group)

            send_group(p)

            @pl.when(group == 0)
            def _():
                send_carry(p, nothing[0])
                send_weight(sent + 2 * p, sent + 2 * p + 2 if p < ways - 1 else 2 * chunks)

            @pl.when(group > 0)
            def _():
                send_weight(sent + 2 * p, sent + 2 * p + 2)

        some_within(2 if p < ways - 1 else len(units))
    with jax.named_scope("take_group"):
        @pl.when(group > 0)
        def _():
            for p in range(ways):
                at = sent + 2 * ways + p
                send_carry(p, take_group(p))
                send_weight(at, at + 1 if p < ways - 1 else 2 * chunks)

    def project(k, first, last):
        at = pl.ds(k * CHUNK, CHUNK)
        total = partial[:, at] if first > 0 else None
        for p in range(first, last):
            term = dot(gated[:, pl.ds(p * half, half)], weight[p, k])
            total = term if total is None else total + term
        if last < cores:
            partial[:, at] = total
        else:
            out_ref[:, at] = total.astype(BF16)

    early = parts - ways
    with jax.named_scope("wait_carry"):
        for p in range(early):
            wait_carry(p)
    with jax.named_scope("finish"):
        finish(range(early))
    with jax.named_scope("wait_weight"):
        wait_all(weight.at[:, pl.ds(0, lead)], w_sem.at[0])
    with jax.named_scope("project_lead"):
        for k in range(lead - 2):
            project(k, 0, cores - 1)
    with jax.named_scope("wait_carry"):
        for p in range(early, parts):
            wait_carry(p)
    with jax.named_scope("finish"):
        finish(range(early, parts), range(lead - 2, lead))
    with jax.named_scope("project_led"):
        for k in range(lead):
            project(k, cores - 1, cores)
    for at in range(lead, chunks, 2):
        pair = range(at, min(at + 2, chunks))
        with jax.named_scope("wait_weight"):
            for k in pair:
                wait_all(weight.at[:, k], weight_sem(k))
        with jax.named_scope("project_rest"):
            for k in pair:
                project(k, 0, cores)

    def drain_groups(g, c):
        for p in range(ways):
            group_copy(p, g, group).wait_send()
        return c

    with jax.named_scope("drain"):
        lax.fori_loop(group + 1, groups, drain_groups, 0)
        wait_all(inbox.at[:, some], s_send.at[0])
        wait_all(cbox.at[:, some], c_send.at[0])
        wait_all(weight.at[other], w_send.at[0])
        for i in range(2):
            small_copy(i, core).wait_send()


def shards(n, cores, rec, key, val, fade, gate, reward, gain, mapping):
    tokens, width = rec.shape
    breadth = reward.shape[1]
    half, depth = mapping.shape
    ways = WAYS
    parts = ways * cores
    blocks, chunks, span = tokens // BLOCK, depth // CHUNK, width // parts // LANES
    members, groups = span * cores, n // span
    boxed = breadth + EXTRA
    dma = pltpu.SemaphoreType.DMA
    narrow = pltpu.VMEM((tokens, width), BF16)
    wide = pltpu.VMEM((tokens, width), F32)
    return pl.pallas_call(
        functools.partial(kernel, n, cores, breadth),
        out_shape=pltpu.VMEM((tokens, depth), BF16),
        in_specs=[pl.BlockSpec(memory_space=pl.ANY)] * 8,
        out_specs=pl.BlockSpec(memory_space=pltpu.VMEM),
        scratch_shapes=[
            pltpu.VMEM((5, tokens, width), BF16),
            pltpu.VMEM((cores,) + reward.shape, F32),
            pltpu.VMEM((cores, 1, half), F32),
            pltpu.VMEM((cores, chunks, half, CHUNK), BF16),
            pltpu.VMEM((1, width), F32),
            wide, narrow, narrow, narrow, wide, wide,
            pltpu.VMEM((parts, max(blocks - 1, 1), span, breadth, LANES), BF16),
            pltpu.VMEM((blocks, 1, width), F32),
            pltpu.VMEM((blocks, 1, width), F32),
            pltpu.VMEM((parts, span, boxed, LANES), BF16),
            pltpu.VMEM((ways, members, boxed, LANES), BF16),
            pltpu.VMEM((ways, members, breadth, LANES), F32),
            pltpu.VMEM((ways, members, 1, LANES), F32),
            pltpu.VMEM((ways, boxed, LANES), BF16),
            pltpu.VMEM((ways, groups, boxed, LANES), BF16),
            pltpu.VMEM((ways, members, breadth, LANES), BF16),
            pltpu.VMEM((parts, span, breadth, LANES), BF16),
            narrow,
            pltpu.VMEM((tokens, depth), F32),
            dma((cores + 3,)), dma((2,)), dma((2,)), dma((2,)),
            dma((max(chunks - LEAD, 0) + 1,)), dma((1,)),
            dma((1,)), dma((ways,)), dma((ways, groups)), dma((ways, groups)),
            dma((1,)), dma((parts,)), pltpu.SemaphoreType.REGULAR,
        ],
        compiler_params=pltpu.CompilerParams(
            collective_id=0, has_side_effects=True, vmem_limit_bytes=52 * 2**20
        ),
    )(rec, key, val, fade, gate, reward, gain.reshape(1, -1), mapping)


def solution(mesh):
    tokens = P(("seq", "head"), None)
    placed = (tokens,) * 5 + (P("head", None), P("head"), P("head", None))
    return jax.shard_map(
        functools.partial(shards, mesh.shape["seq"], mesh.shape["head"]),
        mesh=mesh, in_specs=placed, out_specs=tokens, check_vma=False,
    )
```

```python
import functools

import jax
import jax.numpy as jnp
from jax import lax
from jax.experimental import pallas as pl
from jax.experimental.pallas import tpu as pltpu
from jax.sharding import PartitionSpec as P

BLOCK = 128
LANES = 128
QUAD = 256
CHUNK = 512
LEAD = 4
WAYS = 2
TAIL = 2
EXTRA = 8
EPS = 1e-05
MESH = pl.DeviceIdType.MESH
F32 = jnp.float32
BF16 = jnp.bfloat16


def dot(a, b):
    return jnp.dot(a, b, preferred_element_type=F32)


def dot_nt(a, b):
    return lax.dot_general(a, b, (((1,), (1,)), ((), ())), preferred_element_type=F32)


def dot_tn(a, b):
    return lax.dot_general(a, b, (((0,), (0,)), ((), ())), preferred_element_type=F32)


def split_heads(x, low):
    zero = jnp.zeros_like(x)
    return jnp.concatenate([jnp.where(low, x, zero), jnp.where(low, zero, x)], axis=0)


def flip(r, i, members):
    q, bit = 0, 1
    while bit < members:
        q = q + bit * (((r // bit) % 2 + (i // bit) % 2) % 2)
        bit *= 2
    return q


def kernel(
    n, cores, breadth,
    rec_hbm, key_hbm, val_hbm, fade_hbm, gate_hbm, reward_hbm, gain_hbm, map_hbm,
    out_ref, gated, weight_tail,
    held, rewards, gains, weight_head,
    reward_row, cumx, key_mid, centred, recs, local_out, swish, entering, pref_row, mid_row,
    outbox, inbox, before, before_dec, gout, gin, cbox, carry, partial,
    in_sem, p_local, p_send, p_recv, w_sem, w_send,
    s_send, s_recv, g_send, g_recv, c_send, c_recv, ready,
):
    me, core = lax.axis_index("seq"), lax.axis_index("head")
    other = 1 - core
    tokens, width = held.shape[1:]
    half = width // cores
    parts, span = outbox.shape[:2]
    ways = parts // cores
    lane = width // parts
    blocks, quads = tokens // BLOCK, lane // QUAD
    split = weight_head.shape[1]
    chunks = split + weight_tail.shape[1]
    lead = min(LEAD, chunks)
    members = span * cores
    groups = n // span
    group = me // span
    chip = me % span
    r = chip * cores + core
    peers = [flip(r, i, members) for i in range(members - 1, 0, -1)]
    chips = [flip(chip, i, span) for i in range(span - 1, -1, -1)]
    fade, key, val, rec, gate = (held.at[i] for i in range(5))
    sources = (fade_hbm, key_hbm, val_hbm, rec_hbm, gate_hbm)

    def place(q):
        return (group * span + q // cores, q % cores)

    def above(g):
        return (g * span + me % span, core)

    barrier = pltpu.get_barrier_semaphore()
    for q in peers:
        pl.semaphore_signal(barrier, inc=1, device_id=place(q), device_id_type=MESH)

    for p in range(cores):
        for i in (0, 2, 1):
            at = pl.ds(p * half, half)
            sem = in_sem.at[i if p == 0 else p + 2]
            pltpu.make_async_copy(sources[i].at[:, at], held.at[i, :, at], sem).start()

    def greet_above(g, c):
        pl.semaphore_signal(barrier, inc=1, device_id=above(g), device_id_type=MESH)
        return c

    lax.fori_loop(group + 1, groups, greet_above, 0)
    for i in range(3, 5):
        pltpu.make_async_copy(sources[i], held.at[i], in_sem.at[cores + 2]).start()

    def wait_all(ref, sem):
        pltpu.make_async_copy(ref, ref, sem).wait()

    small = ((reward_hbm, rewards), (gain_hbm, gains))
    small_local = [
        pltpu.make_async_copy(src, dst.at[core], p_local.at[i]) for i, (src, dst) in enumerate(small)
    ]

    def small_copy(i, side):
        src, dst = small[i]
        return pltpu.make_async_remote_copy(
            src_ref=src, dst_ref=dst.at[side], send_sem=p_send.at[i], recv_sem=p_recv.at[i],
            device_id=(me, other), device_id_type=MESH,
        )

    for copy in small_local:
        copy.start()

    def columns(k):
        return map_hbm.at[:, pl.ds(k * CHUNK, CHUNK)]

    def weight(side, k):
        return weight_head.at[side, k] if k < split else weight_tail.at[side, k - split]

    def weight_sem(k):
        return w_sem.at[max(k - lead + 1, 0)]

    def send_weight(start, stop=2 * chunks):
        for piece in range(start, min(stop, 2 * chunks)):
            k, rows = piece // 2, pl.ds(piece % 2 * (half // 2), half // 2)
            pltpu.make_async_remote_copy(
                src_ref=map_hbm.at[rows, pl.ds(k * CHUNK, CHUNK)], dst_ref=weight(core, k).at[rows],
                send_sem=w_send.at[0], recv_sem=weight_sem(k),
                device_id=(me, other), device_id_type=MESH,
            ).start()

    t_id = lax.broadcasted_iota(jnp.int32, (BLOCK, 2 * BLOCK), 0)
    s_id = lax.rem(lax.broadcasted_iota(jnp.int32, (BLOCK, 2 * BLOCK), 1), BLOCK)
    incl = jnp.where(t_id >= s_id, 1.0, 0.0).astype(BF16)
    low = lax.broadcasted_iota(jnp.int32, (BLOCK, LANES), 1) < breadth
    low_s = lax.broadcasted_iota(jnp.int32, (breadth, LANES), 1) < breadth
    row_x = lax.broadcasted_iota(jnp.int32, (EXTRA, LANES), 0)
    head_i = lax.broadcasted_iota(jnp.int32, (QUAD, QUAD), 0)
    head_j = lax.broadcasted_iota(jnp.int32, (QUAD, QUAD), 1)
    same, equal = head_i // breadth == head_j // breadth, head_i == head_j
    means = jnp.where(same, 1.0 / breadth, 0.0).astype(BF16)
    centre = (jnp.where(equal, 1.0, 0.0) - jnp.where(same, 1.0 / breadth, 0.0)).astype(BF16)
    ones = jnp.where(same, 1.0, 0.0).astype(BF16)
    state_rows, decay_rows = pl.ds(0, breadth), pl.ds(breadth, EXTRA)
    cuts = [slice(j * LANES, (j + 1) * LANES) for j in range(2)]

    def pack_rows(dec):
        hi = dec.astype(BF16).astype(F32)
        return jnp.where(row_x == 0, hi, jnp.where(row_x == 1, dec - hi, 0.0)).astype(BF16)

    def unpack_rows(x):
        x = x.astype(F32)
        return x[0:1] + x[1:2]

    def quad_lanes(p, t):
        return pl.ds(p * lane + t * QUAD, QUAD)

    def arrive(p, i):
        if p == 0:
            wait_all(held.at[i, :, pl.ds(0, half)], in_sem.at[i])

    def decays(p):
        cells = [(t, b) for t in range(quads) for b in range(blocks)]
        cums, vbs, kms, products = {}, {}, {}, {}
        arrive(p, 0)
        for t, b in cells:
            at, lanes = pl.ds(b * BLOCK, BLOCK), quad_lanes(p, t)
            log_decay = -jnp.exp(fade[at, lanes].astype(F32))
            hi = log_decay.astype(BF16)
            lo = (log_decay - hi.astype(F32)).astype(BF16)
            cum = dot(incl, jnp.concatenate([hi, lo], axis=0))
            cumx[at, lanes] = cum - log_decay
            cums[t, b] = cum
        arrive(p, 2)
        for t, b in cells:
            at, lanes = pl.ds(b * BLOCK, BLOCK), quad_lanes(p, t)
            vbs[t, b] = dot(val[at, lanes], centre).astype(BF16)
            centred[at, lanes] = vbs[t, b]
        arrive(p, 1)
        for t, b in cells:
            at, lanes = pl.ds(b * BLOCK, BLOCK), quad_lanes(p, t)
            mid = cums[t, b][BLOCK // 2 - 1 : BLOCK // 2]
            kms[t, b] = (key[at, lanes].astype(F32) * jnp.exp(mid - cums[t, b])).astype(BF16)
            key_mid[at, lanes] = kms[t, b]
            mid_row[b, :, lanes] = mid
        for t, b in cells:
            for j, cut in enumerate(cuts):
                products[t, b, j] = dot_tn(vbs[t, b][:, cut], kms[t, b][:, cut])
        for t in range(quads):
            lanes = quad_lanes(p, t)
            states = [jnp.zeros((breadth, LANES), F32) for _ in range(2)]
            pref = jnp.zeros((1, QUAD), F32)
            for b in range(blocks):
                cum = cums[t, b]
                mid, total = cum[BLOCK // 2 - 1 : BLOCK // 2], cum[BLOCK - 1 :]
                end, whole, begin = jnp.exp(total - mid), jnp.exp(total), jnp.exp(mid)
                pref_row[b, :, lanes] = pref
                for j, cut in enumerate(cuts):
                    if b > 0:
                        entering[p, b - 1, 2 * t + j] = (states[j] * begin[:, cut]).astype(BF16)
                    product = products[t, b, j]
                    own = jnp.where(low_s, product[:breadth], product[breadth:])
                    states[j] = states[j] * whole[:, cut] + own * end[:, cut]
                pref = pref + total
            gone = jnp.exp(pref)
            for j, cut in enumerate(cuts):
                outbox[p, 2 * t + j, state_rows, :] = states[j].astype(BF16)
                outbox[p, 2 * t + j, decay_rows, :] = pack_rows(gone[:, cut])

    def within(units):
        cells = [(p, t, b) for p, t in units for b in range(blocks)]
        rms, diags, scored = {}, {}, {}
        for p, t, b in cells:
            at, lanes = pl.ds(b * BLOCK, BLOCK), quad_lanes(p, t)
            cx = cumx[at, lanes]
            rf = rec[at, lanes].astype(F32)
            rms[p, t, b] = (rf * jnp.exp(cx - mid_row[b, :, lanes])).astype(BF16)
            recs[at, lanes] = (rf * jnp.exp(cx + pref_row[b, :, lanes])).astype(BF16)
            own = rf * key[at, lanes].astype(F32) * reward_row[:, lanes]
            diags[p, t, b] = dot(own.astype(BF16), ones)
            kb = key_mid[at, lanes]
            for j, cut in enumerate(cuts):
                scored[p, t, b, j] = dot_nt(rms[p, t, b][:, cut], split_heads(kb[:, cut], low))
        for p, t, b in cells:
            at, lanes = pl.ds(b * BLOCK, BLOCK), quad_lanes(p, t)
            g = gate[at, lanes].astype(F32)
            swish[at, lanes] = g / (1.0 + jnp.exp(-g)) * gains[p * lane // half, :, pl.ds(p * lane % half + t * QUAD, QUAD)]
        for p, t, b in cells:
            at, lanes = pl.ds(b * BLOCK, BLOCK), quad_lanes(p, t)
            vb = centred[at, lanes]
            for j, cut in enumerate(cuts):
                scores = jnp.where(t_id > s_id, scored[p, t, b, j], 0.0).astype(BF16)
                o = dot(scores, split_heads(vb[:, cut], low))
                if b > 0:
                    came = split_heads(entering[p, b - 1, 2 * t + j], low_s)
                    o = o + dot_nt(rms[p, t, b][:, cut], came)
                o = o + diags[p, t, b][:, cut] * vb[:, cut].astype(F32)
                local_out[at, pl.ds(p * lane + t * QUAD + j * LANES, LANES)] = o

    def finish(ps, between=()):
        cells = [(p, t, b) for p in ps for t in range(quads) for b in range(blocks)]
        states, outs, variances = {}, {}, {}
        for p in ps:
            for t in range(quads):
                x, y = (split_heads(carry[p, 2 * t + j], low_s) for j in range(2))
                none = jnp.zeros_like(x)
                states[p, t] = jnp.concatenate(
                    [jnp.concatenate([x, none], axis=1), jnp.concatenate([none, y], axis=1)], axis=0
                )
        for p, t, b in cells:
            at, lanes = pl.ds(b * BLOCK, BLOCK), quad_lanes(p, t)
            outs[p, t, b] = local_out[at, lanes] + dot_nt(recs[at, lanes], states[p, t])
        for p, t, b in cells:
            out = outs[p, t, b]
            variances[p, t, b] = dot((out * out).astype(BF16), means)
        for k in between:
            project(k, 0, cores - 1)
        for p, t, b in cells:
            at, lanes = pl.ds(b * BLOCK, BLOCK), quad_lanes(p, t)
            scale = lax.rsqrt(variances[p, t, b] + EPS) * swish[at, lanes]
            gated[at, lanes] = (outs[p, t, b] * scale).astype(BF16)

    def send_states(p):
        way, owner = p // cores, p % cores
        for t in chips[:-1]:
            pltpu.make_async_remote_copy(
                src_ref=outbox.at[p, t], dst_ref=inbox.at[way, r],
                send_sem=s_send.at[0], recv_sem=s_recv.at[way],
                device_id=(group * span + t, owner), device_id_type=MESH,
            ).start()

        @pl.when(core == owner)
        def _():
            inbox[way, r] = outbox[p, chip]

        @pl.when(core != owner)
        def _():
            pltpu.make_async_remote_copy(
                src_ref=outbox.at[p, chip], dst_ref=inbox.at[way, r],
                send_sem=s_send.at[0], recv_sem=s_recv.at[way],
                device_id=(me, owner), device_id_type=MESH,
            ).start()

    some = pl.ds(0, members - 1)

    def advance(box, state):
        s, d = state
        e = unpack_rows(box[decay_rows, :])
        return s * e + box[state_rows, :].astype(F32), d * e

    nothing = (jnp.zeros((breadth, LANES), F32), jnp.ones((1, LANES), F32))

    def scan(p):
        state = nothing
        for j in range(members):
            before[p, j] = state[0]
            before_dec[p, j] = state[1]
            state = advance(inbox.at[p, j], state)
        gout[p, state_rows, :] = state[0].astype(BF16)
        gout[p, decay_rows, :] = pack_rows(state[1])

    def group_copy(p, g, slot):
        return pltpu.make_async_remote_copy(
            src_ref=gout.at[p], dst_ref=gin.at[p, slot],
            send_sem=g_send.at[0], recv_sem=g_recv.at[p, slot],
            device_id=above(g), device_id_type=MESH,
        )

    def send_group(p):
        def body(i, c):
            group_copy(p, groups - 1 - i, group).start()
            return c

        lax.fori_loop(0, groups - 1 - group, body, 0)

    def take_group(p):
        def body(g, state):
            group_copy(p, g, g).wait_recv()
            return advance(gin.at[p, g], state)

        return lax.fori_loop(0, group, body, nothing)[0]

    def send_carry(way, came):
        p = way * cores + core
        for j in range(members):
            cbox[way, j] = (came * before_dec[way, j] + before[way, j]).astype(BF16)
        for q in peers:
            pltpu.make_async_remote_copy(
                src_ref=cbox.at[way, q], dst_ref=carry.at[p, chip],
                send_sem=c_send.at[0], recv_sem=c_recv.at[p],
                device_id=place(q), device_id_type=MESH,
            ).start()
        carry[p, chip] = cbox[way, r]

    def wait_carry(p):
        @pl.when(core == p % cores)
        def _():
            wait_all(carry.at[p, pl.ds(0, span - 1)], c_recv.at[p])

        @pl.when(core != p % cores)
        def _():
            wait_all(carry.at[p], c_recv.at[p])

    with jax.named_scope("decays0"):
        decays(0)
    with jax.named_scope("barrier"):
        pl.semaphore_wait(barrier, members - 1 + group)
        send_states(0)
        for i in range(2):
            small_copy(i, core).start()
        send_weight(0, 1)

        def here(g, c):
            pl.semaphore_signal(ready, inc=1, device_id=above(g), device_id_type=MESH)
            return c

        lax.fori_loop(0, group, here, 0)
        for k in range(chunks):
            pltpu.make_async_copy(columns(k), weight(core, k), weight_sem(k)).start()
    for p in range(1, parts):
        if p % ways == 0:
            with jax.named_scope("in1"):
                side = p // ways
                wait_all(held.at[pl.ds(0, 3), :, pl.ds(side * half, half)], in_sem.at[side + 2])
        with jax.named_scope("decays1"):
            decays(p)
        with jax.named_scope("send1"):
            send_states(p)
            send_weight(p, p + 1 if p < parts - 1 else p + 2)
    sent = parts + 1

    with jax.named_scope("in2"):
        wait_all(held.at[pl.ds(3, 2)], in_sem.at[cores + 2])
        for i in range(2):
            small_local[i].wait()
            small_copy(i, other).wait_recv()
        for h in range(width // breadth):
            reward_row[:, pl.ds(h * breadth, breadth)] = rewards[
                h * breadth // half, pl.ds(h % (half // breadth), 1), :
            ]

    units = [(p, t) for p in range(parts) for t in range(quads)]
    done = 0

    def some_within(count):
        nonlocal done
        for at in range(done, min(done + count, len(units)), 2):
            with jax.named_scope("within"):
                within(units[at : at + 2])
        done += count

    some_within(4)
    for p in range(ways):
        with jax.named_scope("wait_states"):
            wait_all(inbox.at[p, some], s_recv.at[p])
        with jax.named_scope("scan"):
            scan(p)
        with jax.named_scope("send_group"):
            if p == 0:
                @pl.when(group < groups - 1)
                def _():
                    pl.semaphore_wait(ready, groups - 1 - group)

            send_group(p)

            @pl.when(group == 0)
            def _():
                send_carry(p, nothing[0])
                send_weight(sent + 2 * p, sent + 2 * p + 2 if p < ways - 1 else 2 * chunks)

            @pl.when(group > 0)
            def _():
                send_weight(sent + 2 * p, sent + 2 * p + 2)

        some_within(2 if p < ways - 1 else len(units))
    with jax.named_scope("take_group"):
        @pl.when(group > 0)
        def _():
            for p in range(ways):
                at = sent + 2 * ways + p
                send_carry(p, take_group(p))
                send_weight(at, at + 1 if p < ways - 1 else 2 * chunks)

    def project(k, first, last):
        at = pl.ds(k * CHUNK, CHUNK)
        total = partial[:, at] if first > 0 else None
        for p in range(first, last):
            term = dot(gated[:, pl.ds(p * half, half)], weight(p, k)[...])
            total = term if total is None else total + term
        if last < cores:
            partial[:, at] = total
        else:
            out_ref[:, at] = total.astype(BF16)

    early = parts - ways
    with jax.named_scope("wait_carry"):
        for p in range(early):
            wait_carry(p)
    with jax.named_scope("finish"):
        finish(range(early))
    with jax.named_scope("wait_weight"):
        wait_all(weight_head.at[:, pl.ds(0, lead)], w_sem.at[0])
    with jax.named_scope("project_lead"):
        for k in range(lead - 2):
            project(k, 0, cores - 1)
    with jax.named_scope("wait_carry"):
        for p in range(early, parts):
            wait_carry(p)
    with jax.named_scope("finish"):
        finish(range(early, parts), range(lead - 2, lead))
    with jax.named_scope("project_led"):
        for k in range(lead):
            project(k, cores - 1, cores)
    with jax.named_scope("wait_weight"):
        for k in range(lead, split):
            wait_all(weight_head.at[:, k], weight_sem(k))
    with jax.named_scope("project_rest"):
        for k in range(lead, split):
            project(k, 0, cores)
    with jax.named_scope("wait_weight"):
        for k in range(split, chunks):
            wait_all(weight_tail.at[:, k - split], weight_sem(k))

    def drain_groups(g):
        wait_all(gin.at[:, pl.ds(0, groups - 1 - g)], g_send.at[0])

    with jax.named_scope("drain"):
        for g in range(groups - 1):
            pl.when(group == g)(functools.partial(drain_groups, g))
        wait_all(inbox.at[:, some], s_send.at[0])
        wait_all(cbox.at[:, some], c_send.at[0])
        wait_all(map_hbm, w_send.at[0])
        for i in range(2):
            small_copy(i, core).wait_send()


def tail_kernel(done_ref, gated_ref, weight_ref, out_hbm, last, sem):
    cores, tail, half, chunk = weight_ref.shape
    done = done_ref.shape[1]
    copies = [pltpu.make_async_copy(done_ref, out_hbm.at[:, pl.ds(0, done)], sem.at[0])]
    copies[0].start()
    for k in range(tail):
        total = dot(gated_ref[:, pl.ds(0, half)], weight_ref[0, k])
        for p in range(1, cores):
            total = total + dot(gated_ref[:, pl.ds(p * half, half)], weight_ref[p, k])
        last[k] = total.astype(BF16)
        at = pl.ds(done + k * chunk, chunk)
        copies.append(pltpu.make_async_copy(last.at[k], out_hbm.at[:, at], sem.at[k + 1]))
        copies[-1].start()
    for copy in copies:
        copy.wait()


def shards(n, cores, rec, key, val, fade, gate, reward, gain, mapping):
    tokens, width = rec.shape
    breadth = reward.shape[1]
    half, depth = mapping.shape
    ways = WAYS
    parts = ways * cores
    blocks, chunks, span = tokens // BLOCK, depth // CHUNK, width // parts // LANES
    members, groups = span * cores, n // span
    boxed = breadth + EXTRA
    dma = pltpu.SemaphoreType.DMA
    narrow = pltpu.VMEM((tokens, width), BF16)
    wide = pltpu.VMEM((tokens, width), F32)
    tail = min(TAIL, chunks - LEAD)
    split = chunks - tail
    vmem = pl.BlockSpec(memory_space=pltpu.VMEM)
    done, gated, last = pl.pallas_call(
        functools.partial(kernel, n, cores, breadth),
        out_shape=(
            pltpu.VMEM((tokens, split * CHUNK), BF16),
            pltpu.VMEM((tokens, width), BF16),
            pltpu.VMEM((cores, tail, half, CHUNK), BF16),
        ),
        in_specs=[pl.BlockSpec(memory_space=pl.ANY)] * 8,
        out_specs=(vmem,) * 3,
        scratch_shapes=[
            pltpu.VMEM((5, tokens, width), BF16),
            pltpu.VMEM((cores,) + reward.shape, F32),
            pltpu.VMEM((cores, 1, half), F32),
            pltpu.VMEM((cores, split, half, CHUNK), BF16),
            pltpu.VMEM((1, width), F32),
            wide, narrow, narrow, narrow, wide, wide,
            pltpu.VMEM((parts, max(blocks - 1, 1), span, breadth, LANES), BF16),
            pltpu.VMEM((blocks, 1, width), F32),
            pltpu.VMEM((blocks, 1, width), F32),
            pltpu.VMEM((parts, span, boxed, LANES), BF16),
            pltpu.VMEM((ways, members, boxed, LANES), BF16),
            pltpu.VMEM((ways, members, breadth, LANES), F32),
            pltpu.VMEM((ways, members, 1, LANES), F32),
            pltpu.VMEM((ways, boxed, LANES), BF16),
            pltpu.VMEM((ways, groups, boxed, LANES), BF16),
            pltpu.VMEM((ways, members, breadth, LANES), BF16),
            pltpu.VMEM((parts, span, breadth, LANES), BF16),
            pltpu.VMEM((tokens, LEAD * CHUNK), F32),
            dma((cores + 3,)), dma((2,)), dma((2,)), dma((2,)),
            dma((max(chunks - LEAD, 0) + 1,)), dma((1,)),
            dma((1,)), dma((ways,)), dma((1,)), dma((ways, groups)),
            dma((1,)), dma((parts,)), pltpu.SemaphoreType.REGULAR,
        ],
        compiler_params=pltpu.CompilerParams(
            collective_id=0, has_side_effects=True, vmem_limit_bytes=55 * 2**20
        ),
    )(rec, key, val, fade, gate, reward, gain.reshape(1, -1), mapping)
    return pl.pallas_call(
        tail_kernel,
        out_shape=jax.ShapeDtypeStruct((tokens, depth), BF16),
        in_specs=[vmem] * 3,
        out_specs=pl.BlockSpec(memory_space=pl.ANY),
        scratch_shapes=[pltpu.VMEM((tail, tokens, CHUNK), BF16), dma((tail + 1,))],
        compiler_params=pltpu.CompilerParams(vmem_limit_bytes=16 * 2**20),
    )(done, gated, last)


def solution(mesh):
    tokens = P(("seq", "head"), None)
    placed = (tokens,) * 5 + (P("head", None), P("head"), P("head", None))
    return jax.shard_map(
        functools.partial(shards, mesh.shape["seq"], mesh.shape["head"]),
        mesh=mesh, in_specs=placed, out_specs=tokens, check_vma=False,
    )
```

```python
import functools

import jax
import jax.numpy as jnp
from jax import lax
from jax.experimental import pallas as pl
from jax.experimental.pallas import tpu as pltpu
from jax.sharding import PartitionSpec as P

BLOCK = 128
LANES = 128
QUAD = 256
CHUNK = 512
LEAD = 4
WAYS = 2
TAIL = 2
EXTRA = 8
EPS = 1e-05
MESH = pl.DeviceIdType.MESH
F32 = jnp.float32
BF16 = jnp.bfloat16


def dot(a, b):
    return jnp.dot(a, b, preferred_element_type=F32)


def dot_nt(a, b):
    return lax.dot_general(a, b, (((1,), (1,)), ((), ())), preferred_element_type=F32)


def dot_tn(a, b):
    return lax.dot_general(a, b, (((0,), (0,)), ((), ())), preferred_element_type=F32)


def split_heads(x, low):
    zero = jnp.zeros_like(x)
    return jnp.concatenate([jnp.where(low, x, zero), jnp.where(low, zero, x)], axis=0)


def flip(r, i, members):
    q, bit = 0, 1
    while bit < members:
        q = q + bit * (((r // bit) % 2 + (i // bit) % 2) % 2)
        bit *= 2
    return q


def kernel(
    n, cores, breadth,
    rec_hbm, key_hbm, val_hbm, fade_hbm, gate_hbm, reward_hbm, gain_hbm, map_hbm,
    out_ref, gated, weight_tail,
    held, rewards, gains, weight_head,
    reward_row, cumx, key_mid, centred, recs, local_out, swish, entering, pref_row, mid_row,
    outbox, inbox, before, before_dec, gout, gin, cbox, carry, partial,
    in_sem, p_local, p_send, p_recv, w_sem, w_send,
    s_send, s_recv, g_send, g_recv, c_send, c_recv, ready,
):
    me, core = lax.axis_index("seq"), lax.axis_index("head")
    other = 1 - core
    tokens, width = held.shape[1:]
    half = width // cores
    parts, span = outbox.shape[:2]
    ways = parts // cores
    lane = width // parts
    blocks, quads = tokens // BLOCK, lane // QUAD
    split = weight_head.shape[1]
    chunks = split + weight_tail.shape[1]
    lead = min(LEAD, chunks)
    members = span * cores
    groups = n // span
    group = me // span
    chip = me % span
    r = chip * cores + core
    peers = [flip(r, i, members) for i in range(members - 1, 0, -1)]
    chips = [flip(chip, i, span) for i in range(span - 1, -1, -1)]
    fade, key, val, rec, gate = (held.at[i] for i in range(5))
    sources = (fade_hbm, key_hbm, val_hbm, rec_hbm, gate_hbm)

    def place(q):
        return (group * span + q // cores, q % cores)

    def above(g):
        return (g * span + me % span, core)

    barrier = pltpu.get_barrier_semaphore()
    for q in peers:
        pl.semaphore_signal(barrier, inc=1, device_id=place(q), device_id_type=MESH)

    pieces = [pl.ds(p * lane, lane) for p in range(ways)]
    pieces += [pl.ds(side * half, half) for side in range(1, cores)]
    for piece, at in enumerate(pieces):
        for i in (0, 2, 1):
            sem = in_sem.at[i if piece == 0 else piece + 2]
            pltpu.make_async_copy(sources[i].at[:, at], held.at[i, :, at], sem).start()

    def greet_above(g, c):
        pl.semaphore_signal(barrier, inc=1, device_id=above(g), device_id_type=MESH)
        return c

    lax.fori_loop(group + 1, groups, greet_above, 0)
    for i in range(3, 5):
        pltpu.make_async_copy(sources[i], held.at[i], in_sem.at[len(pieces) + 2]).start()

    def wait_all(ref, sem):
        pltpu.make_async_copy(ref, ref, sem).wait()

    small = ((reward_hbm, rewards), (gain_hbm, gains))
    small_local = [
        pltpu.make_async_copy(src, dst.at[core], p_local.at[i]) for i, (src, dst) in enumerate(small)
    ]

    def small_copy(i, side):
        src, dst = small[i]
        return pltpu.make_async_remote_copy(
            src_ref=src, dst_ref=dst.at[side], send_sem=p_send.at[i], recv_sem=p_recv.at[i],
            device_id=(me, other), device_id_type=MESH,
        )

    for copy in small_local:
        copy.start()

    def columns(k):
        return map_hbm.at[:, pl.ds(k * CHUNK, CHUNK)]

    def weight(side, k):
        return weight_head.at[side, k] if k < split else weight_tail.at[side, k - split]

    def weight_sem(k):
        return w_sem.at[max(k - lead + 1, 0)]

    def send_weight(start, stop=2 * chunks):
        for piece in range(start, min(stop, 2 * chunks)):
            k, rows = piece // 2, pl.ds(piece % 2 * (half // 2), half // 2)
            pltpu.make_async_remote_copy(
                src_ref=map_hbm.at[rows, pl.ds(k * CHUNK, CHUNK)], dst_ref=weight(core, k).at[rows],
                send_sem=w_send.at[0], recv_sem=weight_sem(k),
                device_id=(me, other), device_id_type=MESH,
            ).start()

    t_id = lax.broadcasted_iota(jnp.int32, (BLOCK, 2 * BLOCK), 0)
    s_id = lax.rem(lax.broadcasted_iota(jnp.int32, (BLOCK, 2 * BLOCK), 1), BLOCK)
    incl = jnp.where(t_id >= s_id, 1.0, 0.0).astype(BF16)
    low = lax.broadcasted_iota(jnp.int32, (BLOCK, LANES), 1) < breadth
    low_s = lax.broadcasted_iota(jnp.int32, (breadth, LANES), 1) < breadth
    row_x = lax.broadcasted_iota(jnp.int32, (EXTRA, LANES), 0)
    head_i = lax.broadcasted_iota(jnp.int32, (QUAD, QUAD), 0)
    head_j = lax.broadcasted_iota(jnp.int32, (QUAD, QUAD), 1)
    same, equal = head_i // breadth == head_j // breadth, head_i == head_j
    means = jnp.where(same, 1.0 / breadth, 0.0).astype(BF16)
    centre = (jnp.where(equal, 1.0, 0.0) - jnp.where(same, 1.0 / breadth, 0.0)).astype(BF16)
    ones = jnp.where(same, 1.0, 0.0).astype(BF16)
    state_rows, decay_rows = pl.ds(0, breadth), pl.ds(breadth, EXTRA)
    cuts = [slice(j * LANES, (j + 1) * LANES) for j in range(2)]

    def pack_rows(dec):
        hi = dec.astype(BF16).astype(F32)
        return jnp.where(row_x == 0, hi, jnp.where(row_x == 1, dec - hi, 0.0)).astype(BF16)

    def unpack_rows(x):
        x = x.astype(F32)
        return x[0:1] + x[1:2]

    def quad_lanes(p, t):
        return pl.ds(p * lane + t * QUAD, QUAD)

    def arrive(p, i):
        if p == 0:
            wait_all(held.at[i, :, pieces[0]], in_sem.at[i])

    def decays(p):
        cells = [(t, b) for t in range(quads) for b in range(blocks)]
        cums, vbs, kms, products = {}, {}, {}, {}
        arrive(p, 0)
        for t, b in cells:
            at, lanes = pl.ds(b * BLOCK, BLOCK), quad_lanes(p, t)
            log_decay = -jnp.exp(fade[at, lanes].astype(F32))
            hi = log_decay.astype(BF16)
            lo = (log_decay - hi.astype(F32)).astype(BF16)
            cum = dot(incl, jnp.concatenate([hi, lo], axis=0))
            cumx[at, lanes] = cum - log_decay
            cums[t, b] = cum
        arrive(p, 2)
        for t, b in cells:
            at, lanes = pl.ds(b * BLOCK, BLOCK), quad_lanes(p, t)
            vbs[t, b] = dot(val[at, lanes], centre).astype(BF16)
            centred[at, lanes] = vbs[t, b]
        arrive(p, 1)
        for t, b in cells:
            at, lanes = pl.ds(b * BLOCK, BLOCK), quad_lanes(p, t)
            mid = cums[t, b][BLOCK // 2 - 1 : BLOCK // 2]
            kms[t, b] = (key[at, lanes].astype(F32) * jnp.exp(mid - cums[t, b])).astype(BF16)
            key_mid[at, lanes] = kms[t, b]
            mid_row[b, :, lanes] = mid
        for t, b in cells:
            for j, cut in enumerate(cuts):
                products[t, b, j] = dot_tn(vbs[t, b][:, cut], kms[t, b][:, cut])
        for t in range(quads):
            lanes = quad_lanes(p, t)
            states = [jnp.zeros((breadth, LANES), F32) for _ in range(2)]
            pref = jnp.zeros((1, QUAD), F32)
            for b in range(blocks):
                cum = cums[t, b]
                mid, total = cum[BLOCK // 2 - 1 : BLOCK // 2], cum[BLOCK - 1 :]
                end, whole, begin = jnp.exp(total - mid), jnp.exp(total), jnp.exp(mid)
                pref_row[b, :, lanes] = pref
                for j, cut in enumerate(cuts):
                    if b > 0:
                        entering[p, b - 1, 2 * t + j] = (states[j] * begin[:, cut]).astype(BF16)
                    product = products[t, b, j]
                    own = jnp.where(low_s, product[:breadth], product[breadth:])
                    states[j] = states[j] * whole[:, cut] + own * end[:, cut]
                pref = pref + total
            gone = jnp.exp(pref)
            for j, cut in enumerate(cuts):
                outbox[p, 2 * t + j, state_rows, :] = states[j].astype(BF16)
                outbox[p, 2 * t + j, decay_rows, :] = pack_rows(gone[:, cut])

    def within(units):
        cells = [(p, t, b) for p, t in units for b in range(blocks)]
        rms, diags, scored = {}, {}, {}
        for p, t, b in cells:
            at, lanes = pl.ds(b * BLOCK, BLOCK), quad_lanes(p, t)
            cx = cumx[at, lanes]
            rf = rec[at, lanes].astype(F32)
            rms[p, t, b] = (rf * jnp.exp(cx - mid_row[b, :, lanes])).astype(BF16)
            recs[at, lanes] = (rf * jnp.exp(cx + pref_row[b, :, lanes])).astype(BF16)
            own = rf * key[at, lanes].astype(F32) * reward_row[:, lanes]
            diags[p, t, b] = dot(own.astype(BF16), ones)
            kb = key_mid[at, lanes]
            for j, cut in enumerate(cuts):
                scored[p, t, b, j] = dot_nt(rms[p, t, b][:, cut], split_heads(kb[:, cut], low))
        for p, t, b in cells:
            at, lanes = pl.ds(b * BLOCK, BLOCK), quad_lanes(p, t)
            g = gate[at, lanes].astype(F32)
            swish[at, lanes] = g / (1.0 + jnp.exp(-g)) * gains[p * lane // half, :, pl.ds(p * lane % half + t * QUAD, QUAD)]
        for p, t, b in cells:
            at, lanes = pl.ds(b * BLOCK, BLOCK), quad_lanes(p, t)
            vb = centred[at, lanes]
            for j, cut in enumerate(cuts):
                scores = jnp.where(t_id > s_id, scored[p, t, b, j], 0.0).astype(BF16)
                o = dot(scores, split_heads(vb[:, cut], low))
                if b > 0:
                    came = split_heads(entering[p, b - 1, 2 * t + j], low_s)
                    o = o + dot_nt(rms[p, t, b][:, cut], came)
                o = o + diags[p, t, b][:, cut] * vb[:, cut].astype(F32)
                local_out[at, pl.ds(p * lane + t * QUAD + j * LANES, LANES)] = o

    def finish(ps, between=()):
        cells = [(p, t) for p in ps for t in range(quads)]
        states, outs = {}, {}
        for p, t in cells:
            x, y = (split_heads(carry[p, 2 * t + j], low_s) for j in range(2))
            none = jnp.zeros_like(x)
            states[p, t] = jnp.concatenate(
                [jnp.concatenate([x, none], axis=1), jnp.concatenate([none, y], axis=1)], axis=0
            )
        for p, t in cells:
            lanes = quad_lanes(p, t)
            outs[p, t] = local_out[:, lanes] + dot_nt(recs[:, lanes], states[p, t])
        squares = [(outs[cell] * outs[cell]).astype(BF16) for cell in cells]
        variances = dot(jnp.concatenate(squares, axis=0), means)
        for k in between:
            project(k, 0, cores - 1)
        for i, (p, t) in enumerate(cells):
            lanes = quad_lanes(p, t)
            variance = variances[i * tokens : (i + 1) * tokens]
            scale = lax.rsqrt(variance + EPS) * swish[:, lanes]
            gated[:, lanes] = (outs[p, t] * scale).astype(BF16)

    def send_states(p):
        way, owner = p // cores, p % cores
        for t in chips[:-1]:
            pltpu.make_async_remote_copy(
                src_ref=outbox.at[p, t], dst_ref=inbox.at[way, r],
                send_sem=s_send.at[0], recv_sem=s_recv.at[way],
                device_id=(group * span + t, owner), device_id_type=MESH,
            ).start()

        @pl.when(core == owner)
        def _():
            inbox[way, r] = outbox[p, chip]

        @pl.when(core != owner)
        def _():
            pltpu.make_async_remote_copy(
                src_ref=outbox.at[p, chip], dst_ref=inbox.at[way, r],
                send_sem=s_send.at[0], recv_sem=s_recv.at[way],
                device_id=(me, owner), device_id_type=MESH,
            ).start()

    some = pl.ds(0, members - 1)

    def advance(box, state):
        s, d = state
        e = unpack_rows(box[decay_rows, :])
        return s * e + box[state_rows, :].astype(F32), d * e

    nothing = (jnp.zeros((breadth, LANES), F32), jnp.ones((1, LANES), F32))

    def scan(p):
        state = nothing
        for j in range(members):
            before[p, j] = state[0]
            before_dec[p, j] = state[1]
            state = advance(inbox.at[p, j], state)
        gout[p, state_rows, :] = state[0].astype(BF16)
        gout[p, decay_rows, :] = pack_rows(state[1])

    def group_copy(p, g, slot):
        return pltpu.make_async_remote_copy(
            src_ref=gout.at[p], dst_ref=gin.at[p, slot],
            send_sem=g_send.at[0], recv_sem=g_recv.at[p, slot],
            device_id=above(g), device_id_type=MESH,
        )

    def send_group(p):
        def body(i, c):
            group_copy(p, groups - 1 - i, group).start()
            return c

        lax.fori_loop(0, groups - 1 - group, body, 0)

    def take_group(p):
        def body(g, state):
            group_copy(p, g, g).wait_recv()
            return advance(gin.at[p, g], state)

        return lax.fori_loop(0, group, body, nothing)[0]

    def send_carry(way, came):
        p = way * cores + core
        for j in range(members):
            cbox[way, j] = (came * before_dec[way, j] + before[way, j]).astype(BF16)
        for q in peers:
            pltpu.make_async_remote_copy(
                src_ref=cbox.at[way, q], dst_ref=carry.at[p, chip],
                send_sem=c_send.at[0], recv_sem=c_recv.at[p],
                device_id=place(q), device_id_type=MESH,
            ).start()
        carry[p, chip] = cbox[way, r]

    def wait_carry(p):
        @pl.when(core == p % cores)
        def _():
            wait_all(carry.at[p, pl.ds(0, span - 1)], c_recv.at[p])

        @pl.when(core != p % cores)
        def _():
            wait_all(carry.at[p], c_recv.at[p])

    with jax.named_scope("decays0"):
        decays(0)
    with jax.named_scope("barrier"):
        pl.semaphore_wait(barrier, members - 1 + group)
        send_states(0)
        for i in range(2):
            small_copy(i, core).start()
        send_weight(0, 1)

        def here(g, c):
            pl.semaphore_signal(ready, inc=1, device_id=above(g), device_id_type=MESH)
            return c

        lax.fori_loop(0, group, here, 0)
        for k in range(chunks):
            pltpu.make_async_copy(columns(k), weight(core, k), weight_sem(k)).start()
    for p in range(1, parts):
        piece = p if p < ways else ways - 1 + p // ways
        if p < ways or p % ways == 0:
            with jax.named_scope("in1"):
                wait_all(held.at[pl.ds(0, 3), :, pieces[piece]], in_sem.at[piece + 2])
        with jax.named_scope("decays1"):
            decays(p)
        with jax.named_scope("send1"):
            send_states(p)
            send_weight(p, p + 1)
    sent = parts

    @pl.when(group > 0)
    def _():
        send_weight(sent, sent + 1)

    with jax.named_scope("in2"):
        wait_all(held.at[pl.ds(3, 2)], in_sem.at[len(pieces) + 2])
        for i in range(2):
            small_local[i].wait()
            small_copy(i, other).wait_recv()
        for h in range(width // breadth):
            reward_row[:, pl.ds(h * breadth, breadth)] = rewards[
                h * breadth // half, pl.ds(h % (half // breadth), 1), :
            ]

    units = [(p, t) for p in range(parts) for t in range(quads)]
    done = 0

    def some_within(count):
        nonlocal done
        for at in range(done, min(done + count, len(units)), 2):
            with jax.named_scope("within"):
                within(units[at : at + 2])
        done += count

    some_within(4)
    for p in range(ways):
        with jax.named_scope("wait_states"):
            wait_all(inbox.at[p, some], s_recv.at[p])
        with jax.named_scope("scan"):
            scan(p)
        with jax.named_scope("send_group"):
            if p == 0:
                @pl.when(group < groups - 1)
                def _():
                    pl.semaphore_wait(ready, groups - 1 - group)

            send_group(p)

            @pl.when(group == 0)
            def _():
                send_carry(p, nothing[0])
                send_weight(sent + p, sent + p + 1 if p < ways - 1 else 2 * chunks)

            @pl.when(group > 0)
            def _():
                send_weight(sent + 2 * p + 1, sent + 2 * p + 3)

        some_within(2 if p < ways - 1 else len(units))
    with jax.named_scope("take_group"):
        @pl.when(group > 0)
        def _():
            for p in range(ways):
                at = sent + 2 * ways + p + 1
                send_carry(p, take_group(p))
                send_weight(at, at + 1 if p < ways - 1 else 2 * chunks)

    def project(k, first, last):
        at = pl.ds(k * CHUNK, CHUNK)
        total = partial[:, at] if first > 0 else None
        for p in range(first, last):
            term = dot(gated[:, pl.ds(p * half, half)], weight(p, k)[...])
            total = term if total is None else total + term
        if last < cores:
            partial[:, at] = total
        else:
            out_ref[:, at] = total.astype(BF16)

    early = parts - ways
    with jax.named_scope("wait_carry"):
        for p in range(early):
            wait_carry(p)
    with jax.named_scope("finish"):
        finish(range(early))
    with jax.named_scope("wait_weight"):
        wait_all(weight_head.at[:, pl.ds(0, lead)], w_sem.at[0])
    with jax.named_scope("project_lead"):
        for k in range(lead - 2):
            project(k, 0, cores - 1)
    with jax.named_scope("wait_carry"):
        for p in range(early, parts):
            wait_carry(p)
    with jax.named_scope("finish"):
        finish(range(early, parts), range(lead - 2, lead))
    with jax.named_scope("project_led"):
        for k in range(lead):
            project(k, cores - 1, cores)
    with jax.named_scope("wait_weight"):
        for k in range(lead, split):
            wait_all(weight_head.at[:, k], weight_sem(k))
    with jax.named_scope("project_rest"):
        for k in range(lead, split):
            project(k, 0, cores)
    with jax.named_scope("wait_weight"):
        for k in range(split, chunks):
            wait_all(weight_tail.at[:, k - split], weight_sem(k))

    def drain_groups(g):
        wait_all(gin.at[:, pl.ds(0, groups - 1 - g)], g_send.at[0])

    with jax.named_scope("drain"):
        for g in range(groups - 1):
            pl.when(group == g)(functools.partial(drain_groups, g))
        wait_all(inbox.at[:, some], s_send.at[0])
        wait_all(cbox.at[:, some], c_send.at[0])
        wait_all(map_hbm, w_send.at[0])
        for i in range(2):
            small_copy(i, core).wait_send()


def tail_kernel(done_ref, gated_ref, weight_ref, out_hbm, last, sem):
    cores, tail, half, chunk = weight_ref.shape
    done = done_ref.shape[1]
    copies = [pltpu.make_async_copy(done_ref, out_hbm.at[:, pl.ds(0, done)], sem.at[0])]
    copies[0].start()
    for k in range(tail):
        total = dot(gated_ref[:, pl.ds(0, half)], weight_ref[0, k])
        for p in range(1, cores):
            total = total + dot(gated_ref[:, pl.ds(p * half, half)], weight_ref[p, k])
        last[k] = total.astype(BF16)
        at = pl.ds(done + k * chunk, chunk)
        copies.append(pltpu.make_async_copy(last.at[k], out_hbm.at[:, at], sem.at[k + 1]))
        copies[-1].start()
    for copy in copies:
        copy.wait()


def shards(n, cores, rec, key, val, fade, gate, reward, gain, mapping):
    tokens, width = rec.shape
    breadth = reward.shape[1]
    half, depth = mapping.shape
    ways = WAYS
    parts = ways * cores
    blocks, chunks, span = tokens // BLOCK, depth // CHUNK, width // parts // LANES
    members, groups = span * cores, n // span
    boxed = breadth + EXTRA
    dma = pltpu.SemaphoreType.DMA
    narrow = pltpu.VMEM((tokens, width), BF16)
    wide = pltpu.VMEM((tokens, width), F32)
    tail = min(TAIL, chunks - LEAD)
    split = chunks - tail
    vmem = pl.BlockSpec(memory_space=pltpu.VMEM)
    done, gated, last = pl.pallas_call(
        functools.partial(kernel, n, cores, breadth),
        out_shape=(
            pltpu.VMEM((tokens, split * CHUNK), BF16),
            pltpu.VMEM((tokens, width), BF16),
            pltpu.VMEM((cores, tail, half, CHUNK), BF16),
        ),
        in_specs=[pl.BlockSpec(memory_space=pl.ANY)] * 8,
        out_specs=(vmem,) * 3,
        scratch_shapes=[
            pltpu.VMEM((5, tokens, width), BF16),
            pltpu.VMEM((cores,) + reward.shape, F32),
            pltpu.VMEM((cores, 1, half), F32),
            pltpu.VMEM((cores, split, half, CHUNK), BF16),
            pltpu.VMEM((1, width), F32),
            wide, narrow, narrow, narrow, wide, wide,
            pltpu.VMEM((parts, max(blocks - 1, 1), span, breadth, LANES), BF16),
            pltpu.VMEM((blocks, 1, width), F32),
            pltpu.VMEM((blocks, 1, width), F32),
            pltpu.VMEM((parts, span, boxed, LANES), BF16),
            pltpu.VMEM((ways, members, boxed, LANES), BF16),
            pltpu.VMEM((ways, members, breadth, LANES), F32),
            pltpu.VMEM((ways, members, 1, LANES), F32),
            pltpu.VMEM((ways, boxed, LANES), BF16),
            pltpu.VMEM((ways, groups, boxed, LANES), BF16),
            pltpu.VMEM((ways, members, breadth, LANES), BF16),
            pltpu.VMEM((parts, span, breadth, LANES), BF16),
            pltpu.VMEM((tokens, LEAD * CHUNK), F32),
            dma((ways + cores + 2,)), dma((2,)), dma((2,)), dma((2,)),
            dma((max(chunks - LEAD, 0) + 1,)), dma((1,)),
            dma((1,)), dma((ways,)), dma((1,)), dma((ways, groups)),
            dma((1,)), dma((parts,)), pltpu.SemaphoreType.REGULAR,
        ],
        compiler_params=pltpu.CompilerParams(
            collective_id=0, has_side_effects=True, vmem_limit_bytes=55 * 2**20
        ),
    )(rec, key, val, fade, gate, reward, gain.reshape(1, -1), mapping)
    return pl.pallas_call(
        tail_kernel,
        out_shape=jax.ShapeDtypeStruct((tokens, depth), BF16),
        in_specs=[vmem] * 3,
        out_specs=pl.BlockSpec(memory_space=pl.ANY),
        scratch_shapes=[pltpu.VMEM((tail, tokens, CHUNK), BF16), dma((tail + 1,))],
        compiler_params=pltpu.CompilerParams(vmem_limit_bytes=16 * 2**20),
    )(done, gated, last)


def solution(mesh):
    tokens = P(("seq", "head"), None)
    placed = (tokens,) * 5 + (P("head", None), P("head"), P("head", None))
    return jax.shard_map(
        functools.partial(shards, mesh.shape["seq"], mesh.shape["head"]),
        mesh=mesh, in_specs=placed, out_specs=tokens, check_vma=False,
    )
```

```python
import functools

import jax
import jax.numpy as jnp
from jax import lax
from jax.experimental import pallas as pl
from jax.experimental.pallas import tpu as pltpu
from jax.sharding import PartitionSpec as P

BLOCK = 128
LANES = 128
QUAD = 256
CHUNK = 512
LEAD = 4
WAYS = 2
TAIL = 2
EXTRA = 8
EPS = 1e-05
MESH = pl.DeviceIdType.MESH
F32 = jnp.float32
BF16 = jnp.bfloat16


def dot(a, b):
    return jnp.dot(a, b, preferred_element_type=F32)


def dot_nt(a, b):
    return lax.dot_general(a, b, (((1,), (1,)), ((), ())), preferred_element_type=F32)


def dot_tn(a, b):
    return lax.dot_general(a, b, (((0,), (0,)), ((), ())), preferred_element_type=F32)


def split_heads(x, low):
    zero = jnp.zeros_like(x)
    return jnp.concatenate([jnp.where(low, x, zero), jnp.where(low, zero, x)], axis=0)


def flip(r, i, members):
    q, bit = 0, 1
    while bit < members:
        q = q + bit * (((r // bit) % 2 + (i // bit) % 2) % 2)
        bit *= 2
    return q


def kernel(
    n, cores, breadth,
    rec_hbm, key_hbm, val_hbm, fade_hbm, gate_hbm, reward_hbm, gain_hbm, map_hbm,
    out_ref, gated, weight_tail,
    held, rewards, gains, weight_head,
    reward_row, cumx, key_mid, centred, recs, local_out, swish, entering, pref_row, mid_row,
    outbox, inbox, before, before_dec, gout, gin, cbox, carry, partial,
    in_sem, p_local, p_send, p_recv, w_sem, w_send,
    s_send, s_recv, g_send, g_recv, c_send, c_recv, ready,
):
    me, core = lax.axis_index("seq"), lax.axis_index("head")
    other = 1 - core
    tokens, width = held.shape[1:]
    half = width // cores
    parts, span = outbox.shape[:2]
    ways = parts // cores
    lane = width // parts
    blocks, quads = tokens // BLOCK, lane // QUAD
    split = weight_head.shape[1]
    chunks = split + weight_tail.shape[1]
    lead = min(LEAD, chunks)
    members = span * cores
    groups = n // span
    group = me // span
    chip = me % span
    r = chip * cores + core
    peers = [flip(r, i, members) for i in range(members - 1, 0, -1)]
    chips = [flip(chip, i, span) for i in range(span - 1, -1, -1)]
    fade, key, val, rec, gate = (held.at[i] for i in range(5))
    sources = (fade_hbm, key_hbm, val_hbm, rec_hbm, gate_hbm)

    def place(q):
        return (group * span + q // cores, q % cores)

    def above(g):
        return (g * span + me % span, core)

    barrier = pltpu.get_barrier_semaphore()
    for q in peers:
        pl.semaphore_signal(barrier, inc=1, device_id=place(q), device_id_type=MESH)

    pieces = [pl.ds(p * lane, lane) for p in range(ways)]
    pieces += [pl.ds(side * half, half) for side in range(1, cores)]
    for piece, at in enumerate(pieces):
        for i in (0, 2, 1):
            sem = in_sem.at[i if piece == 0 else piece + 2]
            pltpu.make_async_copy(sources[i].at[:, at], held.at[i, :, at], sem).start()

    def greet_above(g, c):
        pl.semaphore_signal(barrier, inc=1, device_id=above(g), device_id_type=MESH)
        return c

    lax.fori_loop(group + 1, groups, greet_above, 0)
    for i in range(3, 5):
        pltpu.make_async_copy(sources[i], held.at[i], in_sem.at[len(pieces) + 2]).start()

    def wait_all(ref, sem):
        pltpu.make_async_copy(ref, ref, sem).wait()

    small = ((reward_hbm, rewards), (gain_hbm, gains))
    small_local = [
        pltpu.make_async_copy(src, dst.at[core], p_local.at[i]) for i, (src, dst) in enumerate(small)
    ]

    def small_copy(i, side):
        src, dst = small[i]
        return pltpu.make_async_remote_copy(
            src_ref=src, dst_ref=dst.at[side], send_sem=p_send.at[i], recv_sem=p_recv.at[i],
            device_id=(me, other), device_id_type=MESH,
        )

    for copy in small_local:
        copy.start()

    def columns(k):
        return map_hbm.at[:, pl.ds(k * CHUNK, CHUNK)]

    def weight(side, k):
        return weight_head.at[side, k] if k < split else weight_tail.at[side, k - split]

    def weight_sem(k):
        return w_sem.at[0 if k < lead else 1 if k < split else 2]

    def send_weight(start, stop=2 * chunks):
        for piece in range(start, min(stop, 2 * chunks)):
            k, rows = piece // 2, pl.ds(piece % 2 * (half // 2), half // 2)
            pltpu.make_async_remote_copy(
                src_ref=map_hbm.at[rows, pl.ds(k * CHUNK, CHUNK)], dst_ref=weight(core, k).at[rows],
                send_sem=w_send.at[0], recv_sem=weight_sem(k),
                device_id=(me, other), device_id_type=MESH,
            ).start()

    t_id = lax.broadcasted_iota(jnp.int32, (BLOCK, 2 * BLOCK), 0)
    s_id = lax.rem(lax.broadcasted_iota(jnp.int32, (BLOCK, 2 * BLOCK), 1), BLOCK)
    incl = jnp.where(t_id >= s_id, 1.0, 0.0).astype(BF16)
    low = lax.broadcasted_iota(jnp.int32, (BLOCK, LANES), 1) < breadth
    low_s = lax.broadcasted_iota(jnp.int32, (breadth, LANES), 1) < breadth
    row_x = lax.broadcasted_iota(jnp.int32, (EXTRA, LANES), 0)
    head_i = lax.broadcasted_iota(jnp.int32, (QUAD, QUAD), 0)
    head_j = lax.broadcasted_iota(jnp.int32, (QUAD, QUAD), 1)
    same, equal = head_i // breadth == head_j // breadth, head_i == head_j
    means = jnp.where(same, 1.0 / breadth, 0.0).astype(BF16)
    centre = (jnp.where(equal, 1.0, 0.0) - jnp.where(same, 1.0 / breadth, 0.0)).astype(BF16)
    ones = jnp.where(same, 1.0, 0.0).astype(BF16)
    state_rows, decay_rows = pl.ds(0, breadth), pl.ds(breadth, EXTRA)
    cuts = [slice(j * LANES, (j + 1) * LANES) for j in range(2)]

    def pack_rows(dec):
        hi = dec.astype(BF16).astype(F32)
        return jnp.where(row_x == 0, hi, jnp.where(row_x == 1, dec - hi, 0.0)).astype(BF16)

    def unpack_rows(x):
        x = x.astype(F32)
        return x[0:1] + x[1:2]

    def quad_lanes(p, t):
        return pl.ds(p * lane + t * QUAD, QUAD)

    def arrive(p, i):
        if p == 0:
            wait_all(held.at[i, :, pieces[0]], in_sem.at[i])

    def decays(p):
        cells = [(t, b) for t in range(quads) for b in range(blocks)]
        cums, vbs, kms, products = {}, {}, {}, {}
        arrive(p, 0)
        for t, b in cells:
            at, lanes = pl.ds(b * BLOCK, BLOCK), quad_lanes(p, t)
            log_decay = -jnp.exp(fade[at, lanes].astype(F32))
            hi = log_decay.astype(BF16)
            lo = (log_decay - hi.astype(F32)).astype(BF16)
            cum = dot(incl, jnp.concatenate([hi, lo], axis=0))
            cumx[at, lanes] = cum - log_decay
            cums[t, b] = cum
        arrive(p, 2)
        for t, b in cells:
            at, lanes = pl.ds(b * BLOCK, BLOCK), quad_lanes(p, t)
            vbs[t, b] = dot(val[at, lanes], centre).astype(BF16)
            centred[at, lanes] = vbs[t, b]
        arrive(p, 1)
        for t, b in cells:
            at, lanes = pl.ds(b * BLOCK, BLOCK), quad_lanes(p, t)
            mid = cums[t, b][BLOCK // 2 - 1 : BLOCK // 2]
            kms[t, b] = (key[at, lanes].astype(F32) * jnp.exp(mid - cums[t, b])).astype(BF16)
            key_mid[at, lanes] = kms[t, b]
            mid_row[b, :, lanes] = mid
        for t, b in cells:
            for j, cut in enumerate(cuts):
                products[t, b, j] = dot_tn(vbs[t, b][:, cut], kms[t, b][:, cut])
        for t in range(quads):
            lanes = quad_lanes(p, t)
            states = [jnp.zeros((breadth, LANES), F32) for _ in range(2)]
            pref = jnp.zeros((1, QUAD), F32)
            for b in range(blocks):
                cum = cums[t, b]
                mid, total = cum[BLOCK // 2 - 1 : BLOCK // 2], cum[BLOCK - 1 :]
                end, whole, begin = jnp.exp(total - mid), jnp.exp(total), jnp.exp(mid)
                pref_row[b, :, lanes] = pref
                for j, cut in enumerate(cuts):
                    if b > 0:
                        entering[p, b - 1, 2 * t + j] = (states[j] * begin[:, cut]).astype(BF16)
                    product = products[t, b, j]
                    own = jnp.where(low_s, product[:breadth], product[breadth:])
                    states[j] = states[j] * whole[:, cut] + own * end[:, cut]
                pref = pref + total
            gone = jnp.exp(pref)
            for j, cut in enumerate(cuts):
                outbox[p, 2 * t + j, state_rows, :] = states[j].astype(BF16)
                outbox[p, 2 * t + j, decay_rows, :] = pack_rows(gone[:, cut])

    def within(units):
        cells = [(p, t, b) for p, t in units for b in range(blocks)]
        rms, diags, scored = {}, {}, {}
        for p, t, b in cells:
            at, lanes = pl.ds(b * BLOCK, BLOCK), quad_lanes(p, t)
            cx = cumx[at, lanes]
            rf = rec[at, lanes].astype(F32)
            rms[p, t, b] = (rf * jnp.exp(cx - mid_row[b, :, lanes])).astype(BF16)
            recs[at, lanes] = (rf * jnp.exp(cx + pref_row[b, :, lanes])).astype(BF16)
            own = rf * key[at, lanes].astype(F32) * reward_row[:, lanes]
            diags[p, t, b] = dot(own.astype(BF16), ones)
            kb = key_mid[at, lanes]
            for j, cut in enumerate(cuts):
                scored[p, t, b, j] = dot_nt(rms[p, t, b][:, cut], split_heads(kb[:, cut], low))
        for p, t, b in cells:
            at, lanes = pl.ds(b * BLOCK, BLOCK), quad_lanes(p, t)
            g = gate[at, lanes].astype(F32)
            swish[at, lanes] = g / (1.0 + jnp.exp(-g)) * gains[p * lane // half, :, pl.ds(p * lane % half + t * QUAD, QUAD)]
        for p, t, b in cells:
            at, lanes = pl.ds(b * BLOCK, BLOCK), quad_lanes(p, t)
            vb = centred[at, lanes]
            for j, cut in enumerate(cuts):
                scores = jnp.where(t_id > s_id, scored[p, t, b, j], 0.0).astype(BF16)
                o = dot(scores, split_heads(vb[:, cut], low))
                if b > 0:
                    came = split_heads(entering[p, b - 1, 2 * t + j], low_s)
                    o = o + dot_nt(rms[p, t, b][:, cut], came)
                o = o + diags[p, t, b][:, cut] * vb[:, cut].astype(F32)
                local_out[at, pl.ds(p * lane + t * QUAD + j * LANES, LANES)] = o

    def finish(ps, between=()):
        cells = [(p, t) for p in ps for t in range(quads)]
        states, outs = {}, {}
        for p, t in cells:
            x, y = (split_heads(carry[p, 2 * t + j], low_s) for j in range(2))
            none = jnp.zeros_like(x)
            states[p, t] = jnp.concatenate(
                [jnp.concatenate([x, none], axis=1), jnp.concatenate([none, y], axis=1)], axis=0
            )
        for p, t in cells:
            lanes = quad_lanes(p, t)
            outs[p, t] = local_out[:, lanes] + dot_nt(recs[:, lanes], states[p, t])
        squares = [(outs[cell] * outs[cell]).astype(BF16) for cell in cells]
        variances = dot(jnp.concatenate(squares, axis=0), means)
        for k in between:
            project(k, 0, cores - 1)
        for i, (p, t) in enumerate(cells):
            lanes = quad_lanes(p, t)
            variance = variances[i * tokens : (i + 1) * tokens]
            scale = lax.rsqrt(variance + EPS) * swish[:, lanes]
            gated[:, lanes] = (outs[p, t] * scale).astype(BF16)

    def send_states(p):
        way, owner = p // cores, p % cores
        for t in chips[:-1]:
            pltpu.make_async_remote_copy(
                src_ref=outbox.at[p, t], dst_ref=inbox.at[way, r],
                send_sem=s_send.at[0], recv_sem=s_recv.at[way],
                device_id=(group * span + t, owner), device_id_type=MESH,
            ).start()

        @pl.when(core == owner)
        def _():
            inbox[way, r] = outbox[p, chip]

        @pl.when(core != owner)
        def _():
            pltpu.make_async_remote_copy(
                src_ref=outbox.at[p, chip], dst_ref=inbox.at[way, r],
                send_sem=s_send.at[0], recv_sem=s_recv.at[way],
                device_id=(me, owner), device_id_type=MESH,
            ).start()

    some = pl.ds(0, members - 1)

    def advance(box, state):
        s, d = state
        e = unpack_rows(box[decay_rows, :])
        return s * e + box[state_rows, :].astype(F32), d * e

    nothing = (jnp.zeros((breadth, LANES), F32), jnp.ones((1, LANES), F32))

    def scan(p):
        state = nothing
        for j in range(members):
            before[p, j] = state[0]
            before_dec[p, j] = state[1]
            state = advance(inbox.at[p, j], state)
        gout[p, state_rows, :] = state[0].astype(BF16)
        gout[p, decay_rows, :] = pack_rows(state[1])

    def group_copy(p, g, slot):
        return pltpu.make_async_remote_copy(
            src_ref=gout.at[p], dst_ref=gin.at[p, slot],
            send_sem=g_send.at[0], recv_sem=g_recv.at[p, slot],
            device_id=above(g), device_id_type=MESH,
        )

    def send_group(p):
        def body(i, c):
            group_copy(p, groups - 1 - i, group).start()
            return c

        lax.fori_loop(0, groups - 1 - group, body, 0)

    def take_group(p):
        def body(g, state):
            group_copy(p, g, g).wait_recv()
            return advance(gin.at[p, g], state)

        return lax.fori_loop(0, group, body, nothing)[0]

    def send_carry(way, came):
        p = way * cores + core
        for j in range(members):
            cbox[way, j] = (came * before_dec[way, j] + before[way, j]).astype(BF16)
        for q in peers:
            pltpu.make_async_remote_copy(
                src_ref=cbox.at[way, q], dst_ref=carry.at[p, chip],
                send_sem=c_send.at[0], recv_sem=c_recv.at[p // ways],
                device_id=place(q), device_id_type=MESH,
            ).start()
        carry[p, chip] = cbox[way, r]

    with jax.named_scope("decays0"):
        decays(0)
    with jax.named_scope("barrier"):
        pl.semaphore_wait(barrier, members - 1 + group)
        send_states(0)
        for i in range(2):
            small_copy(i, core).start()
        send_weight(0, 1)

        def here(g, c):
            pl.semaphore_signal(ready, inc=1, device_id=above(g), device_id_type=MESH)
            return c

        lax.fori_loop(0, group, here, 0)
        for k in range(chunks):
            pltpu.make_async_copy(columns(k), weight(core, k), weight_sem(k)).start()
    for p in range(1, parts):
        piece = p if p < ways else ways - 1 + p // ways
        if p < ways or p % ways == 0:
            with jax.named_scope("in1"):
                wait_all(held.at[pl.ds(0, 3), :, pieces[piece]], in_sem.at[piece + 2])
        with jax.named_scope("decays1"):
            decays(p)
        with jax.named_scope("send1"):
            send_states(p)
            send_weight(p, p + 1 if p < parts - 1 else p + 2)
    sent = parts + 1

    with jax.named_scope("in2"):
        wait_all(held.at[pl.ds(3, 2)], in_sem.at[len(pieces) + 2])
        for i in range(2):
            small_local[i].wait()
            small_copy(i, other).wait_recv()
        for h in range(width // breadth):
            reward_row[:, pl.ds(h * breadth, breadth)] = rewards[
                h * breadth // half, pl.ds(h % (half // breadth), 1), :
            ]

    units = [(p, t) for p in range(parts) for t in range(quads)]
    done = 0

    def some_within(count):
        nonlocal done
        for at in range(done, min(done + count, len(units)), 2):
            with jax.named_scope("within"):
                within(units[at : at + 2])
        done += count

    some_within(4)
    for p in range(ways):
        with jax.named_scope("wait_states"):
            wait_all(inbox.at[p, some], s_recv.at[p])
        with jax.named_scope("scan"):
            scan(p)
        with jax.named_scope("send_group"):
            if p == 0:
                @pl.when(group < groups - 1)
                def _():
                    pl.semaphore_wait(ready, groups - 1 - group)

            send_group(p)

            @pl.when(group == 0)
            def _():
                send_carry(p, nothing[0])
                send_weight(sent + 2 * p, sent + 2 * p + 2 if p < ways - 1 else 2 * chunks)

            @pl.when(group > 0)
            def _():
                send_weight(sent + 2 * p, sent + 2 * p + 2)

        some_within(2 if p < ways - 1 else len(units))
    with jax.named_scope("take_group"):
        @pl.when(group > 0)
        def _():
            for p in range(ways):
                at = sent + 2 * ways + p
                send_carry(p, take_group(p))
                send_weight(at, at + 1 if p < ways - 1 else 2 * chunks)

    def project(k, first, last):
        at = pl.ds(k * CHUNK, CHUNK)
        total = partial[:, at] if first > 0 else None
        for p in range(first, last):
            term = dot(gated[:, pl.ds(p * half, half)], weight(p, k)[...])
            total = term if total is None else total + term
        if last < cores:
            partial[:, at] = total
        else:
            out_ref[:, at] = total.astype(BF16)

    early = parts - ways
    with jax.named_scope("wait_weight"):
        wait_all(weight_head.at[:, pl.ds(0, lead)], w_sem.at[0])
    with jax.named_scope("wait_carry"):
        for side in range(cores - 1):
            wait_all(cbox.at[0, some], c_recv.at[side])
    with jax.named_scope("finish"):
        finish(range(early))
        for k in range(lead - 2):
            project(k, 0, cores - 1)
    with jax.named_scope("wait_weight"):
        wait_all(weight_head.at[:, pl.ds(lead, split - lead)], w_sem.at[1])
    with jax.named_scope("wait_carry"):
        wait_all(cbox.at[0, some], c_recv.at[cores - 1])
    with jax.named_scope("project"):
        finish(range(early, parts), range(lead - 2, lead))
        for k in range(lead):
            project(k, cores - 1, cores)
        for k in range(lead, split):
            project(k, 0, cores)
    with jax.named_scope("wait_weight"):
        wait_all(weight_tail, w_sem.at[2])

    def drain_groups(g):
        wait_all(gin.at[:, pl.ds(0, groups - 1 - g)], g_send.at[0])

    with jax.named_scope("drain"):
        for g in range(groups - 1):
            pl.when(group == g)(functools.partial(drain_groups, g))
        wait_all(inbox.at[:, some], s_send.at[0])
        wait_all(cbox.at[:, some], c_send.at[0])
        wait_all(map_hbm, w_send.at[0])
        for i in range(2):
            small_copy(i, core).wait_send()


def tail_kernel(done_ref, gated_ref, weight_ref, out_hbm, last, sem):
    cores, tail, half, chunk = weight_ref.shape
    done = done_ref.shape[1]
    copies = [pltpu.make_async_copy(done_ref, out_hbm.at[:, pl.ds(0, done)], sem.at[0])]
    copies[0].start()
    for k in range(tail):
        total = dot(gated_ref[:, pl.ds(0, half)], weight_ref[0, k])
        for p in range(1, cores):
            total = total + dot(gated_ref[:, pl.ds(p * half, half)], weight_ref[p, k])
        last[k] = total.astype(BF16)
        at = pl.ds(done + k * chunk, chunk)
        copies.append(pltpu.make_async_copy(last.at[k], out_hbm.at[:, at], sem.at[k + 1]))
        copies[-1].start()
    for copy in copies:
        copy.wait()


def shards(n, cores, rec, key, val, fade, gate, reward, gain, mapping):
    tokens, width = rec.shape
    breadth = reward.shape[1]
    half, depth = mapping.shape
    ways = WAYS
    parts = ways * cores
    blocks, chunks, span = tokens // BLOCK, depth // CHUNK, width // parts // LANES
    members, groups = span * cores, n // span
    boxed = breadth + EXTRA
    dma = pltpu.SemaphoreType.DMA
    narrow = pltpu.VMEM((tokens, width), BF16)
    wide = pltpu.VMEM((tokens, width), F32)
    tail = min(TAIL, chunks - LEAD)
    split = chunks - tail
    vmem = pl.BlockSpec(memory_space=pltpu.VMEM)
    done, gated, last = pl.pallas_call(
        functools.partial(kernel, n, cores, breadth),
        out_shape=(
            pltpu.VMEM((tokens, split * CHUNK), BF16),
            pltpu.VMEM((tokens, width), BF16),
            pltpu.VMEM((cores, tail, half, CHUNK), BF16),
        ),
        in_specs=[pl.BlockSpec(memory_space=pl.ANY)] * 8,
        out_specs=(vmem,) * 3,
        scratch_shapes=[
            pltpu.VMEM((5, tokens, width), BF16),
            pltpu.VMEM((cores,) + reward.shape, F32),
            pltpu.VMEM((cores, 1, half), F32),
            pltpu.VMEM((cores, split, half, CHUNK), BF16),
            pltpu.VMEM((1, width), F32),
            wide, narrow, narrow, narrow, wide, wide,
            pltpu.VMEM((parts, max(blocks - 1, 1), span, breadth, LANES), BF16),
            pltpu.VMEM((blocks, 1, width), F32),
            pltpu.VMEM((blocks, 1, width), F32),
            pltpu.VMEM((parts, span, boxed, LANES), BF16),
            pltpu.VMEM((ways, members, boxed, LANES), BF16),
            pltpu.VMEM((ways, members, breadth, LANES), F32),
            pltpu.VMEM((ways, members, 1, LANES), F32),
            pltpu.VMEM((ways, boxed, LANES), BF16),
            pltpu.VMEM((ways, groups, boxed, LANES), BF16),
            pltpu.VMEM((ways, members, breadth, LANES), BF16),
            pltpu.VMEM((parts, span, breadth, LANES), BF16),
            pltpu.VMEM((tokens, LEAD * CHUNK), F32),
            dma((ways + cores + 2,)), dma((2,)), dma((2,)), dma((2,)),
            dma((3,)), dma((1,)),
            dma((1,)), dma((ways,)), dma((1,)), dma((ways, groups)),
            dma((1,)), dma((cores,)), pltpu.SemaphoreType.REGULAR,
        ],
        compiler_params=pltpu.CompilerParams(
            collective_id=0, has_side_effects=True, vmem_limit_bytes=55 * 2**20
        ),
    )(rec, key, val, fade, gate, reward, gain.reshape(1, -1), mapping)
    return pl.pallas_call(
        tail_kernel,
        out_shape=jax.ShapeDtypeStruct((tokens, depth), BF16),
        in_specs=[vmem] * 3,
        out_specs=pl.BlockSpec(memory_space=pl.ANY),
        scratch_shapes=[pltpu.VMEM((tail, tokens, CHUNK), BF16), dma((tail + 1,))],
        compiler_params=pltpu.CompilerParams(vmem_limit_bytes=16 * 2**20),
    )(done, gated, last)


def solution(mesh):
    tokens = P(("seq", "head"), None)
    placed = (tokens,) * 5 + (P("head", None), P("head"), P("head", None))
    return jax.shard_map(
        functools.partial(shards, mesh.shape["seq"], mesh.shape["head"]),
        mesh=mesh, in_specs=placed, out_specs=tokens, check_vma=False,
    )
```

```python
import functools

import jax
import jax.numpy as jnp
from jax import lax
from jax.experimental import pallas as pl
from jax.experimental.pallas import tpu as pltpu
from jax.sharding import PartitionSpec as P

BLOCK = 128
LANES = 128
QUAD = 256
CHUNK = 512
LEAD = 4
WAYS = 2
TAIL = 2
EXTRA = 8
EPS = 1e-05
MESH = pl.DeviceIdType.MESH
F32 = jnp.float32
BF16 = jnp.bfloat16


def dot(a, b):
    return jnp.dot(a, b, preferred_element_type=F32)


def dot_nt(a, b):
    return lax.dot_general(a, b, (((1,), (1,)), ((), ())), preferred_element_type=F32)


def dot_tn(a, b):
    return lax.dot_general(a, b, (((0,), (0,)), ((), ())), preferred_element_type=F32)


def split_heads(x, low):
    zero = jnp.zeros_like(x)
    return jnp.concatenate([jnp.where(low, x, zero), jnp.where(low, zero, x)], axis=0)


def flip(r, i, members):
    q, bit = 0, 1
    while bit < members:
        q = q + bit * (((r // bit) % 2 + (i // bit) % 2) % 2)
        bit *= 2
    return q


def kernel(
    n, cores, breadth,
    rec_hbm, key_hbm, val_hbm, fade_hbm, gate_hbm, reward_hbm, gain_hbm, map_hbm,
    out_ref, gated, weight_tail,
    held, rewards, gains, weight_head,
    reward_row, cumx, key_mid, centred, recs, local_out, swish, entering, pref_row, mid_row,
    outbox, inbox, before, before_dec, gout, gin, cbox, carry, partial,
    in_sem, p_local, p_send, p_recv, w_sem, w_send,
    s_send, s_recv, g_send, g_recv, c_send, c_recv, ready,
):
    me, core = lax.axis_index("seq"), lax.axis_index("head")
    other = 1 - core
    tokens, width = held.shape[1:]
    half = width // cores
    parts, span = outbox.shape[:2]
    owner = cores - 1
    ways = parts // cores
    lane = width // parts
    blocks, quads = tokens // BLOCK, lane // QUAD
    split = weight_head.shape[1]
    chunks = split + weight_tail.shape[1]
    lead = min(LEAD, chunks)
    members = span * cores
    groups = n // span
    group = me // span
    chip = me % span
    r = chip * cores + core
    peers = [flip(r, i, members) for i in range(members - 1, 0, -1)]
    chips = [flip(chip, i, span) for i in range(span - 1, -1, -1)]
    fade, key, val, rec, gate = (held.at[i] for i in range(5))
    sources = (fade_hbm, key_hbm, val_hbm, rec_hbm, gate_hbm)

    def place(q):
        return (group * span + q // cores, q % cores)

    def above(g):
        return (g * span + me % span, core)

    barrier = pltpu.get_barrier_semaphore()
    for q in peers:
        pl.semaphore_signal(barrier, inc=1, device_id=place(q), device_id_type=MESH)

    pieces = [pl.ds(side * half, half) for side in range(cores)]
    for piece, at in enumerate(pieces):
        for i in (0, 2, 1):
            sem = in_sem.at[i if piece == 0 else piece + 2]
            pltpu.make_async_copy(sources[i].at[:, at], held.at[i, :, at], sem).start()

    def greet_above(g, c):
        pl.semaphore_signal(barrier, inc=1, device_id=above(g), device_id_type=MESH)
        return c

    lax.fori_loop(group + 1, groups, greet_above, 0)
    for i in range(3, 5):
        pltpu.make_async_copy(sources[i], held.at[i], in_sem.at[len(pieces) + 2]).start()

    def wait_all(ref, sem):
        pltpu.make_async_copy(ref, ref, sem).wait()

    small = ((reward_hbm, rewards), (gain_hbm, gains))
    small_local = [
        pltpu.make_async_copy(src, dst.at[core], p_local.at[i]) for i, (src, dst) in enumerate(small)
    ]

    def small_copy(i, side):
        src, dst = small[i]
        return pltpu.make_async_remote_copy(
            src_ref=src, dst_ref=dst.at[side], send_sem=p_send.at[i], recv_sem=p_recv.at[i],
            device_id=(me, other), device_id_type=MESH,
        )

    for copy in small_local:
        copy.start()

    def columns(k):
        return map_hbm.at[:, pl.ds(k * CHUNK, CHUNK)]

    def weight(side, k):
        return weight_head.at[side, k] if k < split else weight_tail.at[side, k - split]

    def weight_sem(k):
        return w_sem.at[0 if k < lead else 1 if k < split else 2]

    def send_weight(start, stop=2 * chunks):
        for piece in range(start, min(stop, 2 * chunks)):
            k, rows = piece // 2, pl.ds(piece % 2 * (half // 2), half // 2)
            pltpu.make_async_remote_copy(
                src_ref=map_hbm.at[rows, pl.ds(k * CHUNK, CHUNK)], dst_ref=weight(core, k).at[rows],
                send_sem=w_send.at[0], recv_sem=weight_sem(k),
                device_id=(me, other), device_id_type=MESH,
            ).start()

    t_id = lax.broadcasted_iota(jnp.int32, (BLOCK, 2 * BLOCK), 0)
    s_id = lax.rem(lax.broadcasted_iota(jnp.int32, (BLOCK, 2 * BLOCK), 1), BLOCK)
    incl = jnp.where(t_id >= s_id, 1.0, 0.0).astype(BF16)
    low = lax.broadcasted_iota(jnp.int32, (BLOCK, LANES), 1) < breadth
    low_s = lax.broadcasted_iota(jnp.int32, (breadth, LANES), 1) < breadth
    row_x = lax.broadcasted_iota(jnp.int32, (EXTRA, LANES), 0)
    head_i = lax.broadcasted_iota(jnp.int32, (QUAD, QUAD), 0)
    head_j = lax.broadcasted_iota(jnp.int32, (QUAD, QUAD), 1)
    same, equal = head_i // breadth == head_j // breadth, head_i == head_j
    means = jnp.where(same, 1.0 / breadth, 0.0).astype(BF16)
    centre = (jnp.where(equal, 1.0, 0.0) - jnp.where(same, 1.0 / breadth, 0.0)).astype(BF16)
    ones = jnp.where(same, 1.0, 0.0).astype(BF16)
    state_rows, decay_rows = pl.ds(0, breadth), pl.ds(breadth, EXTRA)
    cuts = [slice(j * LANES, (j + 1) * LANES) for j in range(2)]

    def pack_rows(dec):
        hi = dec.astype(BF16).astype(F32)
        return jnp.where(row_x == 0, hi, jnp.where(row_x == 1, dec - hi, 0.0)).astype(BF16)

    def unpack_rows(x):
        x = x.astype(F32)
        return x[0:1] + x[1:2]

    def quad_lanes(p, t):
        return pl.ds(p * lane + t * QUAD, QUAD)

    def arrive(side, i):
        if side == 0:
            wait_all(held.at[i, :, pieces[0]], in_sem.at[i])

    def decays(side):
        turns = range(ways * quads)
        cells = [(t, b) for t in turns for b in range(blocks)]
        p = side * ways
        cums, vbs, kms, products = {}, {}, {}, {}
        arrive(side, 0)
        for t, b in cells:
            at, lanes = pl.ds(b * BLOCK, BLOCK), quad_lanes(p, t)
            log_decay = -jnp.exp(fade[at, lanes].astype(F32))
            hi = log_decay.astype(BF16)
            lo = (log_decay - hi.astype(F32)).astype(BF16)
            cum = dot(incl, jnp.concatenate([hi, lo], axis=0))
            cumx[at, lanes] = cum - log_decay
            cums[t, b] = cum
        arrive(side, 2)
        for t, b in cells:
            at, lanes = pl.ds(b * BLOCK, BLOCK), quad_lanes(p, t)
            vbs[t, b] = dot(val[at, lanes], centre).astype(BF16)
            centred[at, lanes] = vbs[t, b]
        arrive(side, 1)
        for t, b in cells:
            at, lanes = pl.ds(b * BLOCK, BLOCK), quad_lanes(p, t)
            mid = cums[t, b][BLOCK // 2 - 1 : BLOCK // 2]
            kms[t, b] = (key[at, lanes].astype(F32) * jnp.exp(mid - cums[t, b])).astype(BF16)
            key_mid[at, lanes] = kms[t, b]
            mid_row[b, :, lanes] = mid
        for t, b in cells:
            for j, cut in enumerate(cuts):
                products[t, b, j] = dot_tn(vbs[t, b][:, cut], kms[t, b][:, cut])
        for t in turns:
            lanes = quad_lanes(p, t)
            states = [jnp.zeros((breadth, LANES), F32) for _ in range(2)]
            pref = jnp.zeros((1, QUAD), F32)
            for b in range(blocks):
                cum = cums[t, b]
                mid, total = cum[BLOCK // 2 - 1 : BLOCK // 2], cum[BLOCK - 1 :]
                end, whole, begin = jnp.exp(total - mid), jnp.exp(total), jnp.exp(mid)
                pref_row[b, :, lanes] = pref
                for j, cut in enumerate(cuts):
                    if b > 0:
                        entering[p + t // quads, b - 1, t % quads * 2 + j] = (states[j] * begin[:, cut]).astype(BF16)
                    product = products[t, b, j]
                    own = jnp.where(low_s, product[:breadth], product[breadth:])
                    states[j] = states[j] * whole[:, cut] + own * end[:, cut]
                pref = pref + total
            gone = jnp.exp(pref)
            for j, cut in enumerate(cuts):
                outbox[p + t // quads, t % quads * 2 + j, state_rows, :] = states[j].astype(BF16)
                outbox[p + t // quads, t % quads * 2 + j, decay_rows, :] = pack_rows(gone[:, cut])

    def within(units):
        cells = [(p, t, b) for p, t in units for b in range(blocks)]
        rms, diags, scored = {}, {}, {}
        for p, t, b in cells:
            at, lanes = pl.ds(b * BLOCK, BLOCK), quad_lanes(p, t)
            cx = cumx[at, lanes]
            rf = rec[at, lanes].astype(F32)
            rms[p, t, b] = (rf * jnp.exp(cx - mid_row[b, :, lanes])).astype(BF16)
            recs[at, lanes] = (rf * jnp.exp(cx + pref_row[b, :, lanes])).astype(BF16)
            own = rf * key[at, lanes].astype(F32) * reward_row[:, lanes]
            diags[p, t, b] = dot(own.astype(BF16), ones)
            kb = key_mid[at, lanes]
            for j, cut in enumerate(cuts):
                scored[p, t, b, j] = dot_nt(rms[p, t, b][:, cut], split_heads(kb[:, cut], low))
        for p, t, b in cells:
            at, lanes = pl.ds(b * BLOCK, BLOCK), quad_lanes(p, t)
            g = gate[at, lanes].astype(F32)
            swish[at, lanes] = g / (1.0 + jnp.exp(-g)) * gains[p * lane // half, :, pl.ds(p * lane % half + t * QUAD, QUAD)]
        for p, t, b in cells:
            at, lanes = pl.ds(b * BLOCK, BLOCK), quad_lanes(p, t)
            vb = centred[at, lanes]
            for j, cut in enumerate(cuts):
                scores = jnp.where(t_id > s_id, scored[p, t, b, j], 0.0).astype(BF16)
                o = dot(scores, split_heads(vb[:, cut], low))
                if b > 0:
                    came = split_heads(entering[p, b - 1, 2 * t + j], low_s)
                    o = o + dot_nt(rms[p, t, b][:, cut], came)
                o = o + diags[p, t, b][:, cut] * vb[:, cut].astype(F32)
                local_out[at, pl.ds(p * lane + t * QUAD + j * LANES, LANES)] = o

    def finish(ps, between=()):
        cells = [(p, t) for p in ps for t in range(quads)]
        states, outs = {}, {}
        for p, t in cells:
            x, y = (split_heads(carry[p, 2 * t + j], low_s) for j in range(2))
            none = jnp.zeros_like(x)
            states[p, t] = jnp.concatenate(
                [jnp.concatenate([x, none], axis=1), jnp.concatenate([none, y], axis=1)], axis=0
            )
        for p, t in cells:
            lanes = quad_lanes(p, t)
            outs[p, t] = local_out[:, lanes] + dot_nt(recs[:, lanes], states[p, t])
        squares = [(outs[cell] * outs[cell]).astype(BF16) for cell in cells]
        variances = dot(jnp.concatenate(squares, axis=0), means)
        for k in between:
            project(k, 0, cores - 1)
        for i, (p, t) in enumerate(cells):
            lanes = quad_lanes(p, t)
            variance = variances[i * tokens : (i + 1) * tokens]
            scale = lax.rsqrt(variance + EPS) * swish[:, lanes]
            gated[:, lanes] = (outs[p, t] * scale).astype(BF16)

    def send_states(p):
        def send(t):
            pltpu.make_async_remote_copy(
                src_ref=outbox.at[p, t], dst_ref=inbox.at[p, r],
                send_sem=s_send.at[0], recv_sem=s_recv.at[p],
                device_id=(group * span + t, owner), device_id_type=MESH,
            ).start()

        for t in chips[:-1]:
            send(t)

        @pl.when(core == owner)
        def _():
            inbox[p, r] = outbox[p, chip]

        @pl.when(core != owner)
        def _():
            send(chip)

    some = pl.ds(0, members - 1)

    def advance(box, state):
        s, d = state
        e = unpack_rows(box[decay_rows, :])
        return s * e + box[state_rows, :].astype(F32), d * e

    nothing = (jnp.zeros((breadth, LANES), F32), jnp.ones((1, LANES), F32))

    def scan(p):
        state = nothing
        for j in range(members):
            before[p, j] = state[0]
            before_dec[p, j] = state[1]
            state = advance(inbox.at[p, j], state)
        gout[p, state_rows, :] = state[0].astype(BF16)
        gout[p, decay_rows, :] = pack_rows(state[1])

    def group_copy(p, g, slot):
        return pltpu.make_async_remote_copy(
            src_ref=gout.at[p], dst_ref=gin.at[p, slot],
            send_sem=g_send.at[0], recv_sem=g_recv.at[p, slot],
            device_id=above(g), device_id_type=MESH,
        )

    def send_group(p):
        def body(i, c):
            group_copy(p, groups - 1 - i, group).start()
            return c

        lax.fori_loop(0, groups - 1 - group, body, 0)

    def take_group(p):
        def body(g, state):
            group_copy(p, g, g).wait_recv()
            return advance(gin.at[p, g], state)

        return lax.fori_loop(0, group, body, nothing)[0]

    def send_carry(way, came):
        p = way
        for j in range(members):
            cbox[way, j] = (came * before_dec[way, j] + before[way, j]).astype(BF16)
        for q in peers:
            pltpu.make_async_remote_copy(
                src_ref=cbox.at[way, q], dst_ref=carry.at[p, chip],
                send_sem=c_send.at[0], recv_sem=c_recv.at[p // ways],
                device_id=place(q), device_id_type=MESH,
            ).start()
        carry[p, chip] = cbox[way, r]

    with jax.named_scope("decays0"):
        decays(0)
    with jax.named_scope("barrier"):
        pl.semaphore_wait(barrier, members - 1 + group)
        for p in range(ways):
            send_states(p)
        for i in range(2):
            small_copy(i, core).start()
        send_weight(0, 1)

        def here(g, c):
            pl.semaphore_signal(ready, inc=1, device_id=above(g), device_id_type=MESH)
            return c

        @pl.when(core == owner)
        def _():
            lax.fori_loop(0, group, here, 0)

        for k in range(chunks):
            pltpu.make_async_copy(columns(k), weight(core, k), weight_sem(k)).start()
    for side in range(1, cores):
        with jax.named_scope("in1"):
            wait_all(held.at[pl.ds(0, 3), :, pieces[side]], in_sem.at[side + 2])
        with jax.named_scope("decays1"):
            decays(side)
        with jax.named_scope("send1"):
            for p in range(side * ways, side * ways + ways):
                send_states(p)
    sent = 5
    send_weight(1, sent)

    @pl.when(core != owner)
    def _():
        send_weight(sent)

    with jax.named_scope("in2"):
        wait_all(held.at[pl.ds(3, 2)], in_sem.at[len(pieces) + 2])
        for i in range(2):
            small_local[i].wait()
            small_copy(i, other).wait_recv()
        for h in range(width // breadth):
            reward_row[:, pl.ds(h * breadth, breadth)] = rewards[
                h * breadth // half, pl.ds(h % (half // breadth), 1), :
            ]

    units = [(p, t) for p in range(parts) for t in range(quads)]
    done = 0

    def some_within(count):
        nonlocal done
        for at in range(done, min(done + count, len(units)), 2):
            with jax.named_scope("within"):
                within(units[at : at + 2])
        done += count

    some_within(4)
    for p in range(parts):
        @pl.when(core == owner)
        def _():
            with jax.named_scope("wait_states"):
                wait_all(inbox.at[p, some], s_recv.at[p])
            with jax.named_scope("scan"):
                scan(p)
            if p == 0:
                @pl.when(group < groups - 1)
                def _():
                    pl.semaphore_wait(ready, groups - 1 - group)

            send_group(p)

            @pl.when(group == 0)
            def _():
                send_carry(p, nothing[0])

            send_weight(sent + p, sent + p + 1)

        if p % 2:
            some_within(2)
    sent += parts

    @pl.when(core == owner)
    def _():
        @pl.when(group > 0)
        def _():
            for p in range(parts):
                with jax.named_scope("take_group"):
                    came = take_group(p)
                with jax.named_scope("send_carry"):
                    send_carry(p, came)

        send_weight(sent)

    def project(k, first, last):
        at = pl.ds(k * CHUNK, CHUNK)
        total = partial[:, at] if first > 0 else None
        for p in range(first, last):
            term = dot(gated[:, pl.ds(p * half, half)], weight(p, k)[...])
            total = term if total is None else total + term
        if last < cores:
            partial[:, at] = total
        else:
            out_ref[:, at] = total.astype(BF16)

    early = parts - ways

    def wait_carry(side):
        @pl.when(core == owner)
        def _():
            wait_all(carry.at[pl.ds(0, ways), pl.ds(0, span - 1)], c_recv.at[side])

        @pl.when(core != owner)
        def _():
            wait_all(carry.at[pl.ds(0, ways)], c_recv.at[side])

    with jax.named_scope("wait_weight"):
        wait_all(weight_head.at[:, pl.ds(0, lead)], w_sem.at[0])
    with jax.named_scope("wait_carry"):
        for side in range(cores - 1):
            wait_carry(side)
    with jax.named_scope("finish"):
        finish(range(early))
        for k in range(lead - 2):
            project(k, 0, cores - 1)
    with jax.named_scope("wait_weight"):
        wait_all(weight_head.at[:, pl.ds(lead, split - lead)], w_sem.at[1])
    with jax.named_scope("wait_carry"):
        wait_carry(cores - 1)
    with jax.named_scope("project"):
        finish(range(early, parts), range(lead - 2, lead))
        for k in range(lead):
            project(k, cores - 1, cores)
        for k in range(lead, split):
            project(k, 0, cores)
    with jax.named_scope("wait_weight"):
        wait_all(weight_tail, w_sem.at[2])

    def drain_groups(g):
        wait_all(gin.at[:, pl.ds(0, groups - 1 - g)], g_send.at[0])

    with jax.named_scope("drain"):
        @pl.when(core == owner)
        def _():
            for g in range(groups - 1):
                pl.when(group == g)(functools.partial(drain_groups, g))
            wait_all(outbox.at[:, pl.ds(0, span - 1)], s_send.at[0])
            wait_all(cbox.at[:, some], c_send.at[0])

        @pl.when(core != owner)
        def _():
            wait_all(outbox, s_send.at[0])

        wait_all(map_hbm, w_send.at[0])
        for i in range(2):
            small_copy(i, core).wait_send()


def tail_kernel(done_ref, gated_ref, weight_ref, out_hbm, last, sem):
    cores, tail, half, chunk = weight_ref.shape
    done = done_ref.shape[1]
    copies = [pltpu.make_async_copy(done_ref, out_hbm.at[:, pl.ds(0, done)], sem.at[0])]
    copies[0].start()
    for k in range(tail):
        total = dot(gated_ref[:, pl.ds(0, half)], weight_ref[0, k])
        for p in range(1, cores):
            total = total + dot(gated_ref[:, pl.ds(p * half, half)], weight_ref[p, k])
        last[k] = total.astype(BF16)
        at = pl.ds(done + k * chunk, chunk)
        copies.append(pltpu.make_async_copy(last.at[k], out_hbm.at[:, at], sem.at[k + 1]))
        copies[-1].start()
    for copy in copies:
        copy.wait()


def shards(n, cores, rec, key, val, fade, gate, reward, gain, mapping):
    tokens, width = rec.shape
    breadth = reward.shape[1]
    half, depth = mapping.shape
    ways = WAYS
    parts = ways * cores
    blocks, chunks, span = tokens // BLOCK, depth // CHUNK, width // parts // LANES
    members, groups = span * cores, n // span
    boxed = breadth + EXTRA
    dma = pltpu.SemaphoreType.DMA
    narrow = pltpu.VMEM((tokens, width), BF16)
    wide = pltpu.VMEM((tokens, width), F32)
    tail = min(TAIL, chunks - LEAD)
    split = chunks - tail
    vmem = pl.BlockSpec(memory_space=pltpu.VMEM)
    done, gated, last = pl.pallas_call(
        functools.partial(kernel, n, cores, breadth),
        out_shape=(
            pltpu.VMEM((tokens, split * CHUNK), BF16),
            pltpu.VMEM((tokens, width), BF16),
            pltpu.VMEM((cores, tail, half, CHUNK), BF16),
        ),
        in_specs=[pl.BlockSpec(memory_space=pl.ANY)] * 8,
        out_specs=(vmem,) * 3,
        scratch_shapes=[
            pltpu.VMEM((5, tokens, width), BF16),
            pltpu.VMEM((cores,) + reward.shape, F32),
            pltpu.VMEM((cores, 1, half), F32),
            pltpu.VMEM((cores, split, half, CHUNK), BF16),
            pltpu.VMEM((1, width), F32),
            wide, narrow, narrow, narrow, wide, wide,
            pltpu.VMEM((parts, max(blocks - 1, 1), span, breadth, LANES), BF16),
            pltpu.VMEM((blocks, 1, width), F32),
            pltpu.VMEM((blocks, 1, width), F32),
            pltpu.VMEM((parts, span, boxed, LANES), BF16),
            pltpu.VMEM((parts, members, boxed, LANES), BF16),
            pltpu.VMEM((parts, members, breadth, LANES), F32),
            pltpu.VMEM((parts, members, 1, LANES), F32),
            pltpu.VMEM((parts, boxed, LANES), BF16),
            pltpu.VMEM((parts, groups, boxed, LANES), BF16),
            pltpu.VMEM((parts, members, breadth, LANES), BF16),
            pltpu.VMEM((parts, span, breadth, LANES), BF16),
            pltpu.VMEM((tokens, LEAD * CHUNK), F32),
            dma((cores + 3,)), dma((2,)), dma((2,)), dma((2,)),
            dma((3,)), dma((1,)),
            dma((1,)), dma((parts,)), dma((1,)), dma((parts, groups)),
            dma((1,)), dma((cores,)), pltpu.SemaphoreType.REGULAR,
        ],
        compiler_params=pltpu.CompilerParams(
            collective_id=0, has_side_effects=True, vmem_limit_bytes=55 * 2**20
        ),
    )(rec, key, val, fade, gate, reward, gain.reshape(1, -1), mapping)
    return pl.pallas_call(
        tail_kernel,
        out_shape=jax.ShapeDtypeStruct((tokens, depth), BF16),
        in_specs=[vmem] * 3,
        out_specs=pl.BlockSpec(memory_space=pl.ANY),
        scratch_shapes=[pltpu.VMEM((tail, tokens, CHUNK), BF16), dma((tail + 1,))],
        compiler_params=pltpu.CompilerParams(vmem_limit_bytes=16 * 2**20),
    )(done, gated, last)


def solution(mesh):
    tokens = P(("seq", "head"), None)
    placed = (tokens,) * 5 + (P("head", None), P("head"), P("head", None))
    return jax.shard_map(
        functools.partial(shards, mesh.shape["seq"], mesh.shape["head"]),
        mesh=mesh, in_specs=placed, out_specs=tokens, check_vma=False,
    )
```

```python
import functools

import jax
import jax.numpy as jnp
from jax import lax
from jax.experimental import pallas as pl
from jax.experimental.pallas import tpu as pltpu
from jax.sharding import PartitionSpec as P

BLOCK = 128
LANES = 128
QUAD = 256
CHUNK = 512
LEAD = 4
WAYS = 2
TAIL = 1
EXTRA = 8
EPS = 1e-05
MESH = pl.DeviceIdType.MESH
F32 = jnp.float32
BF16 = jnp.bfloat16


def dot(a, b):
    return jnp.dot(a, b, preferred_element_type=F32)


def dot_nt(a, b):
    return lax.dot_general(a, b, (((1,), (1,)), ((), ())), preferred_element_type=F32)


def dot_tn(a, b):
    return lax.dot_general(a, b, (((0,), (0,)), ((), ())), preferred_element_type=F32)


def split_heads(x, low):
    zero = jnp.zeros_like(x)
    return jnp.concatenate([jnp.where(low, x, zero), jnp.where(low, zero, x)], axis=0)


def flip(r, i, members):
    q, bit = 0, 1
    while bit < members:
        q = q + bit * (((r // bit) % 2 + (i // bit) % 2) % 2)
        bit *= 2
    return q


def kernel(
    n, cores, breadth,
    rec_hbm, key_hbm, val_hbm, fade_hbm, gate_hbm, reward_hbm, gain_hbm, map_hbm,
    out_ref, gated, weight_tail,
    held, rewards, gains, weight_head,
    reward_row, cumx, key_mid, centred, recs, local_out, swish, entering, pref_row, mid_row,
    outbox, inbox, before, before_dec, gout, gin, cbox, carry, partial,
    in_sem, p_local, p_send, p_recv, w_sem, w_send,
    s_send, s_recv, g_send, g_recv, c_send, c_recv, ready,
):
    me, core = lax.axis_index("seq"), lax.axis_index("head")
    other = 1 - core
    tokens, width = held.shape[1:]
    half = width // cores
    parts, span = outbox.shape[:2]
    owner = cores - 1
    ways = parts // cores
    lane = width // parts
    blocks, quads = tokens // BLOCK, lane // QUAD
    split = weight_head.shape[1]
    chunks = split + weight_tail.shape[1]
    lead = min(LEAD, chunks)
    members = span * cores
    groups = n // span
    group = me // span
    chip = me % span
    r = chip * cores + core
    peers = [flip(r, i, members) for i in range(members - 1, 0, -1)]
    chips = [flip(chip, i, span) for i in range(span - 1, -1, -1)]
    fade, key, val, rec, gate = (held.at[i] for i in range(5))
    sources = (fade_hbm, key_hbm, val_hbm, rec_hbm, gate_hbm)

    def place(q):
        return (group * span + q // cores, q % cores)

    def above(g):
        return (g * span + me % span, core)

    barrier = pltpu.get_barrier_semaphore()
    for q in peers:
        pl.semaphore_signal(barrier, inc=1, device_id=place(q), device_id_type=MESH)

    pieces = [pl.ds(side * half, half) for side in range(cores)]
    for piece, at in enumerate(pieces):
        for i in (0, 2, 1):
            sem = in_sem.at[i if piece == 0 else piece + 2]
            pltpu.make_async_copy(sources[i].at[:, at], held.at[i, :, at], sem).start()

    def greet_above(g, c):
        pl.semaphore_signal(barrier, inc=1, device_id=above(g), device_id_type=MESH)
        return c

    lax.fori_loop(group + 1, groups, greet_above, 0)
    for i in range(3, 5):
        pltpu.make_async_copy(sources[i], held.at[i], in_sem.at[len(pieces) + 2]).start()

    def wait_all(ref, sem):
        pltpu.make_async_copy(ref, ref, sem).wait()

    small = ((reward_hbm, rewards), (gain_hbm, gains))
    small_local = [
        pltpu.make_async_copy(src, dst.at[core], p_local.at[i]) for i, (src, dst) in enumerate(small)
    ]

    def small_copy(i, side):
        src, dst = small[i]
        return pltpu.make_async_remote_copy(
            src_ref=src, dst_ref=dst.at[side], send_sem=p_send.at[i], recv_sem=p_recv.at[i],
            device_id=(me, other), device_id_type=MESH,
        )

    for copy in small_local:
        copy.start()

    def columns(k):
        return map_hbm.at[:, pl.ds(k * CHUNK, CHUNK)]

    def weight(side, k):
        return weight_head.at[side, k] if k < split else weight_tail.at[side, k - split]

    def weight_sem(k):
        return w_sem.at[0 if k < lead else 1 if k < split else 2]

    def send_weight(start, stop=2 * chunks):
        for piece in range(start, min(stop, 2 * chunks)):
            k, rows = piece // 2, pl.ds(piece % 2 * (half // 2), half // 2)
            pltpu.make_async_remote_copy(
                src_ref=map_hbm.at[rows, pl.ds(k * CHUNK, CHUNK)], dst_ref=weight(core, k).at[rows],
                send_sem=w_send.at[0], recv_sem=weight_sem(k),
                device_id=(me, other), device_id_type=MESH,
            ).start()

    t_id = lax.broadcasted_iota(jnp.int32, (BLOCK, 2 * BLOCK), 0)
    s_id = lax.rem(lax.broadcasted_iota(jnp.int32, (BLOCK, 2 * BLOCK), 1), BLOCK)
    incl = jnp.where(t_id >= s_id, 1.0, 0.0).astype(BF16)
    low = lax.broadcasted_iota(jnp.int32, (BLOCK, LANES), 1) < breadth
    low_s = lax.broadcasted_iota(jnp.int32, (breadth, LANES), 1) < breadth
    row_x = lax.broadcasted_iota(jnp.int32, (EXTRA, LANES), 0)
    head_i = lax.broadcasted_iota(jnp.int32, (QUAD, QUAD), 0)
    head_j = lax.broadcasted_iota(jnp.int32, (QUAD, QUAD), 1)
    same, equal = head_i // breadth == head_j // breadth, head_i == head_j
    means = jnp.where(same, 1.0 / breadth, 0.0).astype(BF16)
    centre = (jnp.where(equal, 1.0, 0.0) - jnp.where(same, 1.0 / breadth, 0.0)).astype(BF16)
    ones = jnp.where(same, 1.0, 0.0).astype(BF16)
    state_rows, decay_rows = pl.ds(0, breadth), pl.ds(breadth, EXTRA)
    cuts = [slice(j * LANES, (j + 1) * LANES) for j in range(2)]

    def pack_rows(dec):
        hi = dec.astype(BF16).astype(F32)
        return jnp.where(row_x == 0, hi, jnp.where(row_x == 1, dec - hi, 0.0)).astype(BF16)

    def unpack_rows(x):
        x = x.astype(F32)
        return x[0:1] + x[1:2]

    def quad_lanes(p, t):
        return pl.ds(p * lane + t * QUAD, QUAD)

    def arrive(side, i):
        if side == 0:
            wait_all(held.at[i, :, pieces[0]], in_sem.at[i])

    def decays(side):
        turns = range(ways * quads)
        cells = [(t, b) for t in turns for b in range(blocks)]
        p = side * ways
        cums, vbs, kms, products = {}, {}, {}, {}
        arrive(side, 0)
        for t, b in cells:
            at, lanes = pl.ds(b * BLOCK, BLOCK), quad_lanes(p, t)
            log_decay = -jnp.exp(fade[at, lanes].astype(F32))
            hi = log_decay.astype(BF16)
            lo = (log_decay - hi.astype(F32)).astype(BF16)
            cum = dot(incl, jnp.concatenate([hi, lo], axis=0))
            cumx[at, lanes] = cum - log_decay
            cums[t, b] = cum
        arrive(side, 2)
        for t, b in cells:
            at, lanes = pl.ds(b * BLOCK, BLOCK), quad_lanes(p, t)
            vbs[t, b] = dot(val[at, lanes], centre).astype(BF16)
            centred[at, lanes] = vbs[t, b]
        arrive(side, 1)
        for t, b in cells:
            at, lanes = pl.ds(b * BLOCK, BLOCK), quad_lanes(p, t)
            mid = cums[t, b][BLOCK // 2 - 1 : BLOCK // 2]
            kms[t, b] = (key[at, lanes].astype(F32) * jnp.exp(mid - cums[t, b])).astype(BF16)
            key_mid[at, lanes] = kms[t, b]
            mid_row[b, :, lanes] = mid
        for t, b in cells:
            for j, cut in enumerate(cuts):
                products[t, b, j] = dot_tn(vbs[t, b][:, cut], kms[t, b][:, cut])
        for t in turns:
            lanes = quad_lanes(p, t)
            states = [jnp.zeros((breadth, LANES), F32) for _ in range(2)]
            pref = jnp.zeros((1, QUAD), F32)
            for b in range(blocks):
                cum = cums[t, b]
                mid, total = cum[BLOCK // 2 - 1 : BLOCK // 2], cum[BLOCK - 1 :]
                end, whole, begin = jnp.exp(total - mid), jnp.exp(total), jnp.exp(mid)
                pref_row[b, :, lanes] = pref
                for j, cut in enumerate(cuts):
                    if b > 0:
                        entering[p + t // quads, b - 1, t % quads * 2 + j] = (states[j] * begin[:, cut]).astype(BF16)
                    product = products[t, b, j]
                    own = jnp.where(low_s, product[:breadth], product[breadth:])
                    states[j] = states[j] * whole[:, cut] + own * end[:, cut]
                pref = pref + total
            gone = jnp.exp(pref)
            for j, cut in enumerate(cuts):
                outbox[p + t // quads, t % quads * 2 + j, state_rows, :] = states[j].astype(BF16)
                outbox[p + t // quads, t % quads * 2 + j, decay_rows, :] = pack_rows(gone[:, cut])

    def within(units):
        cells = [(p, t, b) for p, t in units for b in range(blocks)]
        rms, diags, scored = {}, {}, {}
        for p, t, b in cells:
            at, lanes = pl.ds(b * BLOCK, BLOCK), quad_lanes(p, t)
            cx = cumx[at, lanes]
            rf = rec[at, lanes].astype(F32)
            rms[p, t, b] = (rf * jnp.exp(cx - mid_row[b, :, lanes])).astype(BF16)
            recs[at, lanes] = (rf * jnp.exp(cx + pref_row[b, :, lanes])).astype(BF16)
            own = rf * key[at, lanes].astype(F32) * reward_row[:, lanes]
            diags[p, t, b] = dot(own.astype(BF16), ones)
            kb = key_mid[at, lanes]
            for j, cut in enumerate(cuts):
                scored[p, t, b, j] = dot_nt(rms[p, t, b][:, cut], split_heads(kb[:, cut], low))
        for p, t, b in cells:
            at, lanes = pl.ds(b * BLOCK, BLOCK), quad_lanes(p, t)
            g = gate[at, lanes].astype(F32)
            swish[at, lanes] = g / (1.0 + jnp.exp(-g)) * gains[p * lane // half, :, pl.ds(p * lane % half + t * QUAD, QUAD)]
        for p, t, b in cells:
            at, lanes = pl.ds(b * BLOCK, BLOCK), quad_lanes(p, t)
            vb = centred[at, lanes]
            for j, cut in enumerate(cuts):
                scores = jnp.where(t_id > s_id, scored[p, t, b, j], 0.0).astype(BF16)
                o = dot(scores, split_heads(vb[:, cut], low))
                if b > 0:
                    came = split_heads(entering[p, b - 1, 2 * t + j], low_s)
                    o = o + dot_nt(rms[p, t, b][:, cut], came)
                o = o + diags[p, t, b][:, cut] * vb[:, cut].astype(F32)
                local_out[at, pl.ds(p * lane + t * QUAD + j * LANES, LANES)] = o

    def finish(ps, between=()):
        cells = [(p, t) for p in ps for t in range(quads)]
        states, outs = {}, {}
        for p, t in cells:
            x, y = (split_heads(carry[p, 2 * t + j], low_s) for j in range(2))
            none = jnp.zeros_like(x)
            states[p, t] = jnp.concatenate(
                [jnp.concatenate([x, none], axis=1), jnp.concatenate([none, y], axis=1)], axis=0
            )
        for p, t in cells:
            lanes = quad_lanes(p, t)
            outs[p, t] = local_out[:, lanes] + dot_nt(recs[:, lanes], states[p, t])
        squares = [(outs[cell] * outs[cell]).astype(BF16) for cell in cells]
        variances = dot(jnp.concatenate(squares, axis=0), means)
        for k in between:
            project(k, 0, cores - 1)
        for i, (p, t) in enumerate(cells):
            lanes = quad_lanes(p, t)
            variance = variances[i * tokens : (i + 1) * tokens]
            scale = lax.rsqrt(variance + EPS) * swish[:, lanes]
            gated[:, lanes] = (outs[p, t] * scale).astype(BF16)

    def send_states(p):
        def send(t):
            pltpu.make_async_remote_copy(
                src_ref=outbox.at[p, t], dst_ref=inbox.at[p, r],
                send_sem=s_send.at[0], recv_sem=s_recv.at[p],
                device_id=(group * span + t, owner), device_id_type=MESH,
            ).start()

        for t in chips[:-1]:
            send(t)

        @pl.when(core == owner)
        def _():
            inbox[p, r] = outbox[p, chip]

        @pl.when(core != owner)
        def _():
            send(chip)

    some = pl.ds(0, members - 1)

    def advance(box, state):
        s, d = state
        e = unpack_rows(box[decay_rows, :])
        return s * e + box[state_rows, :].astype(F32), d * e

    nothing = (jnp.zeros((breadth, LANES), F32), jnp.ones((1, LANES), F32))

    def scan(p):
        state = nothing
        for j in range(members):
            before[p, j] = state[0]
            before_dec[p, j] = state[1]
            state = advance(inbox.at[p, j], state)
        gout[p, state_rows, :] = state[0].astype(BF16)
        gout[p, decay_rows, :] = pack_rows(state[1])

    def group_copy(p, g, slot):
        return pltpu.make_async_remote_copy(
            src_ref=gout.at[p], dst_ref=gin.at[p, slot],
            send_sem=g_send.at[0], recv_sem=g_recv.at[p, slot],
            device_id=above(g), device_id_type=MESH,
        )

    def send_group(p):
        def body(i, c):
            group_copy(p, groups - 1 - i, group).start()
            return c

        lax.fori_loop(0, groups - 1 - group, body, 0)

    def take_group(p):
        def body(g, state):
            group_copy(p, g, g).wait_recv()
            return advance(gin.at[p, g], state)

        return lax.fori_loop(0, group, body, nothing)[0]

    def send_carry(way, came):
        p = way
        for j in range(members):
            cbox[way, j] = (came * before_dec[way, j] + before[way, j]).astype(BF16)
        for q in peers:
            pltpu.make_async_remote_copy(
                src_ref=cbox.at[way, q], dst_ref=carry.at[p, chip],
                send_sem=c_send.at[0], recv_sem=c_recv.at[p // ways],
                device_id=place(q), device_id_type=MESH,
            ).start()
        carry[p, chip] = cbox[way, r]

    with jax.named_scope("decays0"):
        decays(0)
    with jax.named_scope("barrier"):
        pl.semaphore_wait(barrier, members - 1 + group)
        for p in range(ways):
            send_states(p)
        for i in range(2):
            small_copy(i, core).start()
        send_weight(0, 1)

        def here(g, c):
            pl.semaphore_signal(ready, inc=1, device_id=above(g), device_id_type=MESH)
            return c

        @pl.when(core == owner)
        def _():
            lax.fori_loop(0, group, here, 0)

        for k in range(chunks):
            pltpu.make_async_copy(columns(k), weight(core, k), weight_sem(k)).start()
    for side in range(1, cores):
        with jax.named_scope("in1"):
            wait_all(held.at[pl.ds(0, 3), :, pieces[side]], in_sem.at[side + 2])
        with jax.named_scope("decays1"):
            decays(side)
        with jax.named_scope("send1"):
            for p in range(side * ways, side * ways + ways):
                send_states(p)
    sent = 5
    send_weight(1, sent)

    @pl.when(core != owner)
    def _():
        send_weight(sent)

    with jax.named_scope("in2"):
        wait_all(held.at[pl.ds(3, 2)], in_sem.at[len(pieces) + 2])
        for i in range(2):
            small_local[i].wait()
            small_copy(i, other).wait_recv()
        for h in range(width // breadth):
            reward_row[:, pl.ds(h * breadth, breadth)] = rewards[
                h * breadth // half, pl.ds(h % (half // breadth), 1), :
            ]

    units = [(p, t) for p in range(parts) for t in range(quads)]
    done = 0

    def some_within(count):
        nonlocal done
        for at in range(done, min(done + count, len(units)), 2):
            with jax.named_scope("within"):
                within(units[at : at + 2])
        done += count

    some_within(4)
    for p in range(parts):
        @pl.when(core == owner)
        def _():
            with jax.named_scope("wait_states"):
                wait_all(inbox.at[p, some], s_recv.at[p])
            with jax.named_scope("scan"):
                scan(p)
            if p == 0:
                @pl.when(group < groups - 1)
                def _():
                    pl.semaphore_wait(ready, groups - 1 - group)

            send_group(p)

            @pl.when(group == 0)
            def _():
                send_carry(p, nothing[0])
                send_weight(sent + p, sent + p + 1 if p < parts - 1 else 2 * chunks)

            @pl.when(group > 0)
            def _():
                send_weight(sent + p, sent + p + 1 if p < parts - 1 else sent + p + 2)

        if p % 2:
            some_within(2)
    sent += parts + 1

    @pl.when(core == owner)
    def _():
        @pl.when(group > 0)
        def _():
            for p in range(parts):
                with jax.named_scope("take_group"):
                    came = take_group(p)
                with jax.named_scope("send_carry"):
                    send_carry(p, came)
            send_weight(sent)

    def project(k, first, last):
        at = pl.ds(k * CHUNK, CHUNK)
        total = partial[:, at] if first > 0 else None
        for p in range(first, last):
            term = dot(gated[:, pl.ds(p * half, half)], weight(p, k)[...])
            total = term if total is None else total + term
        if last < cores:
            partial[:, at] = total
        else:
            out_ref[:, at] = total.astype(BF16)

    early = parts - ways

    def wait_carry(side):
        @pl.when(core == owner)
        def _():
            wait_all(carry.at[pl.ds(0, ways), pl.ds(0, span - 1)], c_recv.at[side])

        @pl.when(core != owner)
        def _():
            wait_all(carry.at[pl.ds(0, ways)], c_recv.at[side])

    with jax.named_scope("wait_weight"):
        wait_all(weight_head.at[:, pl.ds(0, lead)], w_sem.at[0])
    with jax.named_scope("wait_carry"):
        for side in range(cores - 1):
            wait_carry(side)
    with jax.named_scope("finish"):
        finish(range(early))
        for k in range(lead - 1):
            project(k, 0, cores - 1)
    with jax.named_scope("wait_carry"):
        wait_carry(cores - 1)
    with jax.named_scope("project"):
        finish(range(early, parts), range(lead - 1, lead))
        for k in range(lead):
            project(k, cores - 1, cores)
    with jax.named_scope("wait_weight"):
        wait_all(weight_head.at[:, pl.ds(lead, split - lead)], w_sem.at[1])
    with jax.named_scope("project_rest"):
        for k in range(lead, split):
            project(k, 0, cores)
    with jax.named_scope("wait_weight"):
        wait_all(weight_tail, w_sem.at[2])

    def drain_groups(g):
        wait_all(gin.at[:, pl.ds(0, groups - 1 - g)], g_send.at[0])

    with jax.named_scope("drain"):
        @pl.when(core == owner)
        def _():
            for g in range(groups - 1):
                pl.when(group == g)(functools.partial(drain_groups, g))
            wait_all(outbox.at[:, pl.ds(0, span - 1)], s_send.at[0])
            wait_all(cbox.at[:, some], c_send.at[0])

        @pl.when(core != owner)
        def _():
            wait_all(outbox, s_send.at[0])

        wait_all(map_hbm, w_send.at[0])
        for i in range(2):
            small_copy(i, core).wait_send()


def tail_kernel(done_ref, gated_ref, weight_ref, out_hbm, last, sem):
    cores, tail, half, chunk = weight_ref.shape
    done = done_ref.shape[1]
    copies = [pltpu.make_async_copy(done_ref, out_hbm.at[:, pl.ds(0, done)], sem.at[0])]
    copies[0].start()
    for k in range(tail):
        total = dot(gated_ref[:, pl.ds(0, half)], weight_ref[0, k])
        for p in range(1, cores):
            total = total + dot(gated_ref[:, pl.ds(p * half, half)], weight_ref[p, k])
        last[k] = total.astype(BF16)
        at = pl.ds(done + k * chunk, chunk)
        copies.append(pltpu.make_async_copy(last.at[k], out_hbm.at[:, at], sem.at[k + 1]))
        copies[-1].start()
    for copy in copies:
        copy.wait()


def shards(n, cores, rec, key, val, fade, gate, reward, gain, mapping):
    tokens, width = rec.shape
    breadth = reward.shape[1]
    half, depth = mapping.shape
    ways = WAYS
    parts = ways * cores
    blocks, chunks, span = tokens // BLOCK, depth // CHUNK, width // parts // LANES
    members, groups = span * cores, n // span
    boxed = breadth + EXTRA
    dma = pltpu.SemaphoreType.DMA
    narrow = pltpu.VMEM((tokens, width), BF16)
    wide = pltpu.VMEM((tokens, width), F32)
    tail = min(TAIL, chunks - LEAD)
    split = chunks - tail
    vmem = pl.BlockSpec(memory_space=pltpu.VMEM)
    done, gated, last = pl.pallas_call(
        functools.partial(kernel, n, cores, breadth),
        out_shape=(
            pltpu.VMEM((tokens, split * CHUNK), BF16),
            pltpu.VMEM((tokens, width), BF16),
            pltpu.VMEM((cores, tail, half, CHUNK), BF16),
        ),
        in_specs=[pl.BlockSpec(memory_space=pl.ANY)] * 8,
        out_specs=(vmem,) * 3,
        scratch_shapes=[
            pltpu.VMEM((5, tokens, width), BF16),
            pltpu.VMEM((cores,) + reward.shape, F32),
            pltpu.VMEM((cores, 1, half), F32),
            pltpu.VMEM((cores, split, half, CHUNK), BF16),
            pltpu.VMEM((1, width), F32),
            wide, narrow, narrow, narrow, wide, wide,
            pltpu.VMEM((parts, max(blocks - 1, 1), span, breadth, LANES), BF16),
            pltpu.VMEM((blocks, 1, width), F32),
            pltpu.VMEM((blocks, 1, width), F32),
            pltpu.VMEM((parts, span, boxed, LANES), BF16),
            pltpu.VMEM((parts, members, boxed, LANES), BF16),
            pltpu.VMEM((parts, members, breadth, LANES), F32),
            pltpu.VMEM((parts, members, 1, LANES), F32),
            pltpu.VMEM((parts, boxed, LANES), BF16),
            pltpu.VMEM((parts, groups, boxed, LANES), BF16),
            pltpu.VMEM((parts, members, breadth, LANES), BF16),
            pltpu.VMEM((parts, span, breadth, LANES), BF16),
            pltpu.VMEM((tokens, LEAD * CHUNK), F32),
            dma((cores + 3,)), dma((2,)), dma((2,)), dma((2,)),
            dma((3,)), dma((1,)),
            dma((1,)), dma((parts,)), dma((1,)), dma((parts, groups)),
            dma((1,)), dma((cores,)), pltpu.SemaphoreType.REGULAR,
        ],
        compiler_params=pltpu.CompilerParams(
            collective_id=0, has_side_effects=True, vmem_limit_bytes=55 * 2**20
        ),
    )(rec, key, val, fade, gate, reward, gain.reshape(1, -1), mapping)
    return pl.pallas_call(
        tail_kernel,
        out_shape=jax.ShapeDtypeStruct((tokens, depth), BF16),
        in_specs=[vmem] * 3,
        out_specs=pl.BlockSpec(memory_space=pl.ANY),
        scratch_shapes=[pltpu.VMEM((tail, tokens, CHUNK), BF16), dma((tail + 1,))],
        compiler_params=pltpu.CompilerParams(vmem_limit_bytes=16 * 2**20),
    )(done, gated, last)


def solution(mesh):
    tokens = P(("seq", "head"), None)
    placed = (tokens,) * 5 + (P("head", None), P("head"), P("head", None))
    return jax.shard_map(
        functools.partial(shards, mesh.shape["seq"], mesh.shape["head"]),
        mesh=mesh, in_specs=placed, out_specs=tokens, check_vma=False,
    )
```

```python
import functools

import jax
import jax.numpy as jnp
from jax import lax
from jax.experimental import pallas as pl
from jax.experimental.pallas import tpu as pltpu
from jax.sharding import PartitionSpec as P

BLOCK = 128
LANES = 128
QUAD = 256
CHUNK = 512
LEAD = 4
WAYS = 2
TAIL = 1
EXTRA = 8
EPS = 1e-05
MESH = pl.DeviceIdType.MESH
F32 = jnp.float32
BF16 = jnp.bfloat16


def dot(a, b):
    return jnp.dot(a, b, preferred_element_type=F32)


def dot_nt(a, b):
    return lax.dot_general(a, b, (((1,), (1,)), ((), ())), preferred_element_type=F32)


def dot_tn(a, b):
    return lax.dot_general(a, b, (((0,), (0,)), ((), ())), preferred_element_type=F32)


def split_heads(x, low):
    zero = jnp.zeros_like(x)
    return jnp.concatenate([jnp.where(low, x, zero), jnp.where(low, zero, x)], axis=0)


def flip(r, i, members):
    q, bit = 0, 1
    while bit < members:
        q = q + bit * (((r // bit) % 2 + (i // bit) % 2) % 2)
        bit *= 2
    return q


def kernel(
    n, cores, breadth,
    rec_hbm, key_hbm, val_hbm, fade_hbm, gate_hbm, reward_hbm, gain_hbm, map_hbm,
    out_ref, gated, weight_tail,
    held, rewards, gains, weight_head,
    reward_row, cumx, key_mid, centred, recs, local_out, swish, entering, pref_row, mid_row,
    outbox, inbox, before, before_dec, gout, gin, cbox, carry, partial,
    in_sem, p_local, p_send, p_recv, w_sem, w_send,
    s_send, s_recv, g_send, g_recv, c_send, c_recv, ready,
):
    me, core = lax.axis_index("seq"), lax.axis_index("head")
    other = 1 - core
    tokens, width = held.shape[1:]
    half = width // cores
    parts, span = outbox.shape[:2]
    owner = cores - 1
    ways = parts // cores
    lane = width // parts
    blocks, quads = tokens // BLOCK, lane // QUAD
    split = weight_head.shape[1]
    chunks = split + weight_tail.shape[1]
    lead = min(LEAD, chunks)
    members = span * cores
    groups = n // span
    group = me // span
    chip = me % span
    r = chip * cores + core
    peers = [flip(r, i, members) for i in range(members - 1, 0, -1)]
    chips = [flip(chip, i, span) for i in range(span - 1, -1, -1)]
    fade, key, val, rec, gate = (held.at[i] for i in range(5))
    sources = (fade_hbm, key_hbm, val_hbm, rec_hbm, gate_hbm)

    def place(q):
        return (group * span + q // cores, q % cores)

    def above(g):
        return (g * span + me % span, core)

    barrier = pltpu.get_barrier_semaphore()
    for q in peers:
        pl.semaphore_signal(barrier, inc=1, device_id=place(q), device_id_type=MESH)

    pieces = [pl.ds(side * half, half) for side in range(cores)]
    for piece, at in enumerate(pieces):
        for i in (0, 2, 1):
            sem = in_sem.at[i if piece == 0 else piece + 2]
            pltpu.make_async_copy(sources[i].at[:, at], held.at[i, :, at], sem).start()

    def greet_above(g, c):
        pl.semaphore_signal(barrier, inc=1, device_id=above(g), device_id_type=MESH)
        return c

    lax.fori_loop(group + 1, groups, greet_above, 0)
    for i in range(3, 5):
        pltpu.make_async_copy(sources[i], held.at[i], in_sem.at[len(pieces) + 2]).start()

    def wait_all(ref, sem):
        pltpu.make_async_copy(ref, ref, sem).wait()

    small = ((reward_hbm, rewards), (gain_hbm, gains))
    small_local = [
        pltpu.make_async_copy(src, dst.at[core], p_local.at[i]) for i, (src, dst) in enumerate(small)
    ]

    def small_copy(i, side):
        src, dst = small[i]
        return pltpu.make_async_remote_copy(
            src_ref=src, dst_ref=dst.at[side], send_sem=p_send.at[i], recv_sem=p_recv.at[i],
            device_id=(me, other), device_id_type=MESH,
        )

    for copy in small_local:
        copy.start()

    def columns(k):
        return map_hbm.at[:, pl.ds(k * CHUNK, CHUNK)]

    def weight(side, k):
        return weight_head.at[side, k] if k < split else weight_tail.at[side, k - split]

    def weight_sem(k):
        return w_sem.at[0 if k < lead else 1 if k < split else 2]

    def send_weight(start, stop=2 * chunks):
        for piece in range(start, min(stop, 2 * chunks)):
            k, rows = piece // 2, pl.ds(piece % 2 * (half // 2), half // 2)
            pltpu.make_async_remote_copy(
                src_ref=map_hbm.at[rows, pl.ds(k * CHUNK, CHUNK)], dst_ref=weight(core, k).at[rows],
                send_sem=w_send.at[0], recv_sem=weight_sem(k),
                device_id=(me, other), device_id_type=MESH,
            ).start()

    t_id = lax.broadcasted_iota(jnp.int32, (BLOCK, 2 * BLOCK), 0)
    s_id = lax.rem(lax.broadcasted_iota(jnp.int32, (BLOCK, 2 * BLOCK), 1), BLOCK)
    incl = jnp.where(t_id >= s_id, 1.0, 0.0).astype(BF16)
    low = lax.broadcasted_iota(jnp.int32, (BLOCK, LANES), 1) < breadth
    low_s = lax.broadcasted_iota(jnp.int32, (breadth, LANES), 1) < breadth
    row_x = lax.broadcasted_iota(jnp.int32, (EXTRA, LANES), 0)
    head_i = lax.broadcasted_iota(jnp.int32, (QUAD, QUAD), 0)
    head_j = lax.broadcasted_iota(jnp.int32, (QUAD, QUAD), 1)
    same, equal = head_i // breadth == head_j // breadth, head_i == head_j
    means = jnp.where(same, 1.0 / breadth, 0.0).astype(BF16)
    centre = (jnp.where(equal, 1.0, 0.0) - jnp.where(same, 1.0 / breadth, 0.0)).astype(BF16)
    ones = jnp.where(same, 1.0, 0.0).astype(BF16)
    state_rows, decay_rows = pl.ds(0, breadth), pl.ds(breadth, EXTRA)
    cuts = [slice(j * LANES, (j + 1) * LANES) for j in range(2)]

    def pack_rows(dec):
        hi = dec.astype(BF16).astype(F32)
        return jnp.where(row_x == 0, hi, jnp.where(row_x == 1, dec - hi, 0.0)).astype(BF16)

    def unpack_rows(x):
        x = x.astype(F32)
        return x[0:1] + x[1:2]

    def quad_lanes(p, t):
        return pl.ds(p * lane + t * QUAD, QUAD)

    def arrive(side, i):
        if side == 0:
            wait_all(held.at[i, :, pieces[0]], in_sem.at[i])

    def decays(side):
        turns = range(ways * quads)
        cells = [(t, b) for t in turns for b in range(blocks)]
        p = side * ways
        cums, vbs, kms, products = {}, {}, {}, {}
        arrive(side, 0)
        for t, b in cells:
            at, lanes = pl.ds(b * BLOCK, BLOCK), quad_lanes(p, t)
            log_decay = -jnp.exp(fade[at, lanes].astype(F32))
            hi = log_decay.astype(BF16)
            lo = (log_decay - hi.astype(F32)).astype(BF16)
            cum = dot(incl, jnp.concatenate([hi, lo], axis=0))
            cumx[at, lanes] = cum - log_decay
            cums[t, b] = cum
        arrive(side, 2)
        for t, b in cells:
            at, lanes = pl.ds(b * BLOCK, BLOCK), quad_lanes(p, t)
            vbs[t, b] = dot(val[at, lanes], centre).astype(BF16)
            centred[at, lanes] = vbs[t, b]
        arrive(side, 1)
        for t, b in cells:
            at, lanes = pl.ds(b * BLOCK, BLOCK), quad_lanes(p, t)
            mid = cums[t, b][BLOCK // 2 - 1 : BLOCK // 2]
            kms[t, b] = (key[at, lanes].astype(F32) * jnp.exp(mid - cums[t, b])).astype(BF16)
            key_mid[at, lanes] = kms[t, b]
            mid_row[b, :, lanes] = mid
        for t, b in cells:
            for j, cut in enumerate(cuts):
                products[t, b, j] = dot_tn(vbs[t, b][:, cut], kms[t, b][:, cut])
        for t in turns:
            lanes = quad_lanes(p, t)
            states = [jnp.zeros((breadth, LANES), F32) for _ in range(2)]
            pref = jnp.zeros((1, QUAD), F32)
            for b in range(blocks):
                cum = cums[t, b]
                mid, total = cum[BLOCK // 2 - 1 : BLOCK // 2], cum[BLOCK - 1 :]
                end, whole, begin = jnp.exp(total - mid), jnp.exp(total), jnp.exp(mid)
                pref_row[b, :, lanes] = pref
                for j, cut in enumerate(cuts):
                    if b > 0:
                        entering[p + t // quads, b - 1, t % quads * 2 + j] = (states[j] * begin[:, cut]).astype(BF16)
                    product = products[t, b, j]
                    own = jnp.where(low_s, product[:breadth], product[breadth:])
                    states[j] = states[j] * whole[:, cut] + own * end[:, cut]
                pref = pref + total
            gone = jnp.exp(pref)
            for j, cut in enumerate(cuts):
                outbox[p + t // quads, t % quads * 2 + j, state_rows, :] = states[j].astype(BF16)
                outbox[p + t // quads, t % quads * 2 + j, decay_rows, :] = pack_rows(gone[:, cut])

    def within(units):
        cells = [(p, t, b) for p, t in units for b in range(blocks)]
        rms, diags, scored = {}, {}, {}
        for p, t, b in cells:
            at, lanes = pl.ds(b * BLOCK, BLOCK), quad_lanes(p, t)
            cx = cumx[at, lanes]
            rf = rec[at, lanes].astype(F32)
            rms[p, t, b] = (rf * jnp.exp(cx - mid_row[b, :, lanes])).astype(BF16)
            recs[at, lanes] = (rf * jnp.exp(cx + pref_row[b, :, lanes])).astype(BF16)
            own = rf * key[at, lanes].astype(F32) * reward_row[:, lanes]
            diags[p, t, b] = dot(own.astype(BF16), ones)
            kb = key_mid[at, lanes]
            for j, cut in enumerate(cuts):
                scored[p, t, b, j] = dot_nt(rms[p, t, b][:, cut], split_heads(kb[:, cut], low))
        for p, t, b in cells:
            at, lanes = pl.ds(b * BLOCK, BLOCK), quad_lanes(p, t)
            g = gate[at, lanes].astype(F32)
            swish[at, lanes] = g / (1.0 + jnp.exp(-g)) * gains[p * lane // half, :, pl.ds(p * lane % half + t * QUAD, QUAD)]
        for p, t, b in cells:
            at, lanes = pl.ds(b * BLOCK, BLOCK), quad_lanes(p, t)
            vb = centred[at, lanes]
            for j, cut in enumerate(cuts):
                scores = jnp.where(t_id > s_id, scored[p, t, b, j], 0.0).astype(BF16)
                o = dot(scores, split_heads(vb[:, cut], low))
                if b > 0:
                    came = split_heads(entering[p, b - 1, 2 * t + j], low_s)
                    o = o + dot_nt(rms[p, t, b][:, cut], came)
                o = o + diags[p, t, b][:, cut] * vb[:, cut].astype(F32)
                local_out[at, pl.ds(p * lane + t * QUAD + j * LANES, LANES)] = o

    def finish(ps, between=()):
        cells = [(p, t) for p in ps for t in range(quads)]
        states, outs = {}, {}
        for p, t in cells:
            x, y = (split_heads(carry[p, 2 * t + j], low_s) for j in range(2))
            none = jnp.zeros_like(x)
            states[p, t] = jnp.concatenate(
                [jnp.concatenate([x, none], axis=1), jnp.concatenate([none, y], axis=1)], axis=0
            )
        for p, t in cells:
            lanes = quad_lanes(p, t)
            outs[p, t] = local_out[:, lanes] + dot_nt(recs[:, lanes], states[p, t])
        squares = [(outs[cell] * outs[cell]).astype(BF16) for cell in cells]
        variances = dot(jnp.concatenate(squares, axis=0), means)
        for k in between:
            project(k, 0, cores - 1)
        for i, (p, t) in enumerate(cells):
            lanes = quad_lanes(p, t)
            variance = variances[i * tokens : (i + 1) * tokens]
            scale = lax.rsqrt(variance + EPS) * swish[:, lanes]
            gated[:, lanes] = (outs[p, t] * scale).astype(BF16)

    def send_states(p):
        def send(t):
            pltpu.make_async_remote_copy(
                src_ref=outbox.at[p, t], dst_ref=inbox.at[p, r],
                send_sem=s_send.at[0], recv_sem=s_recv.at[p],
                device_id=(group * span + t, owner), device_id_type=MESH,
            ).start()

        for t in chips[:-1]:
            send(t)

        @pl.when(core == owner)
        def _():
            inbox[p, r] = outbox[p, chip]

        @pl.when(core != owner)
        def _():
            send(chip)

    some = pl.ds(0, members - 1)

    def advance(box, state):
        s, d = state
        e = unpack_rows(box[decay_rows, :])
        return s * e + box[state_rows, :].astype(F32), d * e

    nothing = (jnp.zeros((breadth, LANES), F32), jnp.ones((1, LANES), F32))

    def scan(p):
        state = nothing
        for j in range(members):
            before[p, j] = state[0]
            before_dec[p, j] = state[1]
            state = advance(inbox.at[p, j], state)
        gout[p, state_rows, :] = state[0].astype(BF16)
        gout[p, decay_rows, :] = pack_rows(state[1])

    def group_copy(p, g, slot):
        return pltpu.make_async_remote_copy(
            src_ref=gout.at[p], dst_ref=gin.at[p, slot],
            send_sem=g_send.at[0], recv_sem=g_recv.at[p, slot],
            device_id=above(g), device_id_type=MESH,
        )

    def send_group(p):
        def body(i, c):
            group_copy(p, groups - 1 - i, group).start()
            return c

        lax.fori_loop(0, groups - 1 - group, body, 0)

    def take_group(p):
        def body(g, state):
            group_copy(p, g, g).wait_recv()
            return advance(gin.at[p, g], state)

        return lax.fori_loop(0, group, body, nothing)[0]

    def send_carry(way, came):
        p = way
        for j in range(members):
            cbox[way, j] = (came * before_dec[way, j] + before[way, j]).astype(BF16)
        for q in peers:
            pltpu.make_async_remote_copy(
                src_ref=cbox.at[way, q], dst_ref=carry.at[p, chip],
                send_sem=c_send.at[0], recv_sem=c_recv.at[min(p, parts - ways)],
                device_id=place(q), device_id_type=MESH,
            ).start()
        carry[p, chip] = cbox[way, r]

    with jax.named_scope("decays0"):
        decays(0)
    with jax.named_scope("barrier"):
        pl.semaphore_wait(barrier, members - 1 + group)
        for p in range(ways):
            send_states(p)
        for i in range(2):
            small_copy(i, core).start()
        send_weight(0, 1)

        def here(g, c):
            pl.semaphore_signal(ready, inc=1, device_id=above(g), device_id_type=MESH)
            return c

        @pl.when(core == owner)
        def _():
            lax.fori_loop(0, group, here, 0)

        for k in range(chunks):
            pltpu.make_async_copy(columns(k), weight(core, k), weight_sem(k)).start()
    for side in range(1, cores):
        with jax.named_scope("in1"):
            wait_all(held.at[pl.ds(0, 3), :, pieces[side]], in_sem.at[side + 2])
        with jax.named_scope("decays1"):
            decays(side)
        with jax.named_scope("send1"):
            for p in range(side * ways, side * ways + ways):
                send_states(p)
    sent = 5
    send_weight(1, sent)

    @pl.when(core != owner)
    def _():
        send_weight(sent)

    with jax.named_scope("in2"):
        wait_all(held.at[pl.ds(3, 2)], in_sem.at[len(pieces) + 2])
        for i in range(2):
            small_local[i].wait()
            small_copy(i, other).wait_recv()
        for h in range(width // breadth):
            reward_row[:, pl.ds(h * breadth, breadth)] = rewards[
                h * breadth // half, pl.ds(h % (half // breadth), 1), :
            ]

    units = [(p, t) for p in range(parts) for t in range(quads)]
    done = 0

    def some_within(count):
        nonlocal done
        for at in range(done, min(done + count, len(units)), 2):
            with jax.named_scope("within"):
                within(units[at : at + 2])
        done += count

    some_within(4)
    for p in range(parts):
        @pl.when(core == owner)
        def _():
            with jax.named_scope("wait_states"):
                wait_all(inbox.at[p, some], s_recv.at[p])
            with jax.named_scope("scan"):
                scan(p)
            if p == 0:
                @pl.when(group < groups - 1)
                def _():
                    pl.semaphore_wait(ready, groups - 1 - group)

            send_group(p)

            @pl.when(group == 0)
            def _():
                send_carry(p, nothing[0])
                send_weight(sent + p, sent + p + 1 if p < parts - 1 else 2 * chunks)

            @pl.when(group > 0)
            def _():
                send_weight(sent + p, sent + p + 1 if p < parts - 1 else sent + p + 2)

        if p % 2:
            some_within(2)
    sent += parts + 1

    @pl.when(core == owner)
    def _():
        @pl.when(group > 0)
        def _():
            for p in range(parts):
                with jax.named_scope("take_group"):
                    came = take_group(p)
                with jax.named_scope("send_carry"):
                    send_carry(p, came)
            send_weight(sent)

    def project(k, first, last):
        at = pl.ds(k * CHUNK, CHUNK)
        total = partial[:, at] if first > 0 else None
        for p in range(first, last):
            term = dot(gated[:, pl.ds(p * half, half)], weight(p, k)[...])
            total = term if total is None else total + term
        if last < cores:
            partial[:, at] = total
        else:
            out_ref[:, at] = total.astype(BF16)

    early = parts - ways

    def wait_carry(first, count):
        some_parts = pl.ds(first, count)

        @pl.when(core == owner)
        def _():
            wait_all(carry.at[some_parts, pl.ds(0, span - 1)], c_recv.at[first])

        @pl.when(core != owner)
        def _():
            wait_all(carry.at[some_parts], c_recv.at[first])

    with jax.named_scope("wait_weight"):
        wait_all(weight_head.at[:, pl.ds(0, lead)], w_sem.at[0])
    for p in range(early):
        with jax.named_scope("wait_carry"):
            wait_carry(p, 1)
        if p < early - 1:
            with jax.named_scope("finish"):
                finish([p])
    with jax.named_scope("finish"):
        finish([early - 1])
        for k in range(lead - 1):
            project(k, 0, cores - 1)
    with jax.named_scope("wait_carry"):
        wait_carry(early, ways)
    with jax.named_scope("project"):
        finish(range(early, parts), range(lead - 1, lead))
        for k in range(lead):
            project(k, cores - 1, cores)
    with jax.named_scope("wait_weight"):
        wait_all(weight_head.at[:, pl.ds(lead, split - lead)], w_sem.at[1])
    with jax.named_scope("project_rest"):
        for k in range(lead, split):
            project(k, 0, cores)
    with jax.named_scope("wait_weight"):
        wait_all(weight_tail, w_sem.at[2])

    def drain_groups(g):
        wait_all(gin.at[:, pl.ds(0, groups - 1 - g)], g_send.at[0])

    with jax.named_scope("drain"):
        @pl.when(core == owner)
        def _():
            for g in range(groups - 1):
                pl.when(group == g)(functools.partial(drain_groups, g))
            wait_all(outbox.at[:, pl.ds(0, span - 1)], s_send.at[0])
            wait_all(cbox.at[:, some], c_send.at[0])

        @pl.when(core != owner)
        def _():
            wait_all(outbox, s_send.at[0])

        wait_all(map_hbm, w_send.at[0])
        for i in range(2):
            small_copy(i, core).wait_send()


def tail_kernel(done_ref, gated_ref, weight_ref, out_hbm, last, sem):
    cores, tail, half, chunk = weight_ref.shape
    done = done_ref.shape[1]
    copies = [pltpu.make_async_copy(done_ref, out_hbm.at[:, pl.ds(0, done)], sem.at[0])]
    copies[0].start()
    for k in range(tail):
        total = dot(gated_ref[:, pl.ds(0, half)], weight_ref[0, k])
        for p in range(1, cores):
            total = total + dot(gated_ref[:, pl.ds(p * half, half)], weight_ref[p, k])
        last[k] = total.astype(BF16)
        at = pl.ds(done + k * chunk, chunk)
        copies.append(pltpu.make_async_copy(last.at[k], out_hbm.at[:, at], sem.at[k + 1]))
        copies[-1].start()
    for copy in copies:
        copy.wait()


def shards(n, cores, rec, key, val, fade, gate, reward, gain, mapping):
    tokens, width = rec.shape
    breadth = reward.shape[1]
    half, depth = mapping.shape
    ways = WAYS
    parts = ways * cores
    blocks, chunks, span = tokens // BLOCK, depth // CHUNK, width // parts // LANES
    members, groups = span * cores, n // span
    boxed = breadth + EXTRA
    dma = pltpu.SemaphoreType.DMA
    narrow = pltpu.VMEM((tokens, width), BF16)
    wide = pltpu.VMEM((tokens, width), F32)
    tail = min(TAIL, chunks - LEAD)
    split = chunks - tail
    vmem = pl.BlockSpec(memory_space=pltpu.VMEM)
    done, gated, last = pl.pallas_call(
        functools.partial(kernel, n, cores, breadth),
        out_shape=(
            pltpu.VMEM((tokens, split * CHUNK), BF16),
            pltpu.VMEM((tokens, width), BF16),
            pltpu.VMEM((cores, tail, half, CHUNK), BF16),
        ),
        in_specs=[pl.BlockSpec(memory_space=pl.ANY)] * 8,
        out_specs=(vmem,) * 3,
        scratch_shapes=[
            pltpu.VMEM((5, tokens, width), BF16),
            pltpu.VMEM((cores,) + reward.shape, F32),
            pltpu.VMEM((cores, 1, half), F32),
            pltpu.VMEM((cores, split, half, CHUNK), BF16),
            pltpu.VMEM((1, width), F32),
            wide, narrow, narrow, narrow, wide, wide,
            pltpu.VMEM((parts, max(blocks - 1, 1), span, breadth, LANES), BF16),
            pltpu.VMEM((blocks, 1, width), F32),
            pltpu.VMEM((blocks, 1, width), F32),
            pltpu.VMEM((parts, span, boxed, LANES), BF16),
            pltpu.VMEM((parts, members, boxed, LANES), BF16),
            pltpu.VMEM((parts, members, breadth, LANES), F32),
            pltpu.VMEM((parts, members, 1, LANES), F32),
            pltpu.VMEM((parts, boxed, LANES), BF16),
            pltpu.VMEM((parts, groups, boxed, LANES), BF16),
            pltpu.VMEM((parts, members, breadth, LANES), BF16),
            pltpu.VMEM((parts, span, breadth, LANES), BF16),
            pltpu.VMEM((tokens, LEAD * CHUNK), F32),
            dma((cores + 3,)), dma((2,)), dma((2,)), dma((2,)),
            dma((3,)), dma((1,)),
            dma((1,)), dma((parts,)), dma((1,)), dma((parts, groups)),
            dma((1,)), dma((parts - ways + 1,)), pltpu.SemaphoreType.REGULAR,
        ],
        compiler_params=pltpu.CompilerParams(
            collective_id=0, has_side_effects=True, vmem_limit_bytes=55 * 2**20
        ),
    )(rec, key, val, fade, gate, reward, gain.reshape(1, -1), mapping)
    return pl.pallas_call(
        tail_kernel,
        out_shape=jax.ShapeDtypeStruct((tokens, depth), BF16),
        in_specs=[vmem] * 3,
        out_specs=pl.BlockSpec(memory_space=pl.ANY),
        scratch_shapes=[pltpu.VMEM((tail, tokens, CHUNK), BF16), dma((tail + 1,))],
        compiler_params=pltpu.CompilerParams(vmem_limit_bytes=16 * 2**20),
    )(done, gated, last)


def solution(mesh):
    tokens = P(("seq", "head"), None)
    placed = (tokens,) * 5 + (P("head", None), P("head"), P("head", None))
    return jax.shard_map(
        functools.partial(shards, mesh.shape["seq"], mesh.shape["head"]),
        mesh=mesh, in_specs=placed, out_specs=tokens, check_vma=False,
    )
```
